32 devices in a mesh: dp: 2 (over x), ep: 16 (over z, y, core).
Axes of the slice: x: 2, y: 2, z: 4, core: 2. Of those that a mesh axis runs over, the one named last changes fastest.
Arguments:
- grad_y: bfloat16 [8192, 1024], P(('dp', 'ep')), parts along dimension 0
- gate_vals: float32 [8192, 8], P(('dp', 'ep')), parts along dimension 0
- topk_idx: int32 [8192, 8], P(('dp', 'ep')), parts along dimension 0
- slot_ids: int32 [8192, 8], P(('dp', 'ep')), parts along dimension 0
- pair_counts: int32 [32, 32], P(('dp', 'ep')), parts along dimension 0
- y_routed: bfloat16 [8192, 8, 1024], P(('dp', 'ep')), parts along dimension 0
- x_disp: bfloat16 [64, 2048, 1024], P(('dp', 'ep')), parts along dimension 0
- h_gate: bfloat16 [64, 2048, 512], P(('dp', 'ep')), parts along dimension 0
- h_up: bfloat16 [64, 2048, 512], P(('dp', 'ep')), parts along dimension 0
- w_gate: bfloat16 [32, 1024, 512], P('ep')
- w_up: bfloat16 [32, 1024, 512], P('ep')
- w_down: bfloat16 [32, 512, 1024], P('ep')
Outputs:
- output 1: bfloat16 [8192, 1024], P(('dp', 'ep')), parts along dimension 0
- output 2: float32 [8192, 8], P(('dp', 'ep')), parts along dimension 0
- output 3: float32 [64, 1024, 512], P(('dp', 'ep')), parts along dimension 0
- output 4: float32 [64, 1024, 512], P(('dp', 'ep')), parts along dimension 0
- output 5: float32 [64, 512, 1024], P(('dp', 'ep')), parts along dimension 0
There are 2 independent parts. The reference program is written for one: setup_inputs(seed, part) draws one part's arguments, and reference() takes and returns one part's arrays. A program takes and returns all parts, laid end to end along the dimension named above; an argument that names none is the same for every part.
All inputs are finite; a program needn't handle non-finite values.
Results may differ from the reference program's by a relative error of at most 0.0149559.
Values are sent between devices in bfloat16 or wider.
A program may use at most 1 GiB of HBM per device.

```python
import jax
import jax.numpy as jnp
from jax import lax

GROUP_DEV = 16
TOKENS_DEV = 256
EXPERTS = 32
TOP_K = 8
MODEL_DIM = 1024
FFN_DIM = 512
CAPACITY = 128
N_TOKENS = GROUP_DEV * TOKENS_DEV
EXPERT_ROWS = GROUP_DEV * CAPACITY


def setup_inputs(seed: int = 0, part: int = 0) -> dict:
    base_key = jax.random.fold_in(jax.random.key(seed), part)
    key_list = jax.random.split(base_key, 8)
    weight_keys = jax.random.split(jax.random.key(seed + 1), 3)
    key_noise, key_bias, key_hot = jax.random.split(key_list[0], 3)
    expert_iota = jnp.arange(EXPERTS, dtype=jnp.int32)
    token_iota = jnp.arange(TOKENS_DEV, dtype=jnp.int32)
    noise_int = jax.random.randint(key_noise, (GROUP_DEV, TOKENS_DEV, EXPERTS), 0, 4 * EXPERTS)
    bias_base = jax.random.randint(key_bias, (EXPERTS,), 0, 2 * EXPERTS)
    bias_int = (bias_base * bias_base) // (4 * EXPERTS)
    hot_expert = jax.random.randint(key_hot, (GROUP_DEV,), 0, EXPERTS)
    hot_bonus = jnp.where((token_iota[None, :, None] < CAPACITY) & (expert_iota[None, None, :] == hot_expert[:, None, None]), 8 * EXPERTS, 0)
    scores = (noise_int + bias_int[None, None, :] + hot_bonus) * EXPERTS + expert_iota[None, None, :]
    expert_ids = lax.top_k(scores, TOP_K)[1].astype(jnp.int32)

    def rank_one(ids_dev):
        flat_ids = ids_dev.reshape(-1)
        onehot = (flat_ids[:, None] == expert_iota[None, :]).astype(jnp.int32)
        before = jnp.cumsum(onehot, axis=0) - onehot
        rank_pos = jnp.sum(before * onehot, axis=1)
        return rank_pos.reshape(TOKENS_DEV, TOP_K), jnp.sum(onehot, axis=0)

    rank_pos, n_total = lax.map(rank_one, expert_ids)
    slot_dev = jnp.where(rank_pos < CAPACITY, rank_pos, -1).astype(jnp.int32)
    pair_counts = jnp.minimum(n_total, CAPACITY).astype(jnp.int32)
    is_kept = slot_dev >= 0
    slot_safe = jnp.where(is_kept, slot_dev, CAPACITY)
    slot_clip = jnp.where(is_kept, slot_dev, 0)
    src_dev = jnp.broadcast_to(jnp.arange(GROUP_DEV, dtype=jnp.int32)[:, None, None], expert_ids.shape)

    w_gate = (jax.random.normal(weight_keys[0], (EXPERTS, MODEL_DIM, FFN_DIM), jnp.float32) * MODEL_DIM ** -0.5).astype(jnp.bfloat16)
    w_up = (jax.random.normal(weight_keys[1], (EXPERTS, MODEL_DIM, FFN_DIM), jnp.float32) * MODEL_DIM ** -0.5).astype(jnp.bfloat16)
    w_down = (jax.random.normal(weight_keys[2], (EXPERTS, FFN_DIM, MODEL_DIM), jnp.float32) * FFN_DIM ** -0.5).astype(jnp.bfloat16)
    x_tok = jax.random.normal(key_list[1], (GROUP_DEV, TOKENS_DEV, MODEL_DIM), jnp.float32).astype(jnp.bfloat16)
    stale_rows = jax.random.normal(key_list[2], (EXPERTS, GROUP_DEV, CAPACITY, MODEL_DIM), jnp.float32).astype(jnp.bfloat16)
    x_vals = jnp.broadcast_to(x_tok[:, :, None, :], (GROUP_DEV, TOKENS_DEV, TOP_K, MODEL_DIM))
    x_disp = stale_rows.at[expert_ids, src_dev, slot_safe].set(x_vals, mode="drop").reshape(EXPERTS, EXPERT_ROWS, MODEL_DIM)

    def forward_one(operands):
        x_rows, w_gate_e, w_up_e, w_down_e = operands
        h_g = jnp.dot(x_rows, w_gate_e, preferred_element_type=jnp.float32).astype(jnp.bfloat16)
        h_u = jnp.dot(x_rows, w_up_e, preferred_element_type=jnp.float32).astype(jnp.bfloat16)
        gate_f = h_g.astype(jnp.float32)
        hidden_act = (gate_f * jax.nn.sigmoid(gate_f) * h_u.astype(jnp.float32)).astype(jnp.bfloat16)
        y_rows = jnp.dot(hidden_act, w_down_e, preferred_element_type=jnp.float32).astype(jnp.bfloat16)
        return h_g, h_u, y_rows

    h_gate, h_up, y_exp = lax.map(forward_one, (x_disp, w_gate, w_up, w_down))
    y_pick = y_exp.reshape(EXPERTS, GROUP_DEV, CAPACITY, MODEL_DIM)[expert_ids, src_dev, slot_clip]
    y_routed = jnp.where(is_kept[..., None], y_pick, jnp.zeros((), jnp.bfloat16)).reshape(N_TOKENS, TOP_K, MODEL_DIM)
    grad_y = jax.random.normal(key_list[3], (N_TOKENS, MODEL_DIM), jnp.float32).astype(jnp.bfloat16)
    gate_vals = jax.random.uniform(key_list[4], (N_TOKENS, TOP_K), jnp.float32, 0.25, 1.0)
    return {"grad_y": grad_y, "gate_vals": gate_vals, "topk_idx": expert_ids.reshape(N_TOKENS, TOP_K), "slot_ids": slot_dev.reshape(N_TOKENS, TOP_K), "pair_counts": pair_counts, "y_routed": y_routed, "x_disp": x_disp, "h_gate": h_gate, "h_up": h_up, "w_gate": w_gate, "w_up": w_up, "w_down": w_down}


def reference(grad_y, gate_vals, topk_idx, slot_ids, pair_counts, y_routed, x_disp, h_gate, h_up, w_gate, w_up, w_down):
    grad_gate = jnp.einsum("td,tkd->tk", grad_y.astype(jnp.float32), y_routed.astype(jnp.float32))
    is_kept = slot_ids >= 0
    src_dev = jnp.broadcast_to((jnp.arange(N_TOKENS, dtype=jnp.int32) // TOKENS_DEV)[:, None], topk_idx.shape)
    slot_safe = jnp.where(is_kept, slot_ids, CAPACITY)
    slot_clip = jnp.where(is_kept, slot_ids, 0)
    gated_rows = (gate_vals[:, :, None] * grad_y.astype(jnp.float32)[:, None, :]).astype(jnp.bfloat16)
    disp_rows = jnp.zeros((EXPERTS, GROUP_DEV, CAPACITY, MODEL_DIM), jnp.bfloat16).at[topk_idx, src_dev, slot_safe].set(gated_rows, mode="drop")
    keep_row = jnp.arange(CAPACITY)[None, None, :] < jnp.transpose(pair_counts)[:, :, None]
    disp_rows = jnp.where(keep_row[..., None], disp_rows, jnp.zeros((), jnp.bfloat16)).reshape(EXPERTS, EXPERT_ROWS, MODEL_DIM)

    def expert_one(operands):
        grad_rows, x_rows, hg_rows, hu_rows, w_gate_e, w_up_e, w_down_e = operands
        grad_hidden = jnp.dot(grad_rows, w_down_e.T, preferred_element_type=jnp.float32).astype(jnp.bfloat16)
        gate_f = hg_rows.astype(jnp.float32)
        up_f = hu_rows.astype(jnp.float32)
        gate_sig = jax.nn.sigmoid(gate_f)
        gate_act = gate_f * gate_sig
        hidden_act = (gate_act * up_f).astype(jnp.bfloat16)
        grad_h = grad_hidden.astype(jnp.float32)
        grad_hgate = (grad_h * up_f * gate_sig * (1.0 + gate_f * (1.0 - gate_sig))).astype(jnp.bfloat16)
        grad_hup = (grad_h * gate_act).astype(jnp.bfloat16)
        grad_wdown = jnp.dot(hidden_act.T, grad_rows, preferred_element_type=jnp.float32)
        grad_wgate = jnp.dot(x_rows.T, grad_hgate, preferred_element_type=jnp.float32)
        grad_wup = jnp.dot(x_rows.T, grad_hup, preferred_element_type=jnp.float32)
        grad_disp = (jnp.dot(grad_hgate, w_gate_e.T, preferred_element_type=jnp.float32) + jnp.dot(grad_hup, w_up_e.T, preferred_element_type=jnp.float32)).astype(jnp.bfloat16)
        return grad_disp, grad_wgate, grad_wup, grad_wdown

    grad_disp, grad_w_gate, grad_w_up, grad_w_down = lax.map(expert_one, (disp_rows, x_disp, h_gate, h_up, w_gate, w_up, w_down))
    back_rows = grad_disp.reshape(EXPERTS, GROUP_DEV, CAPACITY, MODEL_DIM)[topk_idx, src_dev, slot_clip]
    grad_x = jnp.sum(jnp.where(is_kept[..., None], back_rows.astype(jnp.float32), 0.0), axis=1).astype(jnp.bfloat16)
    return grad_x, grad_gate, grad_w_gate, grad_w_up, grad_w_down
```

```python
import jax
import jax.numpy as jnp
from jax import lax
from jax.sharding import PartitionSpec as P

F32 = jnp.float32
BF16 = jnp.bfloat16


def routing_tables(gate_vals, topk_idx, slot_ids, pair_counts):
    n_exp = pair_counts.shape[1]
    hit = topk_idx[None] == lax.broadcasted_iota(jnp.int32, (n_exp, 1, 1), 0)
    slot = jnp.max(jnp.where(hit, slot_ids[None], -1), axis=2)
    gate = jnp.sum(jnp.where(hit, gate_vals[None], 0.0), axis=2)
    slot = jnp.where(slot < pair_counts.reshape(n_exp, 1), slot, -1)
    return slot, gate


def solution(mesh):
    n_dev = mesh.shape["ep"]
    rows_spec = P(("dp", "ep"), None)
    cube_spec = P(("dp", "ep"), None, None)
    weight_spec = P("ep", None, None)

    def local_step(grad_y, gate_vals, topk_idx, slot_ids, pair_counts, y_routed, x_disp, h_gate, h_up, w_gate, w_up, w_down):
        n_loc = w_gate.shape[0]
        cap_rows = x_disp.shape[1] // n_dev
        tok, model_dim = grad_y.shape
        all_y = lax.all_gather(grad_y, "ep")
        slot, gate = routing_tables(gate_vals, topk_idx, slot_ids, pair_counts)
        meta = jnp.stack([slot.astype(F32), gate], axis=1).reshape(n_dev, n_loc, 2, tok)
        meta = lax.all_to_all(meta, "ep", 0, 0)
        grad_gate = jnp.einsum("td,tkd->tk", grad_y, y_routed, preferred_element_type=F32)
        hot = meta[:, :, 0][:, :, None, :] == lax.broadcasted_iota(jnp.int32, (1, 1, cap_rows, 1), 2).astype(F32)
        gate_rows = jnp.sum(jnp.where(hot, meta[:, :, 1][:, :, None, :], 0.0), axis=3)
        pick = hot.astype(BF16)
        rows = jnp.einsum("sect,std->escd", pick, all_y, preferred_element_type=F32)
        grad_rows = (rows * jnp.transpose(gate_rows, (1, 0, 2))[..., None]).astype(BF16).reshape(n_loc, n_dev * cap_rows, model_dim)
        grad_h = jnp.einsum("erd,efd->erf", grad_rows, w_down, preferred_element_type=F32).astype(BF16).astype(F32)
        gate_f = h_gate.astype(F32)
        up_f = h_up.astype(F32)
        sig = jax.nn.sigmoid(gate_f)
        act = gate_f * sig
        hidden = (act * up_f).astype(BF16)
        d_gate = (grad_h * up_f * sig * (1.0 + gate_f * (1.0 - sig))).astype(BF16)
        d_up = (grad_h * act).astype(BF16)
        ret = (jnp.einsum("erf,edf->erd", d_gate, w_gate, preferred_element_type=F32) + jnp.einsum("erf,edf->erd", d_up, w_up, preferred_element_type=F32)).astype(BF16)
        part = jnp.einsum("sect,escd->std", pick, ret.reshape(n_loc, n_dev, cap_rows, model_dim), preferred_element_type=F32)
        grad_x = lax.psum_scatter(part.reshape(n_dev * tok, model_dim), "ep", scatter_dimension=0, tiled=True).astype(BF16)
        grad_wdown = jnp.einsum("erf,erd->efd", hidden, grad_rows, preferred_element_type=F32)
        grad_wgate = jnp.einsum("erd,erf->edf", x_disp, d_gate, preferred_element_type=F32)
        grad_wup = jnp.einsum("erd,erf->edf", x_disp, d_up, preferred_element_type=F32)
        return grad_x, grad_gate, grad_wgate, grad_wup, grad_wdown

    return jax.shard_map(local_step, mesh=mesh, in_specs=(rows_spec, rows_spec, rows_spec, rows_spec, rows_spec, cube_spec, cube_spec, cube_spec, cube_spec, weight_spec, weight_spec, weight_spec), out_specs=(rows_spec, rows_spec, cube_spec, cube_spec, cube_spec), check_vma=False)
```

```python
import jax
import jax.numpy as jnp
from jax import lax
from jax.experimental import pallas as pl
from jax.experimental.pallas import tpu as pltpu
from jax.sharding import PartitionSpec as P

F32 = jnp.float32
BF16 = jnp.bfloat16
VMEM = pltpu.VMEM
DMA = pltpu.SemaphoreType.DMA
ANY = pl.BlockSpec(memory_space=pl.ANY)
VM = pl.BlockSpec(memory_space=pltpu.VMEM)


def position():
    me = lax.axis_index("ep")
    return me, me // 4, (me // 2) % 2, me % 2


def near_first(z, k):
    m = z // 2
    zz = z + m * (3 - 2 * z)
    v = (zz, 1 - zz, 2, 3)[k]
    return v + m * (3 - 2 * v)


def far_first(z, k):
    m = z // 2
    zz = z + m * (3 - 2 * z)
    v = 3 - k + zz * jnp.where(k == 1, -2, jnp.where(k >= 2, 1, 0))
    return v + m * (3 - 2 * v)


def dot_nt(a, b):
    return lax.dot_general(a, b, (((1,), (1,)), ((), ())), preferred_element_type=F32)


def dot_tn(a, b):
    return lax.dot_general(a, b, (((0,), (0,)), ((), ())), preferred_element_type=F32)


def one_hot(slot, cap):
    return slot == lax.broadcasted_iota(jnp.int32, (cap, slot.shape[1]), 0).astype(F32)


def gather_kernel(gy, meta_out, hg_hbm, hu_hbm, wd_hbm, dh1_hbm, dh3_hbm, gwd_hbm, meta_res, tok, meta, hg, hu, wd, d_ref, a_ref, dh1, dh3, acc, ld_sem, st_sem, send, recv, m_send, m_recv):
    me, z, y, c = position()
    cap = d_ref.shape[0] // 2
    sib = me + 1 - 2 * c
    ynb = me + 2 - 4 * y
    end = (z == 0) | (z == 3)
    loads = [pltpu.make_async_copy(s, d, ld_sem.at[i]) for i, (s, d) in enumerate(((wd_hbm, wd), (hg_hbm, hg), (hu_hbm, hu)))]
    for cp in loads:
        cp.start()
    barrier = pltpu.get_barrier_semaphore()
    for k in range(1, 16):
        pl.semaphore_signal(barrier, inc=1, device_id={"ep": (me + k) % 16})
    pl.semaphore_wait(barrier, 15)

    def put(src, slot, way, to):
        return pltpu.make_async_remote_copy(src_ref=src, dst_ref=tok.at[slot], send_sem=send.at[slot, way], recv_sem=recv.at[slot], device_id={"ep": to})

    started = []

    def go(src, slot, way, to, cond=None):
        cp = put(src, slot, way, to)
        if cond is None:
            cp.start()
        else:
            pl.when(cond)(cp.start)
        started.append((cp, cond))

    def arrive(slot):
        put(tok.at[slot], slot, 0, me).wait_recv()

    def meta_copy(k):
        to = (me + k) % 16
        return pltpu.make_async_remote_copy(src_ref=meta_out.at[to // 2], dst_ref=meta.at[me], send_sem=m_send.at[k], recv_sem=m_recv.at[me], device_id={"ep": to})

    go(gy, me, 3, sib)
    for k in range(1, 16):
        meta_copy(k).start()
    go(gy, me, 0, (me + 4) % 16, z < 3)
    go(gy, me, 1, (me + 12) % 16, z > 0)
    go(gy, me, 2, ynb)
    tok[me] = gy[...]
    meta[me] = meta_out[me // 2]
    acc[...] = jnp.zeros_like(acc)
    for k in range(1, 16):
        src = (me + k) % 16
        pltpu.make_async_remote_copy(src_ref=meta_out.at[0], dst_ref=meta.at[src], send_sem=m_send.at[k], recv_sem=m_recv.at[src], device_id={"ep": src}).wait_recv()
    for cp in loads:
        cp.wait()

    def slot_of(zs, ys, cs):
        return zs * 4 + ys * 2 + cs

    def relay(k, cond=None):
        zs = near_first(z, k)
        slot = slot_of(zs, y, c)
        away = jnp.where(zs < z, 1, -1)
        nz = z + away
        inside = (nz >= 0) & (nz <= 3)

        def body():
            arrive(slot)
            pl.when(inside)(put(tok.at[slot], slot, 0, (me + 4 * away + 16) % 16).start)
            put(tok.at[slot], slot, 2, ynb).start()
            put(tok.at[slot], slot, 3, sib).start()

        body() if cond is None else pl.when(cond)(body)

    def y_arrival(k):
        slot = slot_of(near_first(z, k), 1 - y, c)
        arrive(slot)
        go(tok.at[slot], slot, 3, sib)

    def compute(zs, ys):
        chip = zs * 2 + ys
        rows = pl.ds(pl.multiple_of(chip * 2 * cap, 2 * cap), 2 * cap)

        def per_expert(e, _):
            for h in range(2):
                s = chip * 2 + h
                hot = one_hot(meta[s, c * 2 + e], cap)
                gate = jnp.sum(jnp.where(hot, meta[s, 4 + c * 2 + e], 0.0), axis=1, keepdims=True)
                picked = jnp.dot(jnp.where(hot, 1.0, 0.0).astype(BF16), tok[s], preferred_element_type=F32)
                d_ref[h * cap:(h + 1) * cap, :] = (picked * gate).astype(BF16)
            g = dot_nt(d_ref[...], wd[e]).astype(BF16).astype(F32)
            h1 = hg[e, rows, :].astype(F32)
            h3 = hu[e, rows, :].astype(F32)
            sig = jax.nn.sigmoid(h1)
            act = h1 * sig
            a_ref[...] = (act * h3).astype(BF16)
            dh1[e, rows, :] = (g * h3 * sig * (1.0 + h1 * (1.0 - sig))).astype(BF16)
            dh3[e, rows, :] = (g * act).astype(BF16)
            acc[e] += dot_tn(a_ref[...], d_ref[...])
            return 0

        lax.fori_loop(0, 2, per_expert, 0)

    def from_sib(k, ys):
        arrive(slot_of(near_first(z, k), ys, 1 - c))

    from_sib(0, y)
    compute(z, y)
    for phase in range(1, 5):
        if phase < 4:
            if phase == 1:
                relay(1)
                relay(2, jnp.logical_not(end))
            elif phase == 2:
                relay(2, end)
                relay(3, jnp.logical_not(end))
            else:
                relay(3, end)
        y_arrival(phase - 1)
        if phase < 4:
            from_sib(phase, y)
        from_sib(phase - 1, 1 - y)
        lo = near_first(z, phase - 1)
        hi = near_first(z, phase) if phase < 4 else lo

        def both(j, _, lo=lo, hi=hi):
            compute(jnp.where(j == 0, hi, lo), jnp.where(j == 0, y, 1 - y))
            return 0

        if phase < 4:
            lax.fori_loop(0, 2, both, 0)
        else:
            compute(lo, 1 - y)

    outs = [pltpu.make_async_copy(s, d, st_sem.at[i]) for i, (s, d) in enumerate(((dh1, dh1_hbm), (dh3, dh3_hbm), (acc, gwd_hbm)))]
    for cp in outs:
        cp.start()
    meta_res[...] = meta[...]
    for cp, cond in started:
        if cond is None:
            cp.wait_send()
        else:
            pl.when(cond)(cp.wait_send)
    for k in range(1, 4):
        zs = near_first(z, k)
        slot = slot_of(zs, y, c)
        nz = z + jnp.where(zs < z, 1, -1)
        pl.when((nz >= 0) & (nz <= 3))(put(tok.at[slot], slot, 0, me).wait_send)
        put(tok.at[slot], slot, 2, ynb).wait_send()
        put(tok.at[slot], slot, 3, sib).wait_send()
    for k in range(1, 16):
        meta_copy(k).wait_send()
    for cp in outs:
        cp.wait()


def return_kernel(meta, dh1_hbm, dh3_hbm, wg_hbm, wu_hbm, x_hbm, gx, gwg_hbm, gwu_hbm, dh1, dh3, wg, wu, x, r_own, r_send, r_recv, y_send, y_recv, tot, z_left, z_right, f_send, f_recv, og, ou, ld_sem, st_sem, rs, rr, ys_sem, yr_sem, zs_sem, zl_sem, zr_sem, fs, fr):
    me, z, y, c = position()
    n_loc, n_rows, ffn = dh1.shape
    cap = n_rows // 16
    half = r_own.shape[3]
    sib = me + 1 - 2 * c
    ynb = me + 2 - 4 * y
    loads = [pltpu.make_async_copy(s, d, ld_sem.at[i]) for i, (s, d) in enumerate(((wg_hbm, wg), (wu_hbm, wu), (dh1_hbm, dh1), (dh3_hbm, dh3), (x_hbm, x)))]
    for cp in loads:
        cp.start()
    barrier = pltpu.get_barrier_semaphore()
    pl.semaphore_signal(barrier, inc=1, device_id={"ep": sib})
    pl.semaphore_signal(barrier, inc=1, device_id={"ep": ynb})

    @pl.when(z > 0)
    def _():
        pl.semaphore_signal(barrier, inc=1, device_id={"ep": (me + 12) % 16})

    @pl.when(z < 3)
    def _():
        pl.semaphore_signal(barrier, inc=1, device_id={"ep": (me + 4) % 16})

    pl.semaphore_wait(barrier, 2 + jnp.where(z > 0, 1, 0) + jnp.where(z < 3, 1, 0))
    for cp in loads[:4]:
        cp.wait()

    def swap(chip):
        return pltpu.make_async_remote_copy(src_ref=r_send.at[chip], dst_ref=r_recv.at[chip], send_sem=rs.at[chip], recv_sem=rr.at[chip], device_id={"ep": sib})

    def y_copy(u):
        return pltpu.make_async_remote_copy(src_ref=y_send.at[u], dst_ref=y_recv.at[u], send_sem=ys_sem.at[u], recv_sem=yr_sem.at[u], device_id={"ep": ynb})

    def to_right(u):
        return pltpu.make_async_remote_copy(src_ref=tot.at[u], dst_ref=z_left.at[u], send_sem=zs_sem.at[u], recv_sem=zl_sem.at[u], device_id={"ep": (me + 4) % 16})

    def to_left(u):
        return pltpu.make_async_remote_copy(src_ref=tot.at[u], dst_ref=z_right.at[u], send_sem=zs_sem.at[u], recv_sem=zr_sem.at[u], device_id={"ep": (me + 12) % 16})

    def last(k=0):
        return pltpu.make_async_remote_copy(src_ref=f_send, dst_ref=f_recv, send_sem=fs.at[0], recv_sem=fr.at[0], device_id={"ep": sib})

    def place(j):
        k, other = j // 2, 1 - j % 2
        return far_first(z, k), y + other * (1 - 2 * y)

    def make_rows(j):
        d, yy = place(j)
        chip = d * 2 + yy
        rows = pl.ds(pl.multiple_of(chip * 2 * cap, 2 * cap), 2 * cap)

        def per_expert(e, _):
            for part, dest in ((1 - c, r_send), (c, r_own)):
                cols = pl.ds(pl.multiple_of(part * half, half), half)
                r = dot_nt(dh1[e, rows, :], wg[e, cols, :]) + dot_nt(dh3[e, rows, :], wu[e, cols, :])
                dest[chip, e] = r.astype(BF16)
            return 0

        lax.fori_loop(0, n_loc, per_expert, 0)
        swap(chip).start()

    def combine(j):
        d, yy = place(j)
        chip = d * 2 + yy
        swap(chip).wait_recv()
        for h in range(2):
            s = chip * 2 + h
            lanes = pl.ds(h * cap, cap)
            ids = (c * 2, c * 2 + 1, 2 - c * 2, 3 - c * 2)
            pick = jnp.concatenate([jnp.where(one_hot(meta[s, i], cap), 1.0, 0.0).astype(BF16) for i in ids], axis=0)
            vals = jnp.concatenate([r_own[chip, 0, lanes, :], r_own[chip, 1, lanes, :], r_recv[chip, 0, lanes, :], r_recv[chip, 1, lanes, :]], axis=0)
            part = dot_tn(pick, vals)
            u = d * 2 + h

            @pl.when(j % 2 == 0)
            def _():
                y_send[u] = part
                y_copy(u).start()

            @pl.when(j % 2 == 1)
            def _():
                tot[u] = part

    def step(j, _):
        @pl.when(j < 8)
        def _():
            make_rows(j)

        @pl.when(j > 0)
        def _():
            combine(j - 1)

        return 0

    lax.fori_loop(0, 9, step, 0)
    loads[4].wait()

    def w_out(i, slot):
        e, t = i // 4, i % 4
        rows = pl.ds(pl.multiple_of(t * og.shape[1], og.shape[1]), og.shape[1])
        return (pltpu.make_async_copy(og.at[slot], gwg_hbm.at[e, rows, :], st_sem.at[slot, 0]),
                pltpu.make_async_copy(ou.at[slot], gwu_hbm.at[e, rows, :], st_sem.at[slot, 1]))

    def weights(i):
        e, t = i // 4, i % 4
        slot = i % 2

        @pl.when(i >= 2)
        def _():
            for cp in w_out(i - 2, slot):
                cp.wait()

        xs = x[e, :, pl.ds(pl.multiple_of(t * og.shape[1], og.shape[1]), og.shape[1])]
        og[slot] = dot_tn(xs, dh1[e])
        ou[slot] = dot_tn(xs, dh3[e])
        for cp in w_out(i, slot):
            cp.start()

    def chain(i, _):
        weights(i)
        d, h = far_first(z, i // 2), i % 2
        u = d * 2 + h
        y_copy(u).wait_recv()
        tot[u] = tot[u] + y_recv[u]

        @pl.when((z <= d) & (z > 0))
        def _():
            to_right(u).wait_recv()
            tot[u] = tot[u] + z_left[u]

        @pl.when((z >= d) & (z < 3))
        def _():
            to_left(u).wait_recv()
            tot[u] = tot[u] + z_right[u]

        @pl.when(z < d)
        def _():
            to_right(u).start()

        @pl.when(z > d)
        def _():
            to_left(u).start()

        @pl.when((z == d) & (h == c))
        def _():
            for k in range(2):
                @pl.when(c == k)
                def _():
                    gx[:, k * half:(k + 1) * half] = tot[u].astype(BF16)

        @pl.when((z == d) & (h != c))
        def _():
            f_send[...] = tot[u].astype(BF16)
            last().start()

        return 0

    lax.fori_loop(0, 8, chain, 0)
    last().wait()
    for k in range(2):
        @pl.when(c == k)
        def _():
            gx[:, (1 - k) * half:(2 - k) * half] = f_recv[...]

    def drain(u, _):
        swap(u).wait_send()
        y_copy(u).wait_send()
        pl.when(z != u // 2)(to_right(u).wait_send)
        return 0

    lax.fori_loop(0, 8, drain, 0)
    for i in (6, 7):
        for cp in w_out(i, i % 2):
            cp.wait()


def routing_tables(gate_vals, topk_idx, slot_ids, pair_counts):
    n_exp = pair_counts.shape[1]
    hit = topk_idx[None] == lax.broadcasted_iota(jnp.int32, (n_exp, 1, 1), 0)
    slot = jnp.max(jnp.where(hit, slot_ids[None], -1), axis=2)
    gate = jnp.sum(jnp.where(hit, gate_vals[None], 0.0), axis=2)
    slot = jnp.where(slot < pair_counts.reshape(n_exp, 1), slot, -1)
    return slot, gate


def solution(mesh):
    rows_spec = P(("dp", "ep"), None)
    cube_spec = P(("dp", "ep"), None, None)
    weight_spec = P("ep", None, None)

    def local_step(grad_y, gate_vals, topk_idx, slot_ids, pair_counts, y_routed, x_disp, h_gate, h_up, w_gate, w_up, w_down):
        n_loc, n_rows, ffn = h_gate.shape
        tok, dim = grad_y.shape
        half = dim // 2
        cap = n_rows // 16
        shape = jax.ShapeDtypeStruct
        slot, gate = routing_tables(gate_vals, topk_idx, slot_ids, pair_counts)
        meta_out = jnp.concatenate([slot.astype(F32).reshape(8, 4, 1, tok), gate.reshape(8, 4, 1, tok)], axis=1)
        dh1, dh3, grad_wdown, meta = pl.pallas_call(
            gather_kernel,
            out_shape=(shape((n_loc, n_rows, ffn), BF16), shape((n_loc, n_rows, ffn), BF16), shape((n_loc, ffn, dim), F32), shape((16, 8, 1, tok), F32)),
            in_specs=[VM, VM, ANY, ANY, ANY],
            out_specs=(ANY, ANY, ANY, VM),
            scratch_shapes=[
                VMEM((16, tok, dim), BF16), VMEM((16, 8, 1, tok), F32),
                VMEM((n_loc, n_rows, ffn), BF16), VMEM((n_loc, n_rows, ffn), BF16), VMEM((n_loc, ffn, dim), BF16),
                VMEM((2 * cap, dim), BF16), VMEM((2 * cap, ffn), BF16),
                VMEM((n_loc, n_rows, ffn), BF16), VMEM((n_loc, n_rows, ffn), BF16), VMEM((n_loc, ffn, dim), F32),
                DMA((3,)), DMA((3,)), DMA((16, 4)), DMA((16,)), DMA((16,)), DMA((16,)),
            ],
            compiler_params=pltpu.CompilerParams(collective_id=1, has_side_effects=True, vmem_limit_bytes=56 << 20),
            name="gather_step",
        )(grad_y, meta_out, h_gate, h_up, w_down)
        grad_gate = jnp.einsum("td,tkd->tk", grad_y, y_routed, preferred_element_type=F32)
        unit = (8, tok, half)
        grad_x, grad_wgate, grad_wup = pl.pallas_call(
            return_kernel,
            out_shape=(shape((tok, dim), BF16), shape((n_loc, dim, ffn), F32), shape((n_loc, dim, ffn), F32)),
            in_specs=[VM, ANY, ANY, ANY, ANY, ANY],
            out_specs=(VM, ANY, ANY),
            scratch_shapes=[
                VMEM((n_loc, n_rows, ffn), BF16), VMEM((n_loc, n_rows, ffn), BF16),
                VMEM((n_loc, dim, ffn), BF16), VMEM((n_loc, dim, ffn), BF16), VMEM((n_loc, n_rows, dim), BF16),
                VMEM((8, n_loc, 2 * cap, half), BF16), VMEM((8, n_loc, 2 * cap, half), BF16), VMEM((8, n_loc, 2 * cap, half), BF16),
                VMEM(unit, F32), VMEM(unit, F32), VMEM(unit, F32), VMEM(unit, F32), VMEM(unit, F32),
                VMEM((tok, half), BF16), VMEM((tok, half), BF16),
                VMEM((2, 256, ffn), F32), VMEM((2, 256, ffn), F32),
                DMA((5,)), DMA((2, 2)), DMA((8,)), DMA((8,)), DMA((8,)), DMA((8,)), DMA((8,)), DMA((8,)), DMA((8,)), DMA((1,)), DMA((1,)),
            ],
            compiler_params=pltpu.CompilerParams(collective_id=2, has_side_effects=True, vmem_limit_bytes=67043328),
            name="return_step",
        )(meta, dh1, dh3, w_gate, w_up, x_disp)
        return grad_x, grad_gate, grad_wgate, grad_wup, grad_wdown

    return jax.shard_map(local_step, mesh=mesh, in_specs=(rows_spec, rows_spec, rows_spec, rows_spec, rows_spec, cube_spec, cube_spec, cube_spec, cube_spec, weight_spec, weight_spec, weight_spec), out_specs=(rows_spec, rows_spec, cube_spec, cube_spec, cube_spec), check_vma=False)
```

```python
import jax
import jax.numpy as jnp
from jax import lax
from jax.experimental import pallas as pl
from jax.experimental.pallas import tpu as pltpu
from jax.sharding import PartitionSpec as P

F32 = jnp.float32
BF16 = jnp.bfloat16
VMEM = pltpu.VMEM
DMA = pltpu.SemaphoreType.DMA
ANY = pl.BlockSpec(memory_space=pl.ANY)
VM = pl.BlockSpec(memory_space=pltpu.VMEM)


def position():
    me = lax.axis_index("ep")
    return me, me // 4, (me // 2) % 2, me % 2


def mirror(z, v):
    return v + (z // 2) * (3 - 2 * v)


def near_first(z, k):
    q = mirror(z, z)
    return mirror(z, (q, 1 - q, 2, 3)[k])


def dot_nt(a, b):
    return lax.dot_general(a, b, (((1,), (1,)), ((), ())), preferred_element_type=F32)


def dot_tn(a, b):
    return lax.dot_general(a, b, (((0,), (0,)), ((), ())), preferred_element_type=F32)


def one_hot(slot, cap):
    return slot == lax.broadcasted_iota(jnp.int32, (cap, slot.shape[1]), 0).astype(F32)


def step_kernel(gy, idx_t, slot_t, gate_t, counts, yr_hbm, hg_hbm, hu_hbm, wd_hbm, wg_hbm, wu_hbm, x_hbm, gx, gg, gwd_hbm, gwg_hbm, gwu_hbm,
                tok, meta, meta_out, hbuf, wd, wg, wu, xs, yr, d_ref, a_ref, dh1, dh3, acc, r_own, r_send, r_recv, tot, z_in, y_send, y_in, f_send, f_recv, og, ou,
                w_sem, h_sem, x_sem, g_sem, st_sem, acc_sem, send, recv, m_send, m_recv, rs, rr, ys, yrs, zs_sem, zr_sem, fs, fr):
    me, z, y, c = position()
    n_loc, n_rows, ffn = dh1.shape
    cap = n_rows // 16
    half = r_own.shape[3]
    n_exp = counts.shape[1]
    sib = me + 1 - 2 * c
    ynb = me + 2 - 4 * y
    m = z // 2
    q = mirror(z, z)
    way = 1 - 2 * m
    end = q == 0
    mid = q == 1
    up = (me + 4 * way + 16) % 16
    down = (me - 4 * way + 16) % 16

    order = ((0, 0), (1, 0), (0, 1), (2, 0), (1, 1), (3, 0), (2, 1), (3, 1))

    def chip_of(t):
        k, other = order[t]
        return near_first(z, k), y + other * (1 - 2 * y)

    def rows_of(chip):
        return pl.ds(pl.multiple_of(chip * 2 * cap, 2 * cap), 2 * cap)

    def h_loads(t):
        d, yy = chip_of(t)
        rows = rows_of(d * 2 + yy)
        return [pltpu.make_async_copy(src.at[:, rows, :], hbuf.at[t % 2, i], h_sem.at[t % 2, i]) for i, src in enumerate((hg_hbm, hu_hbm))]

    w_loads = [pltpu.make_async_copy(src, dst, w_sem.at[i]) for i, (src, dst) in enumerate(((wd_hbm, wd), (wg_hbm, wg), (wu_hbm, wu)))]
    for cp in h_loads(0) + w_loads:
        cp.start()

    def yr_load(i):
        return pltpu.make_async_copy(yr_hbm.at[pl.ds(pl.multiple_of(i * 256, 256), 256), :], yr.at[i % 2], g_sem.at[i % 2])

    yr_load(0).start()

    barrier = pltpu.get_barrier_semaphore()
    for k in range(1, 16):
        pl.semaphore_signal(barrier, inc=1, device_id={"ep": (me + k) % 16})

    idx, slots, gates = idx_t[...], slot_t[...], gate_t[...]
    for e in range(n_exp):
        hit = idx == e
        slot = jnp.max(jnp.where(hit, slots, -1), axis=0, keepdims=True)
        slot = jnp.where(slot < counts[0, e], slot, -1)
        meta_out[e // 4, e % 4] = slot.astype(F32)
        meta_out[e // 4, 4 + e % 4] = jnp.sum(jnp.where(hit, gates, 0.0), axis=0, keepdims=True)
    pl.semaphore_wait(barrier, 15)

    def put(src, slot, link, to):
        return pltpu.make_async_remote_copy(src_ref=src, dst_ref=tok.at[slot], send_sem=send.at[slot, link], recv_sem=recv.at[slot], device_id={"ep": to})

    def arrive(slot):
        put(tok.at[slot], slot, 0, me).wait_recv()

    def meta_copy(k):
        to = (me + k) % 16
        return pltpu.make_async_remote_copy(src_ref=meta_out.at[to // 2], dst_ref=meta.at[me], send_sem=m_send.at[k], recv_sem=m_recv.at[me], device_id={"ep": to})

    own = [(put(gy, me, 0, up), None), (put(gy, me, 1, down), mid), (put(gy, me, 2, ynb), None), (put(gy, me, 3, sib), None)]
    for cp, cond in own:
        cp.start() if cond is None else pl.when(cond)(cp.start)
    for k in range(1, 16):
        meta_copy(k).start()
    tok[me] = gy[...]
    meta[me] = meta_out[me // 2]
    acc[...] = jnp.zeros_like(acc)

    gg[...] = jnp.zeros_like(gg)

    def gate_block(i, _):
        yr_load(i).wait()

        @pl.when(i < 7)
        def _():
            yr_load(i + 1).start()

        base = pl.multiple_of((i // 4) * 128, 128)
        prod = dot_nt(yr[i % 2], gy[pl.ds(base, 128), :]).reshape(32, 8, 128)
        t = lax.broadcasted_iota(jnp.int32, prod.shape, 0) + (i % 4) * 32
        mine = t == lax.broadcasted_iota(jnp.int32, prod.shape, 2)
        gg[:, pl.ds(base, 128)] += jnp.sum(jnp.where(mine, prod, 0.0), axis=0)
        return 0

    lax.fori_loop(0, 8, gate_block, 0)
    for k in range(1, 16):
        src = (me + k) % 16
        pltpu.make_async_remote_copy(src_ref=meta_out.at[0], dst_ref=meta.at[src], send_sem=m_send.at[k], recv_sem=m_recv.at[src], device_id={"ep": src}).wait_recv()
    for cp in w_loads:
        cp.wait()

    def token_slot(k, ys_, cs):
        return near_first(z, k) * 4 + ys_ * 2 + cs

    def relay_to(k):
        zs = near_first(z, k)
        away = jnp.where(zs < z, 1, -1)
        nz = z + away
        return (me + 4 * away + 16) % 16, (nz >= 0) & (nz <= 3)

    def relay(k, cond=None):
        slot = token_slot(k, y, c)
        to, inside = relay_to(k)

        def body():
            arrive(slot)
            pl.when(inside)(put(tok.at[slot], slot, 0, to).start)
            put(tok.at[slot], slot, 2, ynb).start()
            put(tok.at[slot], slot, 3, sib).start()

        body() if cond is None else pl.when(cond)(body)

    def y_arrival(k):
        slot = token_slot(k, 1 - y, c)
        arrive(slot)
        put(tok.at[slot], slot, 3, sib).start()

    def z_slot(w, d, k, leftward, to_z):
        return jnp.where(leftward & (d == to_z), 12 + k, w)

    def z_copy(w, d, k, step):
        dst = z_slot(w, d, k, step < 0, z + step)
        return pltpu.make_async_remote_copy(src_ref=tot.at[w], dst_ref=z_in.at[dst], send_sem=zs_sem.at[w], recv_sem=zr_sem.at[dst], device_id={"ep": (me + 4 * step + 16) % 16})

    def z_add(w, d, k, step):
        src = z_slot(w, d, k, step < 0, z)
        pltpu.make_async_remote_copy(src_ref=tot.at[w], dst_ref=z_in.at[src], send_sem=zs_sem.at[w], recv_sem=zr_sem.at[src], device_id={"ep": me}).wait_recv()
        tot[w] = tot[w] + z_in[src]

    def y_copy(i, src):
        return pltpu.make_async_remote_copy(src_ref=src, dst_ref=y_in.at[i], send_sem=ys.at[i], recv_sem=yrs.at[i], device_id={"ep": ynb})

    def y_add(w, i):
        y_copy(i, y_send.at[0]).wait_recv()
        tot[w] = tot[w] + y_in[i]

    def unit0(dq, other):
        d = mirror(z, dq)
        yy = y + other * (1 - 2 * y)
        return d * 2 + yy, d, yy

    def unit1(dq):
        d = mirror(z, dq)
        return 8 + d, d, 2

    def start_up(unit):
        z_copy(*unit, way).start()

    def pass_up(unit):
        z_add(*unit, way)
        z_copy(*unit, way).start()

    def pass_down(unit):
        z_add(*unit, -way)
        z_copy(*unit, -way).start()

    def swap(chip, slot):
        return pltpu.make_async_remote_copy(src_ref=r_send.at[slot], dst_ref=r_recv.at[chip], send_sem=rs.at[chip], recv_sem=rr.at[chip], device_id={"ep": sib})

    def make(t, slot):
        d, yy = chip_of(t)
        chip = d * 2 + yy
        rows = rows_of(chip)
        for cp in h_loads(t):
            cp.wait()
        if t < 7:
            for cp in h_loads(t + 1):
                cp.start()

        def per_expert(e, _):
            for h in range(2):
                s = chip * 2 + h
                hot = one_hot(meta[s, c * 2 + e], cap)
                gate = jnp.sum(jnp.where(hot, meta[s, 4 + c * 2 + e], 0.0), axis=1, keepdims=True)
                picked = jnp.dot(jnp.where(hot, 1.0, 0.0).astype(BF16), tok[s], preferred_element_type=F32)
                d_ref[h * cap:(h + 1) * cap, :] = (picked * gate).astype(BF16)
            g = dot_nt(d_ref[...], wd[e]).astype(BF16).astype(F32)
            h1 = hbuf[t % 2, 0, e].astype(F32)
            h3 = hbuf[t % 2, 1, e].astype(F32)
            sig = jax.nn.sigmoid(h1)
            act = h1 * sig
            a_ref[...] = (act * h3).astype(BF16)
            dh1[e, rows, :] = (g * h3 * sig * (1.0 + h1 * (1.0 - sig))).astype(BF16)
            dh3[e, rows, :] = (g * act).astype(BF16)
            for part, dest in ((1 - c, r_send), (c, r_own)):
                cols = pl.ds(pl.multiple_of(part * half, half), half)
                r = dot_nt(dh1[e, rows, :], wg[e, cols, :]) + dot_nt(dh3[e, rows, :], wu[e, cols, :])
                dest[slot, e] = r.astype(BF16)
            acc[e] += dot_tn(a_ref[...], d_ref[...])
            return 0

        lax.fori_loop(0, n_loc, per_expert, 0)
        swap(chip, slot).start()

    def combine(t, slot):
        d, yy = chip_of(t)
        chip = d * 2 + yy
        cp = swap(chip, slot)
        cp.wait_recv()
        for h in range(2):
            s = chip * 2 + h
            lanes = pl.ds(h * cap, cap)
            ids = (c * 2, c * 2 + 1, 2 - c * 2, 3 - c * 2)
            pick = jnp.concatenate([jnp.where(one_hot(meta[s, i], cap), 1.0, 0.0).astype(BF16) for i in ids], axis=0)
            vals = jnp.concatenate([r_own[slot, 0, lanes, :], r_own[slot, 1, lanes, :], r_recv[chip, 0, lanes, :], r_recv[chip, 1, lanes, :]], axis=0)
            part = dot_tn(pick, vals)
            if h == 0:
                tot[d * 2 + yy] = part
            elif order[t][1] == 0:
                tot[8 + d] = part
            else:
                y_send[d] = part
        cp.wait_send()

    def y_start(dq):
        d = mirror(z, dq)
        y_copy(d, y_send.at[d]).start()

    arrive(token_slot(0, y, 1 - c))
    make(0, 0)
    combine(0, 0)
    for phase in range(1, 5):
        if phase == 1:
            relay(1)
            relay(2, mid)
        elif phase == 2:
            relay(2, end)
            relay(3, mid)
        elif phase == 3:
            relay(3, end)
        if phase < 4:
            arrive(token_slot(phase, y, 1 - c))
            make(2 * phase - 1, 0)
        y_arrival(phase - 1)
        if phase < 4:
            combine(2 * phase - 1, 0)
            pl.when(end)(lambda phase=phase: start_up(unit0(phase, 0)))
        arrive(token_slot(phase - 1, 1 - y, 1 - c))
        make(2 * phase if phase < 4 else 7, 1)
        combine(2 * phase if phase < 4 else 7, 1)
        if phase == 3:
            @pl.when(end)
            def _():
                start_up(unit0(2, 1))
                y_start(2)

            @pl.when(mid)
            def _():
                y_start(0)
                pass_up(unit0(2, 0))
        if phase == 4:
            y_start(3)

            @pl.when(end)
            def _():
                start_up(unit0(3, 1))
                y_start(1)
                y_start(0)

            @pl.when(mid)
            def _():
                y_start(2)
                y_start(1)
                pass_up(unit0(3, 0))

    width = xs.shape[2]

    def x_load(i):
        e, t = i // 4, i % 4
        return pltpu.make_async_copy(x_hbm.at[e, :, pl.ds(pl.multiple_of(t * width, width), width)], xs.at[i % 2], x_sem.at[i % 2])

    def w_out(i):
        e, t = i // 4, i % 4
        rows = pl.ds(pl.multiple_of(t * width, width), width)
        return (pltpu.make_async_copy(og.at[i % 2], gwg_hbm.at[e, rows, :], st_sem.at[i % 2, 0]),
                pltpu.make_async_copy(ou.at[i % 2], gwu_hbm.at[e, rows, :], st_sem.at[i % 2, 1]))

    def through_y(dq, go):
        unit = unit1(dq)
        y_add(unit[0], unit[1])
        go(unit)

    mid_events = (
        lambda: pass_up(unit0(2, 1)),
        lambda: pass_down(unit0(0, 0)),
        lambda: pass_up(unit0(3, 1)),
        lambda: through_y(3, pass_up),
        lambda: pass_down(unit0(0, 1)),
        lambda: through_y(2, pass_up),
        lambda: through_y(0, pass_down),
    )
    end_events = (
        None,
        lambda: through_y(3, start_up),
        lambda: through_y(2, start_up),
        lambda: start_up(unit0(1, 1)),
        lambda: through_y(1, start_up),
    )
    x_load(0).start()
    acc_out = pltpu.make_async_copy(acc, gwd_hbm, acc_sem.at[0])
    acc_out.start()

    def weights(i, _):
        x_load(i).wait()

        @pl.when(i < 7)
        def _():
            x_load(i + 1).start()

        @pl.when(i >= 2)
        def _():
            for cp in w_out(i - 2):
                cp.wait()

        e = i // 4
        og[i % 2] = dot_tn(xs[i % 2], dh1[e])
        ou[i % 2] = dot_tn(xs[i % 2], dh3[e])
        for cp in w_out(i):
            cp.start()
        for n, event in enumerate(mid_events):
            pl.when(mid & (i == n))(event)
        for n, event in enumerate(end_events):
            if event is not None:
                pl.when(end & (i == n))(event)
        return 0

    lax.fori_loop(0, 8, weights, 0)

    def finish(unit):
        z_add(*unit, -way)
        pl.when(mid)(lambda: z_add(*unit, way))

    own0, cross0, own1 = unit0(q, 0), unit0(q, 1), unit1(q)

    def last():
        return pltpu.make_async_remote_copy(src_ref=f_send, dst_ref=f_recv, send_sem=fs.at[0], recv_sem=fr.at[0], device_id={"ep": sib})

    def deliver(w, h):
        @pl.when(c == h)
        def _():
            gx[:, h * half:(h + 1) * half] = tot[w].astype(BF16)

        @pl.when(c != h)
        def _():
            f_send[...] = tot[w].astype(BF16)
            last().start()

    finish(own0)
    finish(cross0)
    y_copy(4, tot.at[cross0[0]]).start()
    y_add(own1[0], own1[1])
    finish(own1)
    deliver(own1[0], 1)
    y_add(own0[0], 4)
    deliver(own0[0], 0)
    last().wait()
    for h in range(2):
        @pl.when(c == h)
        def _():
            gx[:, (1 - h) * half:(2 - h) * half] = f_recv[...]

    for cp, cond in own:
        cp.wait_send() if cond is None else pl.when(cond)(cp.wait_send)
    for k in range(1, 4):
        slot = token_slot(k, y, c)
        pl.when(relay_to(k)[1])(put(tok.at[slot], slot, 0, me).wait_send)
        put(tok.at[slot], slot, 2, ynb).wait_send()
        put(tok.at[slot], slot, 3, sib).wait_send()
    for k in range(4):
        slot = token_slot(k, 1 - y, c)
        put(tok.at[slot], slot, 3, sib).wait_send()
    for k in range(1, 16):
        meta_copy(k).wait_send()
    for d in range(4):
        y_copy(d, y_send.at[d]).wait_send()
    y_copy(4, tot.at[cross0[0]]).wait_send()

    def z_drain(w, d):
        pl.when(d != z)(pltpu.make_async_remote_copy(src_ref=tot.at[w], dst_ref=z_in.at[w], send_sem=zs_sem.at[w], recv_sem=zr_sem.at[w], device_id={"ep": me}).wait_send)

    for w in range(8):
        z_drain(w, w // 2)
    for d in range(4):
        z_drain(8 + d, d)
    for i in (6, 7):
        for cp in w_out(i):
            cp.wait()
    acc_out.wait()


def solution(mesh):
    rows_spec = P(("dp", "ep"), None)
    cube_spec = P(("dp", "ep"), None, None)
    weight_spec = P("ep", None, None)

    def local_step(grad_y, gate_vals, topk_idx, slot_ids, pair_counts, y_routed, x_disp, h_gate, h_up, w_gate, w_up, w_down):
        n_loc, n_rows, ffn = h_gate.shape
        tok, dim = grad_y.shape
        top_k = topk_idx.shape[1]
        half = dim // 2
        cap = n_rows // 16
        shape = jax.ShapeDtypeStruct
        grad_x, grad_gate, grad_wdown, grad_wgate, grad_wup = pl.pallas_call(
            step_kernel,
            out_shape=(shape((tok, dim), BF16), shape((top_k, tok), F32), shape((n_loc, ffn, dim), F32), shape((n_loc, dim, ffn), F32), shape((n_loc, dim, ffn), F32)),
            in_specs=[VM, VM, VM, VM, pl.BlockSpec(memory_space=pltpu.SMEM)] + [ANY] * 7,
            out_specs=(VM, VM, ANY, ANY, ANY),
            scratch_shapes=[
                VMEM((16, tok, dim), BF16), VMEM((16, 8, 1, tok), F32), VMEM((8, 8, 1, tok), F32),
                VMEM((2, 2, n_loc, 2 * cap, ffn), BF16),
                VMEM((n_loc, ffn, dim), BF16), VMEM((n_loc, dim, ffn), BF16), VMEM((n_loc, dim, ffn), BF16),
                VMEM((2, n_rows, 256), BF16), VMEM((2, 256, dim), BF16),
                VMEM((2 * cap, dim), BF16), VMEM((2 * cap, ffn), BF16),
                VMEM((n_loc, n_rows, ffn), BF16), VMEM((n_loc, n_rows, ffn), BF16), VMEM((n_loc, ffn, dim), F32),
                VMEM((2, n_loc, 2 * cap, half), BF16), VMEM((2, n_loc, 2 * cap, half), BF16), VMEM((8, n_loc, 2 * cap, half), BF16),
                VMEM((12, tok, half), F32), VMEM((15, tok, half), F32), VMEM((4, tok, half), F32), VMEM((5, tok, half), F32),
                VMEM((tok, half), BF16), VMEM((tok, half), BF16),
                VMEM((2, 256, ffn), F32), VMEM((2, 256, ffn), F32),
                DMA((3,)), DMA((2, 2)), DMA((2,)), DMA((2,)), DMA((2, 2)), DMA((1,)),
                DMA((16, 4)), DMA((16,)), DMA((16,)), DMA((16,)), DMA((8,)), DMA((8,)), DMA((5,)), DMA((5,)), DMA((12,)), DMA((15,)), DMA((1,)), DMA((1,)),
            ],
            compiler_params=pltpu.CompilerParams(collective_id=1, has_side_effects=True, vmem_limit_bytes=67043328),
            name="step",
        )(grad_y, topk_idx.T, slot_ids.T, gate_vals.T, pair_counts, y_routed.reshape(tok * top_k, dim), h_gate, h_up, w_down, w_gate, w_up, x_disp)
        return grad_x, grad_gate.T, grad_wgate, grad_wup, grad_wdown

    return jax.shard_map(local_step, mesh=mesh, in_specs=(rows_spec, rows_spec, rows_spec, rows_spec, rows_spec, cube_spec, cube_spec, cube_spec, cube_spec, weight_spec, weight_spec, weight_spec), out_specs=(rows_spec, rows_spec, cube_spec, cube_spec, cube_spec), check_vma=False)
```

```python
import jax
import jax.numpy as jnp
from jax import lax
from jax.experimental import pallas as pl
from jax.experimental.pallas import tpu as pltpu
from jax.sharding import PartitionSpec as P

F32 = jnp.float32
BF16 = jnp.bfloat16
VMEM = pltpu.VMEM
DMA = pltpu.SemaphoreType.DMA
ANY = pl.BlockSpec(memory_space=pl.ANY)
VM = pl.BlockSpec(memory_space=pltpu.VMEM)


def position():
    me = lax.axis_index("ep")
    return me, me // 4, (me // 2) % 2, me % 2


def mirror(z, v):
    return v + (z // 2) * (3 - 2 * v)


def near_first(z, k):
    q = mirror(z, z)
    return mirror(z, (q, 1 - q, 2, 3)[k])


def dot_nt(a, b):
    return lax.dot_general(a, b, (((1,), (1,)), ((), ())), preferred_element_type=F32)


def dot_tn(a, b):
    return lax.dot_general(a, b, (((0,), (0,)), ((), ())), preferred_element_type=F32)


def one_hot(slot, cap):
    return slot == lax.broadcasted_iota(jnp.int32, (cap, slot.shape[1]), 0).astype(F32)


def step_kernel(gy, idx_t, slot_t, gate_t, counts, yr_hbm, hg_hbm, hu_hbm, wd_hbm, wg_hbm, wu_hbm, x_hbm, gx, gg, gwd_hbm, gwg_hbm, gwu_hbm,
                tok, meta, meta_out, hbuf, wd, wg, wu, xs, yr, d_ref, a_ref, dh1, dh3, acc, r_own, r_send, r_recv, tot, z_in, y_send, y_in, f_send, f_recv, og, ou,
                w_sem, h_sem, x_sem, g_sem, st_sem, acc_sem, send, recv, m_send, m_recv, rs, rr, ys, yrs, zs_sem, zr_sem, fs, fr):
    me, z, y, c = position()
    n_loc, n_rows, ffn = dh1.shape
    cap = n_rows // 16
    half = r_own.shape[3]
    n_exp = counts.shape[1]
    sib = me + 1 - 2 * c
    ynb = me + 2 - 4 * y
    m = z // 2
    q = mirror(z, z)
    way = 1 - 2 * m
    end = q == 0
    mid = q == 1
    up = (me + 4 * way + 16) % 16
    down = (me - 4 * way + 16) % 16

    order = ((0, 0), (1, 0), (0, 1), (2, 0), (1, 1), (3, 0), (2, 1), (3, 1))

    def chip_of(t):
        k, other = order[t]
        return near_first(z, k), y + other * (1 - 2 * y)

    def rows_of(chip):
        return pl.ds(pl.multiple_of(chip * 2 * cap, 2 * cap), 2 * cap)

    def h_loads(t):
        d, yy = chip_of(t)
        rows = rows_of(d * 2 + yy)
        return [pltpu.make_async_copy(src.at[:, rows, :], hbuf.at[t % 2, i], h_sem.at[t % 2, i]) for i, src in enumerate((hg_hbm, hu_hbm))]

    w_loads = [pltpu.make_async_copy(src, dst, w_sem.at[i]) for i, (src, dst) in enumerate(((wd_hbm, wd), (wg_hbm, wg), (wu_hbm, wu)))]
    for cp in h_loads(0) + w_loads:
        cp.start()

    def yr_load(i):
        return pltpu.make_async_copy(yr_hbm.at[pl.ds(pl.multiple_of(i * 256, 256), 256), :], yr.at[i % 2], g_sem.at[i % 2])

    yr_load(0).start()

    barrier = pltpu.get_barrier_semaphore()
    for k in range(1, 16):
        pl.semaphore_signal(barrier, inc=1, device_id={"ep": (me + k) % 16})

    idx, slots, gates = idx_t[...], slot_t[...], gate_t[...]
    for e in range(n_exp):
        hit = idx == e
        slot = jnp.max(jnp.where(hit, slots, -1), axis=0, keepdims=True)
        slot = jnp.where(slot < counts[0, e], slot, -1)
        meta_out[e // 4, e % 4] = slot.astype(F32)
        meta_out[e // 4, 4 + e % 4] = jnp.sum(jnp.where(hit, gates, 0.0), axis=0, keepdims=True)
    pl.semaphore_wait(barrier, 15)

    def put(src, slot, link, to):
        return pltpu.make_async_remote_copy(src_ref=src, dst_ref=tok.at[slot], send_sem=send.at[slot, link], recv_sem=recv.at[slot], device_id={"ep": to})

    def arrive(slot):
        put(tok.at[slot], slot, 0, me).wait_recv()

    def meta_copy(k):
        to = (me + k) % 16
        return pltpu.make_async_remote_copy(src_ref=meta_out.at[to // 2], dst_ref=meta.at[me], send_sem=m_send.at[k], recv_sem=m_recv.at[me], device_id={"ep": to})

    own = [(put(gy, me, 0, up), None), (put(gy, me, 1, down), mid), (put(gy, me, 2, ynb), None), (put(gy, me, 3, sib), None)]
    for cp, cond in own:
        cp.start() if cond is None else pl.when(cond)(cp.start)
    for k in range(1, 16):
        meta_copy(k).start()
    tok[me] = gy[...]
    meta[me] = meta_out[me // 2]
    acc[...] = jnp.zeros_like(acc)

    gg[...] = jnp.zeros_like(gg)

    def gate_block(i, _):
        yr_load(i).wait()

        @pl.when(i < 7)
        def _():
            yr_load(i + 1).start()

        base = pl.multiple_of((i // 4) * 128, 128)
        prod = dot_nt(yr[i % 2], gy[pl.ds(base, 128), :]).reshape(32, 8, 128)
        t = lax.broadcasted_iota(jnp.int32, prod.shape, 0) + (i % 4) * 32
        mine = t == lax.broadcasted_iota(jnp.int32, prod.shape, 2)
        gg[:, pl.ds(base, 128)] += jnp.sum(jnp.where(mine, prod, 0.0), axis=0)
        return 0

    lax.fori_loop(0, 8, gate_block, 0)
    for k in range(1, 16):
        src = (me + k) % 16
        pltpu.make_async_remote_copy(src_ref=meta_out.at[0], dst_ref=meta.at[src], send_sem=m_send.at[k], recv_sem=m_recv.at[src], device_id={"ep": src}).wait_recv()
    for cp in w_loads:
        cp.wait()

    def token_slot(k, ys_, cs):
        return near_first(z, k) * 4 + ys_ * 2 + cs

    def relay_to(k):
        zs = near_first(z, k)
        away = jnp.where(zs < z, 1, -1)
        nz = z + away
        return (me + 4 * away + 16) % 16, (nz >= 0) & (nz <= 3)

    def relay(k, cond=None):
        slot = token_slot(k, y, c)
        to, inside = relay_to(k)

        def body():
            arrive(slot)
            pl.when(inside)(put(tok.at[slot], slot, 0, to).start)
            put(tok.at[slot], slot, 2, ynb).start()
            put(tok.at[slot], slot, 3, sib).start()

        body() if cond is None else pl.when(cond)(body)

    def y_arrival(k):
        slot = token_slot(k, 1 - y, c)
        arrive(slot)
        put(tok.at[slot], slot, 3, sib).start()

    def z_slot(w, d, k, leftward, to_z):
        return jnp.where(leftward & (d == to_z), 12 + k, w)

    def z_copy(w, d, k, step):
        dst = z_slot(w, d, k, step < 0, z + step)
        return pltpu.make_async_remote_copy(src_ref=tot.at[w], dst_ref=z_in.at[dst], send_sem=zs_sem.at[w], recv_sem=zr_sem.at[dst], device_id={"ep": (me + 4 * step + 16) % 16})

    def z_add(w, d, k, step):
        src = z_slot(w, d, k, step < 0, z)
        pltpu.make_async_remote_copy(src_ref=tot.at[w], dst_ref=z_in.at[src], send_sem=zs_sem.at[w], recv_sem=zr_sem.at[src], device_id={"ep": me}).wait_recv()
        tot[w] = tot[w] + z_in[src]

    def y_copy(i, src):
        return pltpu.make_async_remote_copy(src_ref=src, dst_ref=y_in.at[i], send_sem=ys.at[i], recv_sem=yrs.at[i], device_id={"ep": ynb})

    def y_add(w, i):
        y_copy(i, y_send.at[0]).wait_recv()
        tot[w] = tot[w] + y_in[i]

    def unit0(dq, other):
        d = mirror(z, dq)
        yy = y + other * (1 - 2 * y)
        return d * 2 + yy, d, yy

    def unit1(dq):
        d = mirror(z, dq)
        return 8 + d, d, 2

    def start_up(unit):
        z_copy(*unit, way).start()

    def pass_up(unit):
        z_add(*unit, way)
        z_copy(*unit, way).start()

    def pass_down(unit):
        z_add(*unit, -way)
        z_copy(*unit, -way).start()

    def swap(chip, slot):
        return pltpu.make_async_remote_copy(src_ref=r_send.at[slot], dst_ref=r_recv.at[chip], send_sem=rs.at[chip], recv_sem=rr.at[chip], device_id={"ep": sib})

    def make(t, slot):
        d, yy = chip_of(t)
        chip = d * 2 + yy
        rows = rows_of(chip)
        for cp in h_loads(t):
            cp.wait()
        if t < 7:
            for cp in h_loads(t + 1):
                cp.start()

        def per_expert(e, _):
            for h in range(2):
                s = chip * 2 + h
                hot = one_hot(meta[s, c * 2 + e], cap)
                gate = jnp.sum(jnp.where(hot, meta[s, 4 + c * 2 + e], 0.0), axis=1, keepdims=True)
                picked = jnp.dot(jnp.where(hot, 1.0, 0.0).astype(BF16), tok[s], preferred_element_type=F32)
                d_ref[h * cap:(h + 1) * cap, :] = (picked * gate).astype(BF16)
            g = dot_nt(d_ref[...], wd[e]).astype(BF16).astype(F32)
            h1 = hbuf[t % 2, 0, e].astype(F32)
            h3 = hbuf[t % 2, 1, e].astype(F32)
            sig = jax.nn.sigmoid(h1)
            act = h1 * sig
            a_ref[...] = (act * h3).astype(BF16)
            dh1[e, rows, :] = (g * h3 * sig * (1.0 + h1 * (1.0 - sig))).astype(BF16)
            dh3[e, rows, :] = (g * act).astype(BF16)
            for part, dest in ((1 - c, r_send), (c, r_own)):
                cols = pl.ds(pl.multiple_of(part * half, half), half)
                r = dot_nt(dh1[e, rows, :], wg[e, cols, :]) + dot_nt(dh3[e, rows, :], wu[e, cols, :])
                dest[slot, e] = r.astype(BF16)
            acc[e] += dot_tn(a_ref[...], d_ref[...])
            return 0

        lax.fori_loop(0, n_loc, per_expert, 0)
        swap(chip, slot).start()

    def combine(t, slot):
        d, yy = chip_of(t)
        chip = d * 2 + yy
        cp = swap(chip, slot)
        cp.wait_recv()
        for h in range(2):
            s = chip * 2 + h
            lanes = pl.ds(h * cap, cap)
            ids = (c * 2, c * 2 + 1, 2 - c * 2, 3 - c * 2)
            pick = jnp.concatenate([jnp.where(one_hot(meta[s, i], cap), 1.0, 0.0).astype(BF16) for i in ids], axis=0)
            vals = jnp.concatenate([r_own[slot, 0, lanes, :], r_own[slot, 1, lanes, :], r_recv[chip, 0, lanes, :], r_recv[chip, 1, lanes, :]], axis=0)
            part = dot_tn(pick, vals)
            if h == 0:
                tot[d * 2 + yy] = part
            elif order[t][1] == 0:
                tot[8 + d] = part
            else:
                y_send[d] = part
        cp.wait_send()

    def y_start(dq):
        d = mirror(z, dq)
        y_copy(d, y_send.at[d]).start()

    arrive(token_slot(0, y, 1 - c))
    make(0, 0)
    combine(0, 0)
    for phase in range(1, 5):
        if phase == 1:
            relay(1)
            relay(2, mid)
        elif phase == 2:
            relay(2, end)
            relay(3, mid)
        elif phase == 3:
            relay(3, end)
        if phase < 4:
            arrive(token_slot(phase, y, 1 - c))
            make(2 * phase - 1, 0)
        y_arrival(phase - 1)
        if phase < 4:
            combine(2 * phase - 1, 0)
            pl.when(end)(lambda phase=phase: start_up(unit0(phase, 0)))
        arrive(token_slot(phase - 1, 1 - y, 1 - c))
        make(2 * phase if phase < 4 else 7, 1)
        combine(2 * phase if phase < 4 else 7, 1)
        if phase == 3:
            @pl.when(end)
            def _():
                start_up(unit0(2, 1))
                y_start(2)

            @pl.when(mid)
            def _():
                y_start(0)
                pass_up(unit0(2, 0))
        if phase == 4:
            y_start(3)

            @pl.when(end)
            def _():
                start_up(unit0(3, 1))
                y_start(1)
                y_start(0)

            @pl.when(mid)
            def _():
                y_start(2)
                y_start(1)
                pass_up(unit0(3, 0))

    width = xs.shape[2]

    def x_load(i):
        e, t = i // 4, i % 4
        return pltpu.make_async_copy(x_hbm.at[e, :, pl.ds(pl.multiple_of(t * width, width), width)], xs.at[i % 2], x_sem.at[i % 2])

    def w_out(i):
        e, t = i // 4, i % 4
        rows = pl.ds(pl.multiple_of(t * width, width), width)
        return (pltpu.make_async_copy(og.at[i % 2], gwg_hbm.at[e, rows, :], st_sem.at[i % 2, 0]),
                pltpu.make_async_copy(ou.at[i % 2], gwu_hbm.at[e, rows, :], st_sem.at[i % 2, 1]))

    def through_y(dq, go):
        unit = unit1(dq)
        y_add(unit[0], unit[1])
        go(unit)

    mid_events = (
        lambda: pass_up(unit0(2, 1)),
        lambda: pass_down(unit0(0, 0)),
        lambda: pass_up(unit0(3, 1)),
        lambda: through_y(3, pass_up),
        lambda: pass_down(unit0(0, 1)),
        lambda: through_y(2, pass_up),
        lambda: through_y(0, pass_down),
    )
    end_events = (
        None,
        lambda: through_y(3, start_up),
        lambda: through_y(2, start_up),
        lambda: start_up(unit0(1, 1)),
        lambda: through_y(1, start_up),
    )
    x_load(0).start()
    acc_out = pltpu.make_async_copy(acc, gwd_hbm, acc_sem.at[0])
    acc_out.start()

    def weights(i, _):
        x_load(i).wait()

        @pl.when(i < 7)
        def _():
            x_load(i + 1).start()

        @pl.when(i >= 2)
        def _():
            for cp in w_out(i - 2):
                cp.wait()

        e = i // 4
        og[i % 2] = dot_tn(xs[i % 2], dh1[e])
        ou[i % 2] = dot_tn(xs[i % 2], dh3[e])
        for cp in w_out(i):
            cp.start()
        for n, event in enumerate(mid_events):
            pl.when(mid & (i == n))(event)
        for n, event in enumerate(end_events):
            if event is not None:
                pl.when(end & (i == n))(event)
        return 0

    lax.fori_loop(0, 8, weights, 0)

    def finish(unit):
        z_add(*unit, -way)
        pl.when(mid)(lambda: z_add(*unit, way))

    own0, cross0, own1 = unit0(q, 0), unit0(q, 1), unit1(q)

    def last():
        return pltpu.make_async_remote_copy(src_ref=f_send, dst_ref=f_recv, send_sem=fs.at[0], recv_sem=fr.at[0], device_id={"ep": sib})

    def deliver(w, h):
        @pl.when(c == h)
        def _():
            gx[:, h * half:(h + 1) * half] = tot[w].astype(BF16)

        @pl.when(c != h)
        def _():
            f_send[...] = tot[w].astype(BF16)
            last().start()

    finish(own0)
    finish(cross0)
    y_copy(4, tot.at[cross0[0]]).start()
    y_add(own1[0], own1[1])
    finish(own1)
    deliver(own1[0], 1)
    y_add(own0[0], 4)
    deliver(own0[0], 0)
    last().wait()
    for h in range(2):
        @pl.when(c == h)
        def _():
            gx[:, (1 - h) * half:(2 - h) * half] = f_recv[...]

    for cp, cond in own:
        cp.wait_send() if cond is None else pl.when(cond)(cp.wait_send)
    for k in range(1, 4):
        slot = token_slot(k, y, c)
        pl.when(relay_to(k)[1])(put(tok.at[slot], slot, 0, me).wait_send)
        put(tok.at[slot], slot, 2, ynb).wait_send()
        put(tok.at[slot], slot, 3, sib).wait_send()
    for k in range(4):
        slot = token_slot(k, 1 - y, c)
        put(tok.at[slot], slot, 3, sib).wait_send()
    for k in range(1, 16):
        meta_copy(k).wait_send()
    for d in range(4):
        y_copy(d, y_send.at[d]).wait_send()
    y_copy(4, tot.at[cross0[0]]).wait_send()

    def z_drain(w, d):
        pl.when(d != z)(pltpu.make_async_remote_copy(src_ref=tot.at[w], dst_ref=z_in.at[w], send_sem=zs_sem.at[w], recv_sem=zr_sem.at[w], device_id={"ep": me}).wait_send)

    for w in range(8):
        z_drain(w, w // 2)
    for d in range(4):
        z_drain(8 + d, d)
    for i in (6, 7):
        for cp in w_out(i):
            cp.wait()
    acc_out.wait()


def deliver_kernel(*refs):
    n = (len(refs) - 2) // 3
    src, dst, buf, (in_sem, out_sem) = refs[:n], refs[n:2 * n], refs[2 * n:3 * n], refs[3 * n:]
    pieces = []
    for s, d, b in zip(src, dst, buf):
        rows = s.shape[-2]
        parts = 2 if len(s.shape) == 3 else 1
        for lead in ([(e,) for e in range(s.shape[0])] if len(s.shape) == 3 else [()]):
            for k in range(parts):
                at = lead + (pl.ds(k * rows // parts, rows // parts),)
                i = len(pieces)
                pieces.append((pltpu.make_async_copy(s.at[at], b.at[at], in_sem.at[i]), pltpu.make_async_copy(b.at[at], d.at[at], out_sem.at[i])))
    for read, _ in pieces:
        read.start()
    for read, write in pieces:
        read.wait()
        write.start()
    for _, write in pieces:
        write.wait()


def deliver(arrays):
    n = 2 + 4 * (len(arrays) - 2)
    return pl.pallas_call(
        deliver_kernel,
        out_shape=tuple(jax.ShapeDtypeStruct(a.shape, a.dtype) for a in arrays),
        in_specs=[ANY] * len(arrays),
        out_specs=(ANY,) * len(arrays),
        scratch_shapes=[VMEM(a.shape, a.dtype) for a in arrays] + [DMA((n,)), DMA((n,))],
        compiler_params=pltpu.CompilerParams(vmem_limit_bytes=67043328),
        name="deliver",
    )(*arrays)


def solution(mesh):
    rows_spec = P(("dp", "ep"), None)
    cube_spec = P(("dp", "ep"), None, None)
    weight_spec = P("ep", None, None)

    def local_step(grad_y, gate_vals, topk_idx, slot_ids, pair_counts, y_routed, x_disp, h_gate, h_up, w_gate, w_up, w_down):
        n_loc, n_rows, ffn = h_gate.shape
        tok, dim = grad_y.shape
        top_k = topk_idx.shape[1]
        half = dim // 2
        cap = n_rows // 16
        shape = jax.ShapeDtypeStruct
        grad_x, grad_gate, grad_wdown, grad_wgate, grad_wup = pl.pallas_call(
            step_kernel,
            out_shape=(shape((tok, dim), BF16), shape((top_k, tok), F32), shape((n_loc, ffn, dim), F32), shape((n_loc, dim, ffn), F32), shape((n_loc, dim, ffn), F32)),
            in_specs=[VM, VM, VM, VM, pl.BlockSpec(memory_space=pltpu.SMEM)] + [ANY] * 7,
            out_specs=(VM, VM, ANY, ANY, ANY),
            scratch_shapes=[
                VMEM((16, tok, dim), BF16), VMEM((16, 8, 1, tok), F32), VMEM((8, 8, 1, tok), F32),
                VMEM((2, 2, n_loc, 2 * cap, ffn), BF16),
                VMEM((n_loc, ffn, dim), BF16), VMEM((n_loc, dim, ffn), BF16), VMEM((n_loc, dim, ffn), BF16),
                VMEM((2, n_rows, 256), BF16), VMEM((2, 256, dim), BF16),
                VMEM((2 * cap, dim), BF16), VMEM((2 * cap, ffn), BF16),
                VMEM((n_loc, n_rows, ffn), BF16), VMEM((n_loc, n_rows, ffn), BF16), VMEM((n_loc, ffn, dim), F32),
                VMEM((2, n_loc, 2 * cap, half), BF16), VMEM((2, n_loc, 2 * cap, half), BF16), VMEM((8, n_loc, 2 * cap, half), BF16),
                VMEM((12, tok, half), F32), VMEM((15, tok, half), F32), VMEM((4, tok, half), F32), VMEM((5, tok, half), F32),
                VMEM((tok, half), BF16), VMEM((tok, half), BF16),
                VMEM((2, 256, ffn), F32), VMEM((2, 256, ffn), F32),
                DMA((3,)), DMA((2, 2)), DMA((2,)), DMA((2,)), DMA((2, 2)), DMA((1,)),
                DMA((16, 4)), DMA((16,)), DMA((16,)), DMA((16,)), DMA((8,)), DMA((8,)), DMA((5,)), DMA((5,)), DMA((12,)), DMA((15,)), DMA((1,)), DMA((1,)),
            ],
            compiler_params=pltpu.CompilerParams(collective_id=1, has_side_effects=True, vmem_limit_bytes=67043328),
            name="step",
        )(grad_y, topk_idx.T, slot_ids.T, gate_vals.T, pair_counts, y_routed.reshape(tok * top_k, dim), h_gate, h_up, w_down, w_gate, w_up, x_disp)
        grad_wgate, grad_wup, grad_wdown, grad_x, grad_gate = deliver((grad_wgate, grad_wup, grad_wdown, grad_x, grad_gate))
        return grad_x, grad_gate.T, grad_wgate, grad_wup, grad_wdown

    return jax.shard_map(local_step, mesh=mesh, in_specs=(rows_spec, rows_spec, rows_spec, rows_spec, rows_spec, cube_spec, cube_spec, cube_spec, cube_spec, weight_spec, weight_spec, weight_spec), out_specs=(rows_spec, rows_spec, cube_spec, cube_spec, cube_spec), check_vma=False)
```

```python
import jax
import jax.numpy as jnp
from jax import lax
from jax.experimental import pallas as pl
from jax.experimental.pallas import tpu as pltpu
from jax.sharding import PartitionSpec as P

F32 = jnp.float32
BF16 = jnp.bfloat16
VMEM = pltpu.VMEM
DMA = pltpu.SemaphoreType.DMA
Z0, Z1, Z2, Z3 = range(4)
OWN, OTHER = CORE0, CORE1 = LO, HI = CORES = HALVES = range(2)
ONWARD, DOWN, CROSS, CORE = range(4)
NZ, GROUP = 4, 16
PEERS = range(1, GROUP)
ANY = pl.BlockSpec(memory_space=pl.ANY)
VM = pl.BlockSpec(memory_space=pltpu.VMEM)


def position():
    me = lax.axis_index("ep")
    return me, me // 4, (me // 2) % 2, me % 2


def mirror(z, v):
    return v + (z // 2) * (3 - 2 * v)


def dot_nt(a, b):
    return lax.dot_general(a, b, (((1,), (1,)), ((), ())), preferred_element_type=F32)


def dot_tn(a, b):
    return lax.dot_general(a, b, (((0,), (0,)), ((), ())), preferred_element_type=F32)


def one_hot(slot, cap):
    return slot == lax.broadcasted_iota(jnp.int32, (cap, slot.shape[1]), 0).astype(F32)


def step_kernel(gy, idx_t, slot_t, gate_t, counts, yr_hbm, hg_hbm, hu_hbm, wd_hbm, wg_hbm, wu_hbm, x_hbm, gx, gg, gwd_hbm, gwg_hbm, gwu_hbm,
                tok, meta, meta_out, hbuf, wd, wg, wu, xs, yr, d_ref, a_ref, dh1, dh3, acc, r_own, r_send, r_recv, tot, z_in, y_in, f_send, f_recv, og, ou,
                w_sem, h_sem, x_sem, g_sem, st_sem, acc_sem, send, recv, m_send, m_recv, rs, rr, ys, yrs, zs_sem, zr_sem, fs, fr):
    me, z, y, c = position()
    n_loc, n_rows, ffn = dh1.shape
    cap = n_rows // 16
    half = r_own.shape[3]
    n_exp = counts.shape[1]
    sib = me + 1 - 2 * c
    ynb = me + 2 - 4 * y
    m = z // 2
    q = mirror(z, z)
    way = 1 - 2 * m
    end = q == 0
    mid = q == 1
    up = (me + 4 * way + GROUP) % GROUP
    down = (me - 4 * way + GROUP) % GROUP

    order = (((Z0, OWN), (Z1, OWN)), ((Z0, OTHER), (Z0, OWN)), ((Z1, OWN), (Z2, OWN)), ((Z1, OTHER), (Z1, OTHER)), ((Z2, OWN), (Z0, OTHER)), ((Z2, OTHER), (Z3, OWN)), ((Z3, OWN), (Z2, OTHER)), ((Z3, OTHER), (Z3, OTHER)))

    def chip_of(t):
        (d_end, o_end), (d_mid, o_mid) = order[t]
        other = o_end + q * (o_mid - o_end)
        return mirror(z, d_end + q * (d_mid - d_end)), y + other * (1 - 2 * y)

    def rows_of(chip):
        return pl.ds(pl.multiple_of(chip * 2 * cap, 2 * cap), 2 * cap)

    def h_loads(t):
        d, yy = chip_of(t)
        rows = rows_of(d * 2 + yy)
        return [pltpu.make_async_copy(src.at[:, rows, :], hbuf.at[t % 2, i], h_sem.at[t % 2, i]) for i, src in enumerate((hg_hbm, hu_hbm))]

    w_loads = [pltpu.make_async_copy(src, dst, w_sem.at[i]) for i, (src, dst) in enumerate(((wd_hbm, wd), (wg_hbm, wg), (wu_hbm, wu)))]
    for cp in h_loads(0) + w_loads:
        cp.start()

    def yr_load(i):
        return pltpu.make_async_copy(yr_hbm.at[pl.ds(pl.multiple_of(i * 256, 256), 256), :], yr.at[i % 2], g_sem.at[i % 2])

    yr_load(0).start()

    barrier = pltpu.get_barrier_semaphore()
    for k in PEERS:
        pl.semaphore_signal(barrier, inc=1, device_id={"ep": (me + k) % GROUP})

    idx, slots, gates = idx_t[...], slot_t[...], gate_t[...]
    for e in range(n_exp):
        hit = idx == e
        slot = jnp.max(jnp.where(hit, slots, -1), axis=0, keepdims=True)
        slot = jnp.where(slot < counts[0, e], slot, -1)
        meta_out[e // 4, e % 4] = slot.astype(F32)
        meta_out[e // 4, 4 + e % 4] = jnp.sum(jnp.where(hit, gates, 0.0), axis=0, keepdims=True)
    pl.semaphore_wait(barrier, 15)

    part_rows = gy.shape[0] // 2

    def part(p):
        return pl.ds(p * part_rows, part_rows)

    def put(slot, link, to, p, src=None):
        src = tok.at[slot, part(p)] if src is None else src
        return pltpu.make_async_remote_copy(src_ref=src, dst_ref=tok.at[slot, part(p)], send_sem=send.at[slot, link, p], recv_sem=recv.at[slot, p], device_id={"ep": to})

    def arrive(slot, p):
        put(slot, 0, me, p).wait_recv()

    def meta_copy(k):
        to = (me + k) % GROUP
        return pltpu.make_async_remote_copy(src_ref=meta_out.at[to // 2], dst_ref=meta.at[me], send_sem=m_send.at[k], recv_sem=m_recv.at[me], device_id={"ep": to})

    own = [(put(me, link, to, p, gy.at[part(p)]), cond) for p in HALVES for link, to, cond in ((ONWARD, up, None), (DOWN, down, mid), (CROSS, ynb, None), (CORE, sib, None))]
    for cp, cond in own:
        cp.start() if cond is None else pl.when(cond)(cp.start)
    for k in PEERS:
        meta_copy(k).start()
    tok[me] = gy[...]
    meta[me] = meta_out[me // 2]
    acc[...] = jnp.zeros_like(acc)

    gg[...] = jnp.zeros_like(gg)

    def gate_block(i, _):
        yr_load(i).wait()

        @pl.when(i < 7)
        def _():
            yr_load(i + 1).start()

        base = pl.multiple_of((i // 4) * 128, 128)
        prod = dot_nt(yr[i % 2], gy[pl.ds(base, 128), :]).reshape(32, 8, 128)
        t = lax.broadcasted_iota(jnp.int32, prod.shape, 0) + (i % 4) * 32
        mine = t == lax.broadcasted_iota(jnp.int32, prod.shape, 2)
        gg[:, pl.ds(base, 128)] += jnp.sum(jnp.where(mine, prod, 0.0), axis=0)
        return 0

    lax.fori_loop(0, 8, gate_block, 0)
    for k in PEERS:
        src = (me + k) % GROUP
        pltpu.make_async_remote_copy(src_ref=meta_out.at[0], dst_ref=meta.at[src], send_sem=m_send.at[k], recv_sem=m_recv.at[src], device_id={"ep": src}).wait_recv()
    for cp in w_loads:
        cp.wait()

    def home(d, other, h):
        return mirror(z, d) * 4 + (y + other * (1 - 2 * y)) * 2 + h

    def relay(d, other, p, links):
        slot = home(d, other, c)
        arrive(slot, p)
        for link in links:
            put(slot, link, ynb if link == CROSS else sib if link == CORE else up if d == Z0 else down, p).start()

    def y_arrival(d, p, onward=False):
        slot = home(d, 1, c)
        arrive(slot, p)
        if onward:
            put(slot, ONWARD, up, p).start()
        put(slot, CORE, sib, p).start()

    def z_base(d, other, h):
        return mirror(z, d) * 2 + h if other == 0 else 7 + mirror(z, d)

    def z_slot(d, other, h, leftward, to_z):
        return jnp.where(leftward & (mirror(z, d) == to_z), 12 if other else 10 + h, z_base(d, other, h))

    def z_copy(d, other, h, p, step):
        dst = z_slot(d, other, h, step < 0, z + step)
        return pltpu.make_async_remote_copy(src_ref=tot.at[home(d, other, h), part(p)], dst_ref=z_in.at[dst, part(p)], send_sem=zs_sem.at[z_base(d, other, h), p], recv_sem=zr_sem.at[dst, p], device_id={"ep": (me + 4 * step + GROUP) % GROUP})

    def z_add(d, other, h, p, step):
        src, w = z_slot(d, other, h, step < 0, z), home(d, other, h)
        pltpu.make_async_remote_copy(src_ref=tot.at[w, part(p)], dst_ref=z_in.at[src, part(p)], send_sem=zs_sem.at[z_base(d, other, h), p], recv_sem=zr_sem.at[src, p], device_id={"ep": me}).wait_recv()
        tot[w, part(p)] = tot[w, part(p)] + z_in[src, part(p)]

    def y_copy(d, h, p):
        i = mirror(z, d) * 2 + h
        return pltpu.make_async_remote_copy(src_ref=tot.at[home(d, 1, h), part(p)], dst_ref=y_in.at[i, part(p)], send_sem=ys.at[i, p], recv_sem=yrs.at[i, p], device_id={"ep": ynb})

    def y_add(d, h, p):
        y_copy(d, h, p).wait_recv()
        w = home(d, 0, h)
        tot[w, part(p)] = tot[w, part(p)] + y_in[mirror(z, d) * 2 + h, part(p)]

    def y_start(d, h):
        for p in HALVES:
            y_copy(d, h, p).start()

    def start_up(d, other, h):
        for p in HALVES:
            z_copy(d, other, h, p, way).start()

    def pass_up(d, other, h, p):
        z_add(d, other, h, p, way)
        z_copy(d, other, h, p, way).start()

    def y_up(d, h, p):
        y_add(d, h, p)
        z_copy(d, OWN, h, p, way).start()

    def y_chain(d, h, p):
        y_add(d, h, p)
        pass_up(d, OWN, h, p)

    def y_down(d, h, p):
        y_add(d, h, p)
        z_add(d, OWN, h, p, -way)
        z_copy(d, OWN, h, p, -way).start()

    def swap(chip, slot):
        return pltpu.make_async_remote_copy(src_ref=r_send.at[slot], dst_ref=r_recv.at[chip], send_sem=rs.at[chip], recv_sem=rr.at[chip], device_id={"ep": sib})

    def make(t):
        slot = t % 2
        d, yy = chip_of(t)
        chip = d * 2 + yy
        for p in HALVES:
            arrive(chip * 2 + 1 - c, p)
        rows = rows_of(chip)
        for cp in h_loads(t):
            cp.wait()
        if t < 7:
            for cp in h_loads(t + 1):
                cp.start()

        def per_expert(e, _):
            for h in CORES:
                s = chip * 2 + h
                hot = one_hot(meta[s, c * 2 + e], cap)
                gate = jnp.sum(jnp.where(hot, meta[s, 4 + c * 2 + e], 0.0), axis=1, keepdims=True)
                picked = jnp.dot(jnp.where(hot, 1.0, 0.0).astype(BF16), tok[s], preferred_element_type=F32)
                d_ref[h * cap:(h + 1) * cap, :] = (picked * gate).astype(BF16)
            g = dot_nt(d_ref[...], wd[e]).astype(BF16).astype(F32)
            h1 = hbuf[t % 2, 0, e].astype(F32)
            h3 = hbuf[t % 2, 1, e].astype(F32)
            sig = jax.nn.sigmoid(h1)
            act = h1 * sig
            a_ref[...] = (act * h3).astype(BF16)
            dh1[e, rows, :] = (g * h3 * sig * (1.0 + h1 * (1.0 - sig))).astype(BF16)
            dh3[e, rows, :] = (g * act).astype(BF16)
            for part, dest in ((1 - c, r_send), (c, r_own)):
                cols = pl.ds(pl.multiple_of(part * half, half), half)
                r = dot_nt(dh1[e, rows, :], wg[e, cols, :]) + dot_nt(dh3[e, rows, :], wu[e, cols, :])
                dest[slot, e] = r.astype(BF16)
            acc[e] += dot_tn(a_ref[...], d_ref[...])
            return 0

        lax.fori_loop(0, n_loc, per_expert, 0)
        swap(chip, slot).start()

    def combine(t):
        slot = t % 2
        d, yy = chip_of(t)
        chip = d * 2 + yy
        cp = swap(chip, slot)
        cp.wait_recv()
        for h in CORES:
            s = chip * 2 + h
            lanes = pl.ds(h * cap, cap)
            ids = (c * 2, c * 2 + 1, 2 - c * 2, 3 - c * 2)
            pick = jnp.concatenate([jnp.where(one_hot(meta[s, i], cap), 1.0, 0.0).astype(BF16) for i in ids], axis=0)
            vals = jnp.concatenate([r_own[slot, 0, lanes, :], r_own[slot, 1, lanes, :], r_recv[chip, 0, lanes, :], r_recv[chip, 1, lanes, :]], axis=0)
            tot[s] = dot_tn(pick, vals)
        cp.wait_send()

    def at_end(fn):
        pl.when(end)(fn)

    def at_mid(fn):
        pl.when(mid)(fn)

    make(0)
    combine(0)

    @at_end
    def _():
        for p in HALVES:
            y_arrival(Z0, p, True)
            relay(Z1, OWN, p, (CROSS, CORE))

    @at_mid
    def _():
        for p in HALVES:
            relay(Z0, OWN, p, (ONWARD, CORE))
            y_arrival(Z1, p)
            relay(Z2, OWN, p, (ONWARD, CROSS, CORE))

    def second(p):
        @at_end
        def _():
            y_arrival(Z1, p)
            relay(Z2, OWN, p, (CROSS, CORE))

        @at_mid
        def _():
            relay(Z0, OTHER, p, (ONWARD, CORE))
            y_arrival(Z2, p)
            relay(Z3, OWN, p, (ONWARD, CORE))

    def third(p):
        @at_end
        def _():
            y_arrival(Z2, p)
            relay(Z3, OWN, p, (CORE,))

        @at_mid
        def _():
            relay(Z3, OTHER, p, (ONWARD, CORE))

    make(1)
    make(2)
    second(LO)
    combine(1)
    combine(2)
    at_end(lambda: start_up(Z1, OWN, CORE0))
    second(HI)
    make(3)
    make(4)
    third(LO)
    combine(3)
    y_start(Z1, CORE1)
    combine(4)
    at_end(lambda: start_up(Z2, OWN, CORE0))
    at_mid(lambda: y_start(Z0, CORE0))
    third(HI)
    make(5)
    make(6)
    at_end(lambda: relay(Z3, OTHER, LO, (CORE,)))
    combine(5)

    @at_end
    def _():
        start_up(Z2, OTHER, CORE0)
        y_start(Z2, CORE1)

    combine(6)
    at_end(lambda: relay(Z3, OTHER, HI, (CORE,)))
    at_mid(lambda: pass_up(Z2, OWN, CORE0, LO))
    make(7)
    combine(7)
    y_start(Z3, CORE0)
    y_start(Z3, CORE1)
    at_end(lambda: y_start(Z0, CORE0))
    y_start(Z0, CORE1)
    at_mid(lambda: y_start(Z2, CORE1))

    width = xs.shape[2]

    def x_load(i):
        e, t = i // 4, i % 4
        return pltpu.make_async_copy(x_hbm.at[e, :, pl.ds(pl.multiple_of(t * width, width), width)], xs.at[i % 2], x_sem.at[i % 2])

    def w_out(i):
        e, t = i // 4, i % 4
        rows = pl.ds(pl.multiple_of(t * width, width), width)
        return (pltpu.make_async_copy(og.at[i % 2], gwg_hbm.at[e, rows, :], st_sem.at[i % 2, 0]),
                pltpu.make_async_copy(ou.at[i % 2], gwu_hbm.at[e, rows, :], st_sem.at[i % 2, 1]))

    def end_tail():
        y_up(Z3, CORE1, HI)
        start_up(Z1, OTHER, CORE0)
        for p in HALVES:
            y_up(Z1, CORE1, p)

    def end_first():
        for p in HALVES:
            y_up(Z2, CORE1, p)

    end_events = dict(enumerate((end_first, lambda: y_up(Z3, CORE0, LO), lambda: y_up(Z3, CORE0, HI), lambda: y_up(Z3, CORE1, LO), end_tail)))
    mid_events = {0: lambda: pass_up(Z2, OWN, CORE0, HI), 1: lambda: pass_up(Z2, OTHER, CORE0, LO), 2: lambda: pass_up(Z2, OTHER, CORE0, HI), 6: lambda: y_chain(Z3, CORE0, LO), 7: lambda: y_chain(Z3, CORE0, HI)}
    x_load(0).start()
    acc_out = pltpu.make_async_copy(acc, gwd_hbm, acc_sem.at[0])
    acc_out.start()

    def weights(i, _):
        x_load(i).wait()

        @pl.when(i < 7)
        def _():
            x_load(i + 1).start()

        @pl.when(i >= 2)
        def _():
            for cp in w_out(i - 2):
                cp.wait()

        e = i // 4
        og[i % 2] = dot_tn(xs[i % 2], dh1[e])
        ou[i % 2] = dot_tn(xs[i % 2], dh3[e])
        for cp in w_out(i):
            cp.start()
        for n, event in mid_events.items():
            pl.when(mid & (i == n))(event)
        for n, event in end_events.items():
            pl.when(end & (i == n))(event)
        return 0

    lax.fori_loop(0, 8, weights, 0)

    def cross(p):
        z_add(Z1, OTHER, CORE0, p, -way)
        z_add(Z1, OTHER, CORE0, p, way)
        y_copy(Z1, CORE0, p).start()

    @at_mid
    def _():
        y_down(Z0, CORE0, LO)
        y_chain(Z3, CORE1, LO)
        y_down(Z0, CORE0, HI)
        y_chain(Z3, CORE1, HI)
        y_down(Z0, CORE1, LO)
        cross(0)
        y_chain(Z2, CORE1, LO)
        y_down(Z0, CORE1, HI)
        cross(1)
        y_chain(Z2, CORE1, HI)

    def last(p):
        return pltpu.make_async_remote_copy(src_ref=f_send.at[part(p)], dst_ref=f_recv.at[part(p)], send_sem=fs.at[p], recv_sem=fr.at[p], device_id={"ep": sib})

    def finish(h, p):
        w = me - c + h
        i = z * 2 + h
        pltpu.make_async_remote_copy(src_ref=tot.at[w, part(p)], dst_ref=y_in.at[i, part(p)], send_sem=ys.at[i, p], recv_sem=yrs.at[i, p], device_id={"ep": ynb}).wait_recv()
        tot[w, part(p)] = tot[w, part(p)] + y_in[i, part(p)]
        at_end(lambda: z_add(Z0, OWN, h, p, -way))

        @at_mid
        def _():
            z_add(Z1, OWN, h, p, -way)
            z_add(Z1, OWN, h, p, way)

        @pl.when(c == h)
        def _():
            gx[part(p), h * half:(h + 1) * half] = tot[w, part(p)].astype(BF16)

        @pl.when(c != h)
        def _():
            f_send[part(p)] = tot[w, part(p)].astype(BF16)
            last(p).start()

    for p in HALVES:
        for h in CORES:
            finish(h, p)
    for p in HALVES:
        last(p).wait()
    for h in CORES:
        @pl.when(c == h)
        def _():
            gx[:, (1 - h) * half:(2 - h) * half] = f_recv[...]

    for cp, cond in own:
        cp.wait_send() if cond is None else pl.when(cond)(cp.wait_send)

    def drain(tokens, y_units, z_units):
        for p in HALVES:
            for d, other, links in tokens:
                for link in links:
                    put(home(d, other, c), link, me, p).wait_send()
            for d, h in y_units:
                y_copy(d, h, p).wait_send()
            for d, other, h in z_units:
                z_copy(d, other, h, p, way).wait_send()

    SENT = (CORE,)
    at_end(lambda: drain(
        ((Z0, OTHER, (ONWARD, CORE)), (Z1, OWN, (CROSS, CORE)), (Z1, OTHER, SENT), (Z2, OWN, (CROSS, CORE)), (Z2, OTHER, SENT), (Z3, OWN, SENT), (Z3, OTHER, SENT)),
        ((Z0, CORE0), (Z0, CORE1), (Z1, CORE1), (Z2, CORE1), (Z3, CORE0), (Z3, CORE1)),
        ((Z1, OWN, CORE0), (Z1, OTHER, CORE0), (Z2, OWN, CORE0), (Z2, OTHER, CORE0), (Z1, OWN, CORE1), (Z2, OWN, CORE1), (Z3, OWN, CORE0), (Z3, OWN, CORE1))))
    at_mid(lambda: drain(
        ((Z1, OTHER, SENT), (Z0, OWN, (ONWARD, CORE)), (Z0, OTHER, (ONWARD, CORE)), (Z2, OWN, (ONWARD, CROSS, CORE)), (Z2, OTHER, SENT), (Z3, OWN, (ONWARD, CORE)), (Z3, OTHER, (ONWARD, CORE))),
        ((Z0, CORE0), (Z0, CORE1), (Z1, CORE0), (Z1, CORE1), (Z2, CORE1), (Z3, CORE0), (Z3, CORE1)),
        ((Z2, OWN, CORE0), (Z2, OTHER, CORE0), (Z3, OWN, CORE0), (Z3, OWN, CORE1), (Z0, OWN, CORE0), (Z0, OWN, CORE1), (Z2, OWN, CORE1))))
    for k in PEERS:
        meta_copy(k).wait_send()
    for i in (6, 7):
        for cp in w_out(i):
            cp.wait()
    acc_out.wait()


def deliver_kernel(*refs):
    n = (len(refs) - 2) // 3
    src, dst, buf, (in_sem, out_sem) = refs[:n], refs[n:2 * n], refs[2 * n:3 * n], refs[3 * n:]
    pieces = []
    for s, d, b in zip(src, dst, buf):
        rows = s.shape[-2]
        parts = 2 if len(s.shape) == 3 else 1
        for lead in ([(e,) for e in range(s.shape[0])] if len(s.shape) == 3 else [()]):
            for k in range(parts):
                at = lead + (pl.ds(k * rows // parts, rows // parts),)
                i = len(pieces)
                pieces.append((pltpu.make_async_copy(s.at[at], b.at[at], in_sem.at[i]), pltpu.make_async_copy(b.at[at], d.at[at], out_sem.at[i])))
    for read, _ in pieces:
        read.start()
    for read, write in pieces:
        read.wait()
        write.start()
    for _, write in pieces:
        write.wait()


def deliver(arrays):
    n = 2 + 4 * (len(arrays) - 2)
    return pl.pallas_call(
        deliver_kernel,
        out_shape=tuple(jax.ShapeDtypeStruct(a.shape, a.dtype) for a in arrays),
        in_specs=[ANY] * len(arrays),
        out_specs=(ANY,) * len(arrays),
        scratch_shapes=[VMEM(a.shape, a.dtype) for a in arrays] + [DMA((n,)), DMA((n,))],
        compiler_params=pltpu.CompilerParams(vmem_limit_bytes=67043328),
        name="deliver",
    )(*arrays)


def solution(mesh):
    rows_spec = P(("dp", "ep"), None)
    cube_spec = P(("dp", "ep"), None, None)
    weight_spec = P("ep", None, None)

    def local_step(grad_y, gate_vals, topk_idx, slot_ids, pair_counts, y_routed, x_disp, h_gate, h_up, w_gate, w_up, w_down):
        n_loc, n_rows, ffn = h_gate.shape
        tok, dim = grad_y.shape
        top_k = topk_idx.shape[1]
        half = dim // 2
        cap = n_rows // 16
        shape = jax.ShapeDtypeStruct
        grad_x, grad_gate, grad_wdown, grad_wgate, grad_wup = pl.pallas_call(
            step_kernel,
            out_shape=(shape((tok, dim), BF16), shape((top_k, tok), F32), shape((n_loc, ffn, dim), F32), shape((n_loc, dim, ffn), F32), shape((n_loc, dim, ffn), F32)),
            in_specs=[VM, VM, VM, VM, pl.BlockSpec(memory_space=pltpu.SMEM)] + [ANY] * 7,
            out_specs=(VM, VM, ANY, ANY, ANY),
            scratch_shapes=[
                VMEM((16, tok, dim), BF16), VMEM((16, 8, 1, tok), F32), VMEM((8, 8, 1, tok), F32),
                VMEM((2, 2, n_loc, 2 * cap, ffn), BF16),
                VMEM((n_loc, ffn, dim), BF16), VMEM((n_loc, dim, ffn), BF16), VMEM((n_loc, dim, ffn), BF16),
                VMEM((2, n_rows, 256), BF16), VMEM((2, 256, dim), BF16),
                VMEM((2 * cap, dim), BF16), VMEM((2 * cap, ffn), BF16),
                VMEM((n_loc, n_rows, ffn), BF16), VMEM((n_loc, n_rows, ffn), BF16), VMEM((n_loc, ffn, dim), F32),
                VMEM((2, n_loc, 2 * cap, half), BF16), VMEM((2, n_loc, 2 * cap, half), BF16), VMEM((8, n_loc, 2 * cap, half), BF16),
                VMEM((16, tok, half), F32), VMEM((13, tok, half), F32), VMEM((8, tok, half), F32),
                VMEM((tok, half), BF16), VMEM((tok, half), BF16),
                VMEM((2, 256, ffn), F32), VMEM((2, 256, ffn), F32),
                DMA((3,)), DMA((2, 2)), DMA((2,)), DMA((2,)), DMA((2, 2)), DMA((1,)),
                DMA((16, 4, 2)), DMA((16, 2)), DMA((16,)), DMA((16,)), DMA((8,)), DMA((8,)), DMA((8, 2)), DMA((8, 2)), DMA((10, 2)), DMA((13, 2)), DMA((2,)), DMA((2,)),
            ],
            compiler_params=pltpu.CompilerParams(collective_id=1, has_side_effects=True, vmem_limit_bytes=67043328),
            name="step",
        )(grad_y, topk_idx.T, slot_ids.T, gate_vals.T, pair_counts, y_routed.reshape(tok * top_k, dim), h_gate, h_up, w_down, w_gate, w_up, x_disp)
        grad_wgate, grad_wup, grad_wdown, grad_x, grad_gate = deliver((grad_wgate, grad_wup, grad_wdown, grad_x, grad_gate))
        return grad_x, grad_gate.T, grad_wgate, grad_wup, grad_wdown

    return jax.shard_map(local_step, mesh=mesh, in_specs=(rows_spec, rows_spec, rows_spec, rows_spec, rows_spec, cube_spec, cube_spec, cube_spec, cube_spec, weight_spec, weight_spec, weight_spec), out_specs=(rows_spec, rows_spec, cube_spec, cube_spec, cube_spec), check_vma=False)
```

```python
import jax
import jax.numpy as jnp
from jax import lax
from jax.experimental import pallas as pl
from jax.experimental.pallas import tpu as pltpu
from jax.sharding import PartitionSpec as P

F32 = jnp.float32
BF16 = jnp.bfloat16
VMEM = pltpu.VMEM
DMA = pltpu.SemaphoreType.DMA
Z0, Z1, Z2, Z3 = range(4)
OWN, OTHER = CORE0, CORE1 = LO, HI = CORES = HALVES = range(2)
ONWARD, DOWN, CROSS, CORE = range(4)
NZ, GROUP = 4, 16
PEERS = range(1, GROUP)
ANY = pl.BlockSpec(memory_space=pl.ANY)
VM = pl.BlockSpec(memory_space=pltpu.VMEM)


def position():
    me = lax.axis_index("ep")
    return me, me // 4, (me // 2) % 2, me % 2


def mirror(z, v):
    return v + (z // 2) * (3 - 2 * v)


def dot_nt(a, b):
    return lax.dot_general(a, b, (((1,), (1,)), ((), ())), preferred_element_type=F32)


def dot_tn(a, b):
    return lax.dot_general(a, b, (((0,), (0,)), ((), ())), preferred_element_type=F32)


def one_hot(slot, cap):
    return slot == lax.broadcasted_iota(jnp.int32, (cap, slot.shape[1]), 0).astype(F32)


def step_kernel(gy, idx_t, slot_t, gate_t, counts, yr_hbm, hg_hbm, hu_hbm, wd_hbm, wg_hbm, wu_hbm, x_hbm, gx, gg, gwd_hbm, gwg_hbm, gwu_hbm,
                tok, meta, meta_out, hbuf, wd, wg, wu, xs, yr, d_ref, a_ref, dh1, dh3, acc, r_own, r_send, r_recv, tot, z_in, y_in, f_send, f_recv, og, ou,
                w_sem, h_sem, x_sem, g_sem, st_sem, acc_sem, send, recv, m_send, m_recv, rs, rr, ys, yrs, zs_sem, zr_sem, fs, fr):
    me, z, y, c = position()
    n_loc, n_rows, ffn = dh1.shape
    cap = n_rows // 16
    half = r_own.shape[3]
    n_exp = counts.shape[1]
    sib = me + 1 - 2 * c
    ynb = me + 2 - 4 * y
    m = z // 2
    q = mirror(z, z)
    way = 1 - 2 * m
    end = q == 0
    mid = q == 1
    up = (me + 4 * way + GROUP) % GROUP
    down = (me - 4 * way + GROUP) % GROUP

    order = (((Z0, OWN), (Z1, OWN)), ((Z0, OTHER), (Z0, OWN)), ((Z1, OWN), (Z2, OWN)), ((Z1, OTHER), (Z1, OTHER)), ((Z2, OWN), (Z0, OTHER)), ((Z2, OTHER), (Z3, OWN)), ((Z3, OWN), (Z2, OTHER)), ((Z3, OTHER), (Z3, OTHER)))

    def chip_of(t):
        (d_end, o_end), (d_mid, o_mid) = order[t]
        other = o_end + q * (o_mid - o_end)
        return mirror(z, d_end + q * (d_mid - d_end)), y + other * (1 - 2 * y)

    def rows_of(chip):
        return pl.ds(pl.multiple_of(chip * 2 * cap, 2 * cap), 2 * cap)

    def h_loads(t):
        d, yy = chip_of(t)
        rows = rows_of(d * 2 + yy)
        return [pltpu.make_async_copy(src.at[:, rows, :], hbuf.at[t % 2, i], h_sem.at[t % 2, i]) for i, src in enumerate((hg_hbm, hu_hbm))]

    w_loads = [pltpu.make_async_copy(src, dst, w_sem.at[i]) for i, (src, dst) in enumerate(((wd_hbm, wd), (wg_hbm, wg), (wu_hbm, wu)))]
    for cp in h_loads(0) + w_loads:
        cp.start()

    def yr_load(i):
        return pltpu.make_async_copy(yr_hbm.at[pl.ds(pl.multiple_of(i * 256, 256), 256), :], yr.at[i % 2], g_sem.at[i % 2])

    yr_load(0).start()

    barrier = pltpu.get_barrier_semaphore()
    for k in PEERS:
        pl.semaphore_signal(barrier, inc=1, device_id={"ep": (me + k) % GROUP})

    idx, slots, gates = idx_t[...], slot_t[...], gate_t[...]
    for e in range(n_exp):
        hit = idx == e
        slot = jnp.max(jnp.where(hit, slots, -1), axis=0, keepdims=True)
        slot = jnp.where(slot < counts[0, e], slot, -1)
        meta_out[e // 4, e % 4] = slot.astype(F32)
        meta_out[e // 4, 4 + e % 4] = jnp.sum(jnp.where(hit, gates, 0.0), axis=0, keepdims=True)
    pl.semaphore_wait(barrier, 15)

    part_rows = gy.shape[0] // 2

    def part(p):
        return pl.ds(p * part_rows, part_rows)

    def put(slot, link, to, p, src=None):
        src = tok.at[slot, part(p)] if src is None else src
        return pltpu.make_async_remote_copy(src_ref=src, dst_ref=tok.at[slot, part(p)], send_sem=send.at[slot, link, p], recv_sem=recv.at[slot, p], device_id={"ep": to})

    def arrive(slot, p):
        put(slot, 0, me, p).wait_recv()

    def meta_copy(k):
        to = (me + k) % GROUP
        return pltpu.make_async_remote_copy(src_ref=meta_out.at[to // 2], dst_ref=meta.at[me], send_sem=m_send.at[k], recv_sem=m_recv.at[me], device_id={"ep": to})

    own = [(put(me, link, to, p, gy.at[part(p)]), cond) for p in HALVES for link, to, cond in ((ONWARD, up, None), (DOWN, down, mid), (CROSS, ynb, None), (CORE, sib, None))]
    for cp, cond in own:
        cp.start() if cond is None else pl.when(cond)(cp.start)
    for k in PEERS:
        meta_copy(k).start()
    tok[me] = gy[...]
    meta[me] = meta_out[me // 2]
    acc[...] = jnp.zeros_like(acc)

    gg[...] = jnp.zeros_like(gg)

    def gate_block(i, _):
        yr_load(i).wait()

        @pl.when(i < 7)
        def _():
            yr_load(i + 1).start()

        base = pl.multiple_of((i // 4) * 128, 128)
        prod = dot_nt(yr[i % 2], gy[pl.ds(base, 128), :]).reshape(32, 8, 128)
        t = lax.broadcasted_iota(jnp.int32, prod.shape, 0) + (i % 4) * 32
        mine = t == lax.broadcasted_iota(jnp.int32, prod.shape, 2)
        gg[:, pl.ds(base, 128)] += jnp.sum(jnp.where(mine, prod, 0.0), axis=0)
        return 0

    lax.fori_loop(0, 8, gate_block, 0)
    for k in PEERS:
        src = (me + k) % GROUP
        pltpu.make_async_remote_copy(src_ref=meta_out.at[0], dst_ref=meta.at[src], send_sem=m_send.at[k], recv_sem=m_recv.at[src], device_id={"ep": src}).wait_recv()
    for cp in w_loads:
        cp.wait()

    def home(d, other, h):
        return mirror(z, d) * 4 + (y + other * (1 - 2 * y)) * 2 + h

    def relay(d, other, p, links):
        slot = home(d, other, c)
        arrive(slot, p)
        for link in links:
            put(slot, link, ynb if link == CROSS else sib if link == CORE else up if d == Z0 else down, p).start()

    def y_arrival(d, p, onward=False):
        slot = home(d, 1, c)
        arrive(slot, p)
        if onward:
            put(slot, ONWARD, up, p).start()
        put(slot, CORE, sib, p).start()

    def z_base(d, other, h):
        return mirror(z, d) * 2 + h if other == 0 else 7 + mirror(z, d)

    def z_slot(d, other, h, leftward, to_z):
        return jnp.where(leftward & (mirror(z, d) == to_z), 12 if other else 10 + h, z_base(d, other, h))

    def z_copy(d, other, h, p, step):
        dst = z_slot(d, other, h, step < 0, z + step)
        return pltpu.make_async_remote_copy(src_ref=tot.at[home(d, other, h), part(p)], dst_ref=z_in.at[dst, part(p)], send_sem=zs_sem.at[z_base(d, other, h), p], recv_sem=zr_sem.at[dst, p], device_id={"ep": (me + 4 * step + GROUP) % GROUP})

    def z_add(d, other, h, p, step):
        src, w = z_slot(d, other, h, step < 0, z), home(d, other, h)
        pltpu.make_async_remote_copy(src_ref=tot.at[w, part(p)], dst_ref=z_in.at[src, part(p)], send_sem=zs_sem.at[z_base(d, other, h), p], recv_sem=zr_sem.at[src, p], device_id={"ep": me}).wait_recv()
        tot[w, part(p)] = tot[w, part(p)] + z_in[src, part(p)]

    def y_copy(d, h, p):
        i = mirror(z, d) * 2 + h
        return pltpu.make_async_remote_copy(src_ref=tot.at[home(d, 1, h), part(p)], dst_ref=y_in.at[i, part(p)], send_sem=ys.at[i, p], recv_sem=yrs.at[i, p], device_id={"ep": ynb})

    def y_add(d, h, p):
        y_copy(d, h, p).wait_recv()
        w = home(d, 0, h)
        tot[w, part(p)] = tot[w, part(p)] + y_in[mirror(z, d) * 2 + h, part(p)]

    def y_start(d, h):
        for p in HALVES:
            y_copy(d, h, p).start()

    def start_up(d, other, h):
        for p in HALVES:
            z_copy(d, other, h, p, way).start()

    def pass_up(d, other, h, p):
        z_add(d, other, h, p, way)
        z_copy(d, other, h, p, way).start()

    def y_up(d, h, p):
        y_add(d, h, p)
        z_copy(d, OWN, h, p, way).start()

    def y_chain(d, h, p):
        y_add(d, h, p)
        pass_up(d, OWN, h, p)

    def y_down(d, h, p):
        y_add(d, h, p)
        z_add(d, OWN, h, p, -way)
        z_copy(d, OWN, h, p, -way).start()

    def swap(chip, slot, e):
        return pltpu.make_async_remote_copy(src_ref=r_send.at[slot, e], dst_ref=r_recv.at[chip, e], send_sem=rs.at[chip, e], recv_sem=rr.at[chip, e], device_id={"ep": sib})

    def build_rows(chip, e):
        for h in CORES:
            s = chip * 2 + h
            hot = one_hot(meta[s, c * 2 + e], cap)
            gate = jnp.sum(jnp.where(hot, meta[s, 4 + c * 2 + e], 0.0), axis=1, keepdims=True)
            picked = jnp.dot(jnp.where(hot, 1.0, 0.0).astype(BF16), tok[s], preferred_element_type=F32)
            d_ref[h * cap:(h + 1) * cap, :] = (picked * gate).astype(BF16)

    def make(t):
        slot = t % 2
        d, yy = chip_of(t)
        chip = d * 2 + yy
        for p in HALVES:
            arrive(chip * 2 + 1 - c, p)
        rows = rows_of(chip)
        for cp in h_loads(t):
            cp.wait()
        if t < 7:
            for cp in h_loads(t + 1):
                cp.start()

        def per_expert(e, _):
            build_rows(chip, e)
            g = dot_nt(d_ref[...], wd[e]).astype(BF16).astype(F32)
            h1 = hbuf[t % 2, 0, e].astype(F32)
            h3 = hbuf[t % 2, 1, e].astype(F32)
            sig = jax.nn.sigmoid(h1)
            act = h1 * sig
            dh1[e, rows, :] = (g * h3 * sig * (1.0 + h1 * (1.0 - sig))).astype(BF16)
            dh3[e, rows, :] = (g * act).astype(BF16)

            def ret_rows(side):
                cols = pl.ds(pl.multiple_of(side * half, half), half)
                return (dot_nt(dh1[e, rows, :], wg[e, cols, :]) + dot_nt(dh3[e, rows, :], wu[e, cols, :])).astype(BF16)

            r_send[slot, e] = ret_rows(1 - c)
            swap(chip, slot, e).start()
            r_own[slot, e] = ret_rows(c)
            return 0

        lax.fori_loop(0, n_loc, per_expert, 0)

    def combine(t):
        slot = t % 2
        d, yy = chip_of(t)
        chip = d * 2 + yy
        for e in range(n_loc):
            swap(chip, slot, e).wait_recv()
        for h in CORES:
            s = chip * 2 + h
            lanes = pl.ds(h * cap, cap)
            ids = (c * 2, c * 2 + 1, 2 - c * 2, 3 - c * 2)
            pick = jnp.concatenate([jnp.where(one_hot(meta[s, i], cap), 1.0, 0.0).astype(BF16) for i in ids], axis=0)
            vals = jnp.concatenate([r_own[slot, 0, lanes, :], r_own[slot, 1, lanes, :], r_recv[chip, 0, lanes, :], r_recv[chip, 1, lanes, :]], axis=0)
            tot[s] = dot_tn(pick, vals)
        for e in range(n_loc):
            swap(chip, slot, e).wait_send()

    def at_end(fn):
        pl.when(end)(fn)

    def at_mid(fn):
        pl.when(mid)(fn)

    make(0)
    combine(0)

    @at_end
    def _():
        for p in HALVES:
            y_arrival(Z0, p, True)
            relay(Z1, OWN, p, (CROSS, CORE))

    @at_mid
    def _():
        for p in HALVES:
            relay(Z0, OWN, p, (ONWARD, CORE))
            y_arrival(Z1, p)
            relay(Z2, OWN, p, (ONWARD, CROSS, CORE))

    def second(p):
        @at_end
        def _():
            y_arrival(Z1, p)
            relay(Z2, OWN, p, (CROSS, CORE))

        @at_mid
        def _():
            relay(Z0, OTHER, p, (ONWARD, CORE))
            y_arrival(Z2, p)
            relay(Z3, OWN, p, (ONWARD, CORE))

    def third(p):
        @at_end
        def _():
            y_arrival(Z2, p)
            relay(Z3, OWN, p, (CORE,))

        @at_mid
        def _():
            relay(Z3, OTHER, p, (ONWARD, CORE))

    make(1)
    make(2)
    second(LO)
    combine(1)
    combine(2)
    at_end(lambda: start_up(Z1, OWN, CORE0))
    second(HI)
    make(3)
    make(4)
    third(LO)
    combine(3)
    y_start(Z1, CORE1)
    combine(4)
    at_end(lambda: start_up(Z2, OWN, CORE0))
    at_mid(lambda: y_start(Z0, CORE0))
    third(HI)
    make(5)
    make(6)
    at_end(lambda: relay(Z3, OTHER, LO, (CORE,)))
    combine(5)

    @at_end
    def _():
        start_up(Z2, OTHER, CORE0)
        y_start(Z2, CORE1)

    combine(6)
    at_end(lambda: relay(Z3, OTHER, HI, (CORE,)))
    at_mid(lambda: pass_up(Z2, OWN, CORE0, LO))
    make(7)
    combine(7)
    y_start(Z3, CORE0)
    y_start(Z3, CORE1)
    at_end(lambda: y_start(Z0, CORE0))
    y_start(Z0, CORE1)
    at_mid(lambda: y_start(Z2, CORE1))

    width = xs.shape[2]

    def x_load(i):
        e, t = i // 4, i % 4
        return pltpu.make_async_copy(x_hbm.at[e, :, pl.ds(pl.multiple_of(t * width, width), width)], xs.at[i % 2], x_sem.at[i % 2])

    def w_out(i):
        e, t = i // 4, i % 4
        rows = pl.ds(pl.multiple_of(t * width, width), width)
        return (pltpu.make_async_copy(og.at[i % 2], gwg_hbm.at[e, rows, :], st_sem.at[i % 2, 0]),
                pltpu.make_async_copy(ou.at[i % 2], gwu_hbm.at[e, rows, :], st_sem.at[i % 2, 1]))

    def end_tail():
        y_up(Z3, CORE1, HI)
        start_up(Z1, OTHER, CORE0)
        for p in HALVES:
            y_up(Z1, CORE1, p)

    def end_first():
        for p in HALVES:
            y_up(Z2, CORE1, p)

    end_events = dict(enumerate((end_first, lambda: y_up(Z3, CORE0, LO), lambda: y_up(Z3, CORE0, HI), lambda: y_up(Z3, CORE1, LO), end_tail)))
    mid_events = {0: lambda: pass_up(Z2, OWN, CORE0, HI), 1: lambda: pass_up(Z2, OTHER, CORE0, LO), 2: lambda: pass_up(Z2, OTHER, CORE0, HI), 6: lambda: y_chain(Z3, CORE0, LO), 7: lambda: y_chain(Z3, CORE0, HI)}
    def tail_loads(i):
        rows = rows_of(i)
        return [pltpu.make_async_copy(src.at[:, rows, :], hbuf.at[i % 2, n], h_sem.at[i % 2, n]) for n, src in enumerate((hg_hbm, hu_hbm))]

    x_load(0).start()
    for cp in tail_loads(0):
        cp.start()

    def down_grad(i):
        for cp in tail_loads(i):
            cp.wait()

        @pl.when(i < 7)
        def _():
            for cp in tail_loads(i + 1):
                cp.start()

        def per_expert(e, _):
            build_rows(i, e)
            h1 = hbuf[i % 2, 0, e].astype(F32)
            a_ref[...] = (h1 * jax.nn.sigmoid(h1) * hbuf[i % 2, 1, e].astype(F32)).astype(BF16)
            acc[e] += dot_tn(a_ref[...], d_ref[...])
            return 0

        lax.fori_loop(0, n_loc, per_expert, 0)


    def weights(i, _):
        x_load(i).wait()

        @pl.when(i < 7)
        def _():
            x_load(i + 1).start()

        @pl.when(i >= 2)
        def _():
            for cp in w_out(i - 2):
                cp.wait()

        e = i // 4
        og[i % 2] = dot_tn(xs[i % 2], dh1[e])
        ou[i % 2] = dot_tn(xs[i % 2], dh3[e])
        for cp in w_out(i):
            cp.start()
        down_grad(i)
        for n, event in mid_events.items():
            pl.when(mid & (i == n))(event)
        for n, event in end_events.items():
            pl.when(end & (i == n))(event)
        return 0

    lax.fori_loop(0, 8, weights, 0)
    acc_out = pltpu.make_async_copy(acc, gwd_hbm, acc_sem.at[0])
    acc_out.start()

    def cross(p):
        z_add(Z1, OTHER, CORE0, p, -way)
        z_add(Z1, OTHER, CORE0, p, way)
        y_copy(Z1, CORE0, p).start()

    @at_mid
    def _():
        y_down(Z0, CORE0, LO)
        y_chain(Z3, CORE1, LO)
        y_down(Z0, CORE0, HI)
        y_chain(Z3, CORE1, HI)
        y_down(Z0, CORE1, LO)
        cross(0)
        y_chain(Z2, CORE1, LO)
        y_down(Z0, CORE1, HI)
        cross(1)
        y_chain(Z2, CORE1, HI)

    def last(p):
        return pltpu.make_async_remote_copy(src_ref=f_send.at[part(p)], dst_ref=f_recv.at[part(p)], send_sem=fs.at[p], recv_sem=fr.at[p], device_id={"ep": sib})

    def finish(h, p):
        w = me - c + h
        i = z * 2 + h
        pltpu.make_async_remote_copy(src_ref=tot.at[w, part(p)], dst_ref=y_in.at[i, part(p)], send_sem=ys.at[i, p], recv_sem=yrs.at[i, p], device_id={"ep": ynb}).wait_recv()
        tot[w, part(p)] = tot[w, part(p)] + y_in[i, part(p)]
        at_end(lambda: z_add(Z0, OWN, h, p, -way))

        @at_mid
        def _():
            z_add(Z1, OWN, h, p, -way)
            z_add(Z1, OWN, h, p, way)

        @pl.when(c == h)
        def _():
            gx[part(p), h * half:(h + 1) * half] = tot[w, part(p)].astype(BF16)

        @pl.when(c != h)
        def _():
            f_send[part(p)] = tot[w, part(p)].astype(BF16)
            last(p).start()

    for p in HALVES:
        for h in CORES:
            finish(h, p)
    for p in HALVES:
        last(p).wait()
    for h in CORES:
        @pl.when(c == h)
        def _():
            gx[:, (1 - h) * half:(2 - h) * half] = f_recv[...]

    for cp, cond in own:
        cp.wait_send() if cond is None else pl.when(cond)(cp.wait_send)

    def drain(tokens, y_units, z_units):
        for p in HALVES:
            for d, other, links in tokens:
                for link in links:
                    put(home(d, other, c), link, me, p).wait_send()
            for d, h in y_units:
                y_copy(d, h, p).wait_send()
            for d, other, h in z_units:
                z_copy(d, other, h, p, way).wait_send()

    SENT = (CORE,)
    at_end(lambda: drain(
        ((Z0, OTHER, (ONWARD, CORE)), (Z1, OWN, (CROSS, CORE)), (Z1, OTHER, SENT), (Z2, OWN, (CROSS, CORE)), (Z2, OTHER, SENT), (Z3, OWN, SENT), (Z3, OTHER, SENT)),
        ((Z0, CORE0), (Z0, CORE1), (Z1, CORE1), (Z2, CORE1), (Z3, CORE0), (Z3, CORE1)),
        ((Z1, OWN, CORE0), (Z1, OTHER, CORE0), (Z2, OWN, CORE0), (Z2, OTHER, CORE0), (Z1, OWN, CORE1), (Z2, OWN, CORE1), (Z3, OWN, CORE0), (Z3, OWN, CORE1))))
    at_mid(lambda: drain(
        ((Z1, OTHER, SENT), (Z0, OWN, (ONWARD, CORE)), (Z0, OTHER, (ONWARD, CORE)), (Z2, OWN, (ONWARD, CROSS, CORE)), (Z2, OTHER, SENT), (Z3, OWN, (ONWARD, CORE)), (Z3, OTHER, (ONWARD, CORE))),
        ((Z0, CORE0), (Z0, CORE1), (Z1, CORE0), (Z1, CORE1), (Z2, CORE1), (Z3, CORE0), (Z3, CORE1)),
        ((Z2, OWN, CORE0), (Z2, OTHER, CORE0), (Z3, OWN, CORE0), (Z3, OWN, CORE1), (Z0, OWN, CORE0), (Z0, OWN, CORE1), (Z2, OWN, CORE1))))
    for k in PEERS:
        meta_copy(k).wait_send()
    for i in (6, 7):
        for cp in w_out(i):
            cp.wait()
    acc_out.wait()


def deliver_kernel(*refs):
    n = (len(refs) - 2) // 3
    src, dst, buf, (in_sem, out_sem) = refs[:n], refs[n:2 * n], refs[2 * n:3 * n], refs[3 * n:]
    pieces = []
    for s, d, b in zip(src, dst, buf):
        rows = s.shape[-2]
        parts = 2 if len(s.shape) == 3 else 1
        for lead in ([(e,) for e in range(s.shape[0])] if len(s.shape) == 3 else [()]):
            for k in range(parts):
                at = lead + (pl.ds(k * rows // parts, rows // parts),)
                i = len(pieces)
                pieces.append((pltpu.make_async_copy(s.at[at], b.at[at], in_sem.at[i]), pltpu.make_async_copy(b.at[at], d.at[at], out_sem.at[i])))
    for read, _ in pieces:
        read.start()
    for read, write in pieces:
        read.wait()
        write.start()
    for _, write in pieces:
        write.wait()


def deliver(arrays):
    n = 2 + 4 * (len(arrays) - 2)
    return pl.pallas_call(
        deliver_kernel,
        out_shape=tuple(jax.ShapeDtypeStruct(a.shape, a.dtype) for a in arrays),
        in_specs=[ANY] * len(arrays),
        out_specs=(ANY,) * len(arrays),
        scratch_shapes=[VMEM(a.shape, a.dtype) for a in arrays] + [DMA((n,)), DMA((n,))],
        compiler_params=pltpu.CompilerParams(vmem_limit_bytes=67043328),
        name="deliver",
    )(*arrays)


def solution(mesh):
    rows_spec = P(("dp", "ep"), None)
    cube_spec = P(("dp", "ep"), None, None)
    weight_spec = P("ep", None, None)

    def local_step(grad_y, gate_vals, topk_idx, slot_ids, pair_counts, y_routed, x_disp, h_gate, h_up, w_gate, w_up, w_down):
        n_loc, n_rows, ffn = h_gate.shape
        tok, dim = grad_y.shape
        top_k = topk_idx.shape[1]
        half = dim // 2
        cap = n_rows // 16
        shape = jax.ShapeDtypeStruct
        grad_x, grad_gate, grad_wdown, grad_wgate, grad_wup = pl.pallas_call(
            step_kernel,
            out_shape=(shape((tok, dim), BF16), shape((top_k, tok), F32), shape((n_loc, ffn, dim), F32), shape((n_loc, dim, ffn), F32), shape((n_loc, dim, ffn), F32)),
            in_specs=[VM, VM, VM, VM, pl.BlockSpec(memory_space=pltpu.SMEM)] + [ANY] * 7,
            out_specs=(VM, VM, ANY, ANY, ANY),
            scratch_shapes=[
                VMEM((16, tok, dim), BF16), VMEM((16, 8, 1, tok), F32), VMEM((8, 8, 1, tok), F32),
                VMEM((2, 2, n_loc, 2 * cap, ffn), BF16),
                VMEM((n_loc, ffn, dim), BF16), VMEM((n_loc, dim, ffn), BF16), VMEM((n_loc, dim, ffn), BF16),
                VMEM((2, n_rows, 256), BF16), VMEM((2, 256, dim), BF16),
                VMEM((2 * cap, dim), BF16), VMEM((2 * cap, ffn), BF16),
                VMEM((n_loc, n_rows, ffn), BF16), VMEM((n_loc, n_rows, ffn), BF16), VMEM((n_loc, ffn, dim), F32),
                VMEM((2, n_loc, 2 * cap, half), BF16), VMEM((2, n_loc, 2 * cap, half), BF16), VMEM((8, n_loc, 2 * cap, half), BF16),
                VMEM((16, tok, half), F32), VMEM((13, tok, half), F32), VMEM((8, tok, half), F32),
                VMEM((tok, half), BF16), VMEM((tok, half), BF16),
                VMEM((2, 256, ffn), F32), VMEM((2, 256, ffn), F32),
                DMA((3,)), DMA((2, 2)), DMA((2,)), DMA((2,)), DMA((2, 2)), DMA((1,)),
                DMA((16, 4, 2)), DMA((16, 2)), DMA((16,)), DMA((16,)), DMA((8, n_loc)), DMA((8, n_loc)), DMA((8, 2)), DMA((8, 2)), DMA((10, 2)), DMA((13, 2)), DMA((2,)), DMA((2,)),
            ],
            compiler_params=pltpu.CompilerParams(collective_id=1, has_side_effects=True, vmem_limit_bytes=67043328),
            name="step",
        )(grad_y, topk_idx.T, slot_ids.T, gate_vals.T, pair_counts, y_routed.reshape(tok * top_k, dim), h_gate, h_up, w_down, w_gate, w_up, x_disp)
        grad_wgate, grad_wup, grad_wdown, grad_x, grad_gate = deliver((grad_wgate, grad_wup, grad_wdown, grad_x, grad_gate))
        return grad_x, grad_gate.T, grad_wgate, grad_wup, grad_wdown

    return jax.shard_map(local_step, mesh=mesh, in_specs=(rows_spec, rows_spec, rows_spec, rows_spec, rows_spec, cube_spec, cube_spec, cube_spec, cube_spec, weight_spec, weight_spec, weight_spec), out_specs=(rows_spec, rows_spec, cube_spec, cube_spec, cube_spec), check_vma=False)
```

```python
import jax
import jax.numpy as jnp
from jax import lax
from jax.experimental import pallas as pl
from jax.experimental.pallas import tpu as pltpu
from jax.sharding import PartitionSpec as P

F32 = jnp.float32
BF16 = jnp.bfloat16
VMEM = pltpu.VMEM
DMA = pltpu.SemaphoreType.DMA
Z0, Z1, Z2, Z3 = range(4)
OWN, OTHER = CORE0, CORE1 = LO, HI = CORES = HALVES = range(2)
ONWARD, DOWN, CROSS, CORE = range(4)
NZ, GROUP = 4, 16
PEERS = range(1, GROUP)
ANY = pl.BlockSpec(memory_space=pl.ANY)
VM = pl.BlockSpec(memory_space=pltpu.VMEM)


def position():
    me = lax.axis_index("ep")
    return me, me // 4, (me // 2) % 2, me % 2


def mirror(z, v):
    return v + (z // 2) * (3 - 2 * v)


def dot_nt(a, b):
    return lax.dot_general(a, b, (((1,), (1,)), ((), ())), preferred_element_type=F32)


def dot_tn(a, b):
    return lax.dot_general(a, b, (((0,), (0,)), ((), ())), preferred_element_type=F32)


def one_hot(slot, cap):
    return slot == lax.broadcasted_iota(jnp.int32, (cap, slot.shape[1]), 0).astype(F32)


def step_kernel(gy, idx_t, slot_t, gate_t, counts, yr_hbm, hg_hbm, hu_hbm, wd_hbm, wg_hbm, wu_hbm, x_hbm, gx, gg, gwd_hbm, gwg_hbm, gwu_hbm,
                tok, meta, meta_out, hbuf, wd, wg, wu, xs, yr, d_ref, a_ref, dh1, dh3, acc, r_own, r_send, r_recv, tot, z_in, y_in, f_send, f_recv, og, ou,
                w_sem, h_sem, x_sem, g_sem, st_sem, acc_sem, send, recv, m_send, m_recv, rs, rr, ys, yrs, zs_sem, zr_sem, fs, fr):
    me, z, y, c = position()
    n_loc, n_rows, ffn = dh1.shape
    cap = n_rows // 16
    half = r_own.shape[3]
    n_exp = counts.shape[1]
    sib = me + 1 - 2 * c
    ynb = me + 2 - 4 * y
    m = z // 2
    q = mirror(z, z)
    way = 1 - 2 * m
    end = q == 0
    mid = q == 1
    up = (me + 4 * way + GROUP) % GROUP
    down = (me - 4 * way + GROUP) % GROUP

    order = (((Z0, OWN), (Z1, OWN)), ((Z0, OTHER), (Z0, OWN)), ((Z1, OWN), (Z2, OWN)), ((Z1, OTHER), (Z1, OTHER)), ((Z2, OWN), (Z0, OTHER)), ((Z2, OTHER), (Z3, OWN)), ((Z3, OWN), (Z2, OTHER)), ((Z3, OTHER), (Z3, OTHER)))

    def chip_of(t):
        (d_end, o_end), (d_mid, o_mid) = order[t]
        other = o_end + q * (o_mid - o_end)
        return mirror(z, d_end + q * (d_mid - d_end)), y + other * (1 - 2 * y)

    def rows_of(chip):
        return pl.ds(pl.multiple_of(chip * 2 * cap, 2 * cap), 2 * cap)

    def h_loads(t):
        d, yy = chip_of(t)
        rows = rows_of(d * 2 + yy)
        return [pltpu.make_async_copy(src.at[:, rows, :], hbuf.at[t % 2, i], h_sem.at[t % 2, i]) for i, src in enumerate((hg_hbm, hu_hbm))]

    w_loads = [pltpu.make_async_copy(src, dst, w_sem.at[i]) for i, (src, dst) in enumerate(((wd_hbm, wd), (wg_hbm, wg), (wu_hbm, wu)))]
    for cp in h_loads(0) + w_loads:
        cp.start()

    def yr_load(i):
        return pltpu.make_async_copy(yr_hbm.at[pl.ds(pl.multiple_of(i * 256, 256), 256), :], yr.at[i % 2], g_sem.at[i % 2])

    yr_load(0).start()

    barrier = pltpu.get_barrier_semaphore()
    for k in PEERS:
        pl.semaphore_signal(barrier, inc=1, device_id={"ep": (me + k) % GROUP})

    idx, slots, gates = idx_t[...], slot_t[...], gate_t[...]
    for e in range(n_exp):
        hit = idx == e
        slot = jnp.max(jnp.where(hit, slots, -1), axis=0, keepdims=True)
        slot = jnp.where(slot < counts[0, e], slot, -1)
        meta_out[e // 4, e % 4] = slot.astype(F32)
        meta_out[e // 4, 4 + e % 4] = jnp.sum(jnp.where(hit, gates, 0.0), axis=0, keepdims=True)
    pl.semaphore_wait(barrier, 15)

    part_rows = gy.shape[0] // 2

    def part(p):
        return pl.ds(p * part_rows, part_rows)

    def put(slot, link, to, p, src=None):
        src = tok.at[slot, part(p)] if src is None else src
        return pltpu.make_async_remote_copy(src_ref=src, dst_ref=tok.at[slot, part(p)], send_sem=send.at[slot, link, p], recv_sem=recv.at[slot, p], device_id={"ep": to})

    def arrive(slot, p):
        put(slot, 0, me, p).wait_recv()

    def meta_copy(k):
        to = (me + k) % GROUP
        return pltpu.make_async_remote_copy(src_ref=meta_out.at[to // 2], dst_ref=meta.at[me], send_sem=m_send.at[k], recv_sem=m_recv.at[me], device_id={"ep": to})

    own = [(put(me, link, to, p, gy.at[part(p)]), cond) for p in HALVES for link, to, cond in ((ONWARD, up, None), (DOWN, down, mid), (CROSS, ynb, None), (CORE, sib, None))]
    for cp, cond in own:
        cp.start() if cond is None else pl.when(cond)(cp.start)
    for k in PEERS:
        meta_copy(k).start()
    tok[me] = gy[...]
    meta[me] = meta_out[me // 2]
    acc[...] = jnp.zeros_like(acc)

    gg[...] = jnp.zeros_like(gg)

    def gate_block(i, _):
        yr_load(i).wait()

        @pl.when(i < 7)
        def _():
            yr_load(i + 1).start()

        base = pl.multiple_of((i // 4) * 128, 128)
        prod = dot_nt(yr[i % 2], gy[pl.ds(base, 128), :]).reshape(32, 8, 128)
        t = lax.broadcasted_iota(jnp.int32, prod.shape, 0) + (i % 4) * 32
        mine = t == lax.broadcasted_iota(jnp.int32, prod.shape, 2)
        gg[:, pl.ds(base, 128)] += jnp.sum(jnp.where(mine, prod, 0.0), axis=0)
        return 0

    lax.fori_loop(0, 8, gate_block, 0)
    for cp in w_loads:
        cp.wait()

    def home(d, other, h):
        return mirror(z, d) * 4 + (y + other * (1 - 2 * y)) * 2 + h

    def relay(d, other, p, links):
        slot = home(d, other, c)
        arrive(slot, p)
        for link in links:
            put(slot, link, ynb if link == CROSS else sib if link == CORE else up if d == Z0 else down, p).start()

    def y_arrival(d, p, onward=False):
        slot = home(d, 1, c)
        arrive(slot, p)
        if onward:
            put(slot, ONWARD, up, p).start()
        put(slot, CORE, sib, p).start()

    def z_base(d, other, h):
        return mirror(z, d) * 2 + h if other == 0 else 7 + mirror(z, d)

    def z_slot(d, other, h, leftward, to_z):
        return jnp.where(leftward & (mirror(z, d) == to_z), 12 if other else 10 + h, z_base(d, other, h))

    def z_copy(d, other, h, p, step):
        dst = z_slot(d, other, h, step < 0, z + step)
        return pltpu.make_async_remote_copy(src_ref=tot.at[home(d, other, h), part(p)], dst_ref=z_in.at[dst, part(p)], send_sem=zs_sem.at[z_base(d, other, h), p], recv_sem=zr_sem.at[dst, p], device_id={"ep": (me + 4 * step + GROUP) % GROUP})

    def z_add(d, other, h, p, step):
        src, w = z_slot(d, other, h, step < 0, z), home(d, other, h)
        pltpu.make_async_remote_copy(src_ref=tot.at[w, part(p)], dst_ref=z_in.at[src, part(p)], send_sem=zs_sem.at[z_base(d, other, h), p], recv_sem=zr_sem.at[src, p], device_id={"ep": me}).wait_recv()
        tot[w, part(p)] = tot[w, part(p)] + z_in[src, part(p)]

    def y_copy(d, h, p):
        i = mirror(z, d) * 2 + h
        return pltpu.make_async_remote_copy(src_ref=tot.at[home(d, 1, h), part(p)], dst_ref=y_in.at[i, part(p)], send_sem=ys.at[i, p], recv_sem=yrs.at[i, p], device_id={"ep": ynb})

    def y_add(d, h, p):
        y_copy(d, h, p).wait_recv()
        w = home(d, 0, h)
        tot[w, part(p)] = tot[w, part(p)] + y_in[mirror(z, d) * 2 + h, part(p)]

    def y_start(d, h):
        for p in HALVES:
            y_copy(d, h, p).start()

    def start_up(d, other, h):
        for p in HALVES:
            z_copy(d, other, h, p, way).start()

    def pass_up(d, other, h, p):
        z_add(d, other, h, p, way)
        z_copy(d, other, h, p, way).start()

    def y_up(d, h, p):
        y_add(d, h, p)
        z_copy(d, OWN, h, p, way).start()

    def y_chain(d, h, p):
        y_add(d, h, p)
        pass_up(d, OWN, h, p)

    def y_down(d, h, p):
        y_add(d, h, p)
        z_add(d, OWN, h, p, -way)
        z_copy(d, OWN, h, p, -way).start()

    def swap(chip, slot, e):
        return pltpu.make_async_remote_copy(src_ref=r_send.at[slot, e], dst_ref=r_recv.at[chip, e], send_sem=rs.at[chip, e], recv_sem=rr.at[chip, e], device_id={"ep": sib})

    def build_rows(chip, e):
        for h in CORES:
            s = chip * 2 + h
            hot = one_hot(meta[s, c * 2 + e], cap)
            gate = jnp.sum(jnp.where(hot, meta[s, 4 + c * 2 + e], 0.0), axis=1, keepdims=True)
            picked = jnp.dot(jnp.where(hot, 1.0, 0.0).astype(BF16), tok[s], preferred_element_type=F32)
            d_ref[h * cap:(h + 1) * cap, :] = (picked * gate).astype(BF16)

    def make(t):
        slot = t % 2
        d, yy = chip_of(t)
        chip = d * 2 + yy
        for h in CORES:
            src = chip * 2 + h

            def table(src=src):
                pltpu.make_async_remote_copy(src_ref=meta_out.at[0], dst_ref=meta.at[src], send_sem=m_send.at[0], recv_sem=m_recv.at[src], device_id={"ep": src}).wait_recv()

            table() if t else pl.when(src != me)(table)
        for p in HALVES:
            arrive(chip * 2 + 1 - c, p)
        rows = rows_of(chip)
        for cp in h_loads(t):
            cp.wait()
        if t < 7:
            for cp in h_loads(t + 1):
                cp.start()

        def per_expert(e, _):
            build_rows(chip, e)
            g = dot_nt(d_ref[...], wd[e]).astype(BF16).astype(F32)
            h1 = hbuf[t % 2, 0, e].astype(F32)
            h3 = hbuf[t % 2, 1, e].astype(F32)
            sig = jax.nn.sigmoid(h1)
            act = h1 * sig
            dh1[e, rows, :] = (g * h3 * sig * (1.0 + h1 * (1.0 - sig))).astype(BF16)
            dh3[e, rows, :] = (g * act).astype(BF16)

            def ret_rows(side):
                cols = pl.ds(pl.multiple_of(side * half, half), half)
                return (dot_nt(dh1[e, rows, :], wg[e, cols, :]) + dot_nt(dh3[e, rows, :], wu[e, cols, :])).astype(BF16)

            r_send[slot, e] = ret_rows(1 - c)
            swap(chip, slot, e).start()
            r_own[slot, e] = ret_rows(c)
            return 0

        lax.fori_loop(0, n_loc, per_expert, 0)

    def combine(t):
        slot = t % 2
        d, yy = chip_of(t)
        chip = d * 2 + yy
        for e in range(n_loc):
            swap(chip, slot, e).wait_recv()
        for h in CORES:
            s = chip * 2 + h
            lanes = pl.ds(h * cap, cap)
            ids = (c * 2, c * 2 + 1, 2 - c * 2, 3 - c * 2)
            pick = jnp.concatenate([jnp.where(one_hot(meta[s, i], cap), 1.0, 0.0).astype(BF16) for i in ids], axis=0)
            vals = jnp.concatenate([r_own[slot, 0, lanes, :], r_own[slot, 1, lanes, :], r_recv[chip, 0, lanes, :], r_recv[chip, 1, lanes, :]], axis=0)
            tot[s] = dot_tn(pick, vals)
        for e in range(n_loc):
            swap(chip, slot, e).wait_send()

    def at_end(fn):
        pl.when(end)(fn)

    def at_mid(fn):
        pl.when(mid)(fn)

    make(0)
    combine(0)

    @at_end
    def _():
        for p in HALVES:
            y_arrival(Z0, p, True)
            relay(Z1, OWN, p, (CROSS, CORE))

    @at_mid
    def _():
        for p in HALVES:
            relay(Z0, OWN, p, (ONWARD, CORE))
            y_arrival(Z1, p)
            relay(Z2, OWN, p, (ONWARD, CROSS, CORE))

    def second(p):
        @at_end
        def _():
            y_arrival(Z1, p)
            relay(Z2, OWN, p, (CROSS, CORE))

        @at_mid
        def _():
            relay(Z0, OTHER, p, (ONWARD, CORE))
            y_arrival(Z2, p)
            relay(Z3, OWN, p, (ONWARD, CORE))

    def third(p):
        @at_end
        def _():
            y_arrival(Z2, p)
            relay(Z3, OWN, p, (CORE,))

        @at_mid
        def _():
            relay(Z3, OTHER, p, (ONWARD, CORE))

    make(1)
    make(2)
    second(LO)
    combine(1)
    combine(2)
    at_end(lambda: start_up(Z1, OWN, CORE0))
    second(HI)
    make(3)
    make(4)
    third(LO)
    combine(3)
    y_start(Z1, CORE1)
    combine(4)
    at_end(lambda: start_up(Z2, OWN, CORE0))
    at_mid(lambda: y_start(Z0, CORE0))
    third(HI)
    make(5)
    make(6)
    at_end(lambda: relay(Z3, OTHER, LO, (CORE,)))
    combine(5)

    @at_end
    def _():
        start_up(Z2, OTHER, CORE0)
        y_start(Z2, CORE1)

    combine(6)
    at_end(lambda: relay(Z3, OTHER, HI, (CORE,)))
    at_mid(lambda: pass_up(Z2, OWN, CORE0, LO))
    make(7)
    combine(7)
    y_start(Z3, CORE0)
    y_start(Z3, CORE1)
    at_end(lambda: y_start(Z0, CORE0))
    y_start(Z0, CORE1)
    at_mid(lambda: y_start(Z2, CORE1))

    width = xs.shape[2]

    def x_load(i):
        e, t = i // 4, i % 4
        return pltpu.make_async_copy(x_hbm.at[e, :, pl.ds(pl.multiple_of(t * width, width), width)], xs.at[i % 2], x_sem.at[i % 2])

    def w_out(i):
        e, t = i // 4, i % 4
        rows = pl.ds(pl.multiple_of(t * width, width), width)
        return (pltpu.make_async_copy(og.at[i % 2], gwg_hbm.at[e, rows, :], st_sem.at[i % 2, 0]),
                pltpu.make_async_copy(ou.at[i % 2], gwu_hbm.at[e, rows, :], st_sem.at[i % 2, 1]))

    def end_tail():
        y_up(Z3, CORE1, HI)
        start_up(Z1, OTHER, CORE0)
        for p in HALVES:
            y_up(Z1, CORE1, p)

    def end_first():
        for p in HALVES:
            y_up(Z2, CORE1, p)

    end_events = dict(enumerate((end_first, lambda: y_up(Z3, CORE0, LO), lambda: y_up(Z3, CORE0, HI), lambda: y_up(Z3, CORE1, LO), end_tail)))
    mid_events = {0: lambda: pass_up(Z2, OWN, CORE0, HI), 1: lambda: pass_up(Z2, OTHER, CORE0, LO), 2: lambda: pass_up(Z2, OTHER, CORE0, HI), 6: lambda: y_chain(Z3, CORE0, LO), 7: lambda: y_chain(Z3, CORE0, HI)}
    def tail_loads(i):
        rows = rows_of(i)
        return [pltpu.make_async_copy(src.at[:, rows, :], hbuf.at[i % 2, n], h_sem.at[i % 2, n]) for n, src in enumerate((hg_hbm, hu_hbm))]

    x_load(0).start()
    for cp in tail_loads(0):
        cp.start()

    def down_grad(i):
        for cp in tail_loads(i):
            cp.wait()

        @pl.when(i < 7)
        def _():
            for cp in tail_loads(i + 1):
                cp.start()

        def per_expert(e, _):
            build_rows(i, e)
            h1 = hbuf[i % 2, 0, e].astype(F32)
            a_ref[...] = (h1 * jax.nn.sigmoid(h1) * hbuf[i % 2, 1, e].astype(F32)).astype(BF16)
            acc[e] += dot_tn(a_ref[...], d_ref[...])
            return 0

        lax.fori_loop(0, n_loc, per_expert, 0)


    def weights(i, _):
        x_load(i).wait()

        @pl.when(i < 7)
        def _():
            x_load(i + 1).start()

        @pl.when(i >= 2)
        def _():
            for cp in w_out(i - 2):
                cp.wait()

        e = i // 4
        og[i % 2] = dot_tn(xs[i % 2], dh1[e])
        ou[i % 2] = dot_tn(xs[i % 2], dh3[e])
        for cp in w_out(i):
            cp.start()
        down_grad(i)
        for n, event in mid_events.items():
            pl.when(mid & (i == n))(event)
        for n, event in end_events.items():
            pl.when(end & (i == n))(event)
        return 0

    lax.fori_loop(0, 8, weights, 0)
    acc_out = pltpu.make_async_copy(acc, gwd_hbm, acc_sem.at[0])
    acc_out.start()

    def cross(p):
        z_add(Z1, OTHER, CORE0, p, -way)
        z_add(Z1, OTHER, CORE0, p, way)
        y_copy(Z1, CORE0, p).start()

    @at_mid
    def _():
        y_down(Z0, CORE0, LO)
        y_chain(Z3, CORE1, LO)
        y_down(Z0, CORE0, HI)
        y_chain(Z3, CORE1, HI)
        y_down(Z0, CORE1, LO)
        cross(0)
        y_chain(Z2, CORE1, LO)
        y_down(Z0, CORE1, HI)
        cross(1)
        y_chain(Z2, CORE1, HI)

    def last(p):
        return pltpu.make_async_remote_copy(src_ref=f_send.at[part(p)], dst_ref=f_recv.at[part(p)], send_sem=fs.at[p], recv_sem=fr.at[p], device_id={"ep": sib})

    def finish(h, p):
        w = me - c + h
        i = z * 2 + h
        pltpu.make_async_remote_copy(src_ref=tot.at[w, part(p)], dst_ref=y_in.at[i, part(p)], send_sem=ys.at[i, p], recv_sem=yrs.at[i, p], device_id={"ep": ynb}).wait_recv()
        tot[w, part(p)] = tot[w, part(p)] + y_in[i, part(p)]
        at_end(lambda: z_add(Z0, OWN, h, p, -way))

        @at_mid
        def _():
            z_add(Z1, OWN, h, p, -way)
            z_add(Z1, OWN, h, p, way)

        @pl.when(c == h)
        def _():
            gx[part(p), h * half:(h + 1) * half] = tot[w, part(p)].astype(BF16)

        @pl.when(c != h)
        def _():
            f_send[part(p)] = tot[w, part(p)].astype(BF16)
            last(p).start()

    for p in HALVES:
        for h in CORES:
            finish(h, p)
    for p in HALVES:
        last(p).wait()
    for h in CORES:
        @pl.when(c == h)
        def _():
            gx[:, (1 - h) * half:(2 - h) * half] = f_recv[...]

    for cp, cond in own:
        cp.wait_send() if cond is None else pl.when(cond)(cp.wait_send)

    def drain(tokens, y_units, z_units):
        for p in HALVES:
            for d, other, links in tokens:
                for link in links:
                    put(home(d, other, c), link, me, p).wait_send()
            for d, h in y_units:
                y_copy(d, h, p).wait_send()
            for d, other, h in z_units:
                z_copy(d, other, h, p, way).wait_send()

    SENT = (CORE,)
    at_end(lambda: drain(
        ((Z0, OTHER, (ONWARD, CORE)), (Z1, OWN, (CROSS, CORE)), (Z1, OTHER, SENT), (Z2, OWN, (CROSS, CORE)), (Z2, OTHER, SENT), (Z3, OWN, SENT), (Z3, OTHER, SENT)),
        ((Z0, CORE0), (Z0, CORE1), (Z1, CORE1), (Z2, CORE1), (Z3, CORE0), (Z3, CORE1)),
        ((Z1, OWN, CORE0), (Z1, OTHER, CORE0), (Z2, OWN, CORE0), (Z2, OTHER, CORE0), (Z1, OWN, CORE1), (Z2, OWN, CORE1), (Z3, OWN, CORE0), (Z3, OWN, CORE1))))
    at_mid(lambda: drain(
        ((Z1, OTHER, SENT), (Z0, OWN, (ONWARD, CORE)), (Z0, OTHER, (ONWARD, CORE)), (Z2, OWN, (ONWARD, CROSS, CORE)), (Z2, OTHER, SENT), (Z3, OWN, (ONWARD, CORE)), (Z3, OTHER, (ONWARD, CORE))),
        ((Z0, CORE0), (Z0, CORE1), (Z1, CORE0), (Z1, CORE1), (Z2, CORE1), (Z3, CORE0), (Z3, CORE1)),
        ((Z2, OWN, CORE0), (Z2, OTHER, CORE0), (Z3, OWN, CORE0), (Z3, OWN, CORE1), (Z0, OWN, CORE0), (Z0, OWN, CORE1), (Z2, OWN, CORE1))))
    for k in PEERS:
        meta_copy(k).wait_send()
    for i in (6, 7):
        for cp in w_out(i):
            cp.wait()
    acc_out.wait()


def deliver_kernel(*refs):
    n = (len(refs) - 2) // 3
    src, dst, buf, (in_sem, out_sem) = refs[:n], refs[n:2 * n], refs[2 * n:3 * n], refs[3 * n:]
    pieces = []
    for s, d, b in zip(src, dst, buf):
        rows = s.shape[-2]
        parts = 2 if len(s.shape) == 3 else 1
        for lead in ([(e,) for e in range(s.shape[0])] if len(s.shape) == 3 else [()]):
            for k in range(parts):
                at = lead + (pl.ds(k * rows // parts, rows // parts),)
                i = len(pieces)
                pieces.append((pltpu.make_async_copy(s.at[at], b.at[at], in_sem.at[i]), pltpu.make_async_copy(b.at[at], d.at[at], out_sem.at[i])))
    for read, _ in pieces:
        read.start()
    for read, write in pieces:
        read.wait()
        write.start()
    for _, write in pieces:
        write.wait()


def deliver(arrays):
    n = 2 + 4 * (len(arrays) - 2)
    return pl.pallas_call(
        deliver_kernel,
        out_shape=tuple(jax.ShapeDtypeStruct(a.shape, a.dtype) for a in arrays),
        in_specs=[ANY] * len(arrays),
        out_specs=(ANY,) * len(arrays),
        scratch_shapes=[VMEM(a.shape, a.dtype) for a in arrays] + [DMA((n,)), DMA((n,))],
        compiler_params=pltpu.CompilerParams(vmem_limit_bytes=67043328),
        name="deliver",
    )(*arrays)


def solution(mesh):
    rows_spec = P(("dp", "ep"), None)
    cube_spec = P(("dp", "ep"), None, None)
    weight_spec = P("ep", None, None)

    def local_step(grad_y, gate_vals, topk_idx, slot_ids, pair_counts, y_routed, x_disp, h_gate, h_up, w_gate, w_up, w_down):
        n_loc, n_rows, ffn = h_gate.shape
        tok, dim = grad_y.shape
        top_k = topk_idx.shape[1]
        half = dim // 2
        cap = n_rows // 16
        shape = jax.ShapeDtypeStruct
        grad_x, grad_gate, grad_wdown, grad_wgate, grad_wup = pl.pallas_call(
            step_kernel,
            out_shape=(shape((tok, dim), BF16), shape((top_k, tok), F32), shape((n_loc, ffn, dim), F32), shape((n_loc, dim, ffn), F32), shape((n_loc, dim, ffn), F32)),
            in_specs=[VM, VM, VM, VM, pl.BlockSpec(memory_space=pltpu.SMEM)] + [ANY] * 7,
            out_specs=(VM, VM, ANY, ANY, ANY),
            scratch_shapes=[
                VMEM((16, tok, dim), BF16), VMEM((16, 8, 1, tok), F32), VMEM((8, 8, 1, tok), F32),
                VMEM((2, 2, n_loc, 2 * cap, ffn), BF16),
                VMEM((n_loc, ffn, dim), BF16), VMEM((n_loc, dim, ffn), BF16), VMEM((n_loc, dim, ffn), BF16),
                VMEM((2, n_rows, 256), BF16), VMEM((2, 256, dim), BF16),
                VMEM((2 * cap, dim), BF16), VMEM((2 * cap, ffn), BF16),
                VMEM((n_loc, n_rows, ffn), BF16), VMEM((n_loc, n_rows, ffn), BF16), VMEM((n_loc, ffn, dim), F32),
                VMEM((2, n_loc, 2 * cap, half), BF16), VMEM((2, n_loc, 2 * cap, half), BF16), VMEM((8, n_loc, 2 * cap, half), BF16),
                VMEM((16, tok, half), F32), VMEM((13, tok, half), F32), VMEM((8, tok, half), F32),
                VMEM((tok, half), BF16), VMEM((tok, half), BF16),
                VMEM((2, 256, ffn), F32), VMEM((2, 256, ffn), F32),
                DMA((3,)), DMA((2, 2)), DMA((2,)), DMA((2,)), DMA((2, 2)), DMA((1,)),
                DMA((16, 4, 2)), DMA((16, 2)), DMA((16,)), DMA((16,)), DMA((8, n_loc)), DMA((8, n_loc)), DMA((8, 2)), DMA((8, 2)), DMA((10, 2)), DMA((13, 2)), DMA((2,)), DMA((2,)),
            ],
            compiler_params=pltpu.CompilerParams(collective_id=1, has_side_effects=True, vmem_limit_bytes=67043328),
            name="step",
        )(grad_y, topk_idx.T, slot_ids.T, gate_vals.T, pair_counts, y_routed.reshape(tok * top_k, dim), h_gate, h_up, w_down, w_gate, w_up, x_disp)
        grad_wgate, grad_wup, grad_wdown, grad_x, grad_gate = deliver((grad_wgate, grad_wup, grad_wdown, grad_x, grad_gate))
        return grad_x, grad_gate.T, grad_wgate, grad_wup, grad_wdown

    return jax.shard_map(local_step, mesh=mesh, in_specs=(rows_spec, rows_spec, rows_spec, rows_spec, rows_spec, cube_spec, cube_spec, cube_spec, cube_spec, weight_spec, weight_spec, weight_spec), out_specs=(rows_spec, rows_spec, cube_spec, cube_spec, cube_spec), check_vma=False)
```

```python
import jax
import jax.numpy as jnp
from jax import lax
from jax.experimental import pallas as pl
from jax.experimental.pallas import tpu as pltpu
from jax.sharding import PartitionSpec as P

F32 = jnp.float32
BF16 = jnp.bfloat16
VMEM = pltpu.VMEM
DMA = pltpu.SemaphoreType.DMA
Z0, Z1, Z2, Z3 = range(4)
OWN, OTHER = CORE0, CORE1 = LO, HI = CORES = HALVES = range(2)
ONWARD, DOWN, CROSS, CORE = range(4)
NZ, GROUP = 4, 16
PEERS = range(1, GROUP)
ANY = pl.BlockSpec(memory_space=pl.ANY)
VM = pl.BlockSpec(memory_space=pltpu.VMEM)


def position():
    me = lax.axis_index("ep")
    return me, me // 4, (me // 2) % 2, me % 2


def mirror(z, v):
    return v + (z // 2) * (3 - 2 * v)


def dot_nt(a, b):
    return lax.dot_general(a, b, (((1,), (1,)), ((), ())), preferred_element_type=F32)


def dot_tn(a, b):
    return lax.dot_general(a, b, (((0,), (0,)), ((), ())), preferred_element_type=F32)


def one_hot(slot, cap):
    return slot == lax.broadcasted_iota(jnp.int32, (cap, slot.shape[1]), 0).astype(F32)


def step_kernel(gy_hbm, idx_hbm, slot_hbm, gate_hbm, counts_hbm, yr_hbm, hg_hbm, hu_hbm, wd_hbm, wg_hbm, wu_hbm, x_hbm, gx, gg, gwd_hbm, gwg_hbm, gwu_hbm,
                gy, idx_t, slot_t, gate_t, counts, tok, meta, meta_out, hbuf, wd, wg, wu, xs, yr, d_ref, a_ref, dh1, dh3, acc, r_own, r_send, r_recv, tot, z_in, y_in, f_send, f_recv, og, ou,
                in_sem, w_sem, h_sem, x_sem, g_sem, st_sem, acc_sem, send, recv, m_send, m_recv, rs, rr, ys, yrs, zs_sem, zr_sem, fs, fr):
    me, z, y, c = position()
    n_loc, n_rows, ffn = dh1.shape
    cap = n_rows // 16
    half = r_own.shape[3]
    n_exp = counts.shape[1]
    sib = me + 1 - 2 * c
    ynb = me + 2 - 4 * y
    m = z // 2
    q = mirror(z, z)
    way = 1 - 2 * m
    end = q == 0
    mid = q == 1
    up = (me + 4 * way + GROUP) % GROUP
    down = (me - 4 * way + GROUP) % GROUP

    barrier = pltpu.get_barrier_semaphore()
    for k in PEERS:
        pl.semaphore_signal(barrier, inc=1, device_id={"ep": (me + k) % GROUP})
    inputs = [pltpu.make_async_copy(src, dst, in_sem.at[i]) for i, (src, dst) in enumerate(((gy_hbm, gy), (idx_hbm, idx_t), (slot_hbm, slot_t), (gate_hbm, gate_t), (counts_hbm, counts)))]
    for cp in inputs:
        cp.start()

    order = (((Z0, OWN), (Z1, OWN)), ((Z0, OTHER), (Z0, OWN)), ((Z1, OWN), (Z2, OWN)), ((Z1, OTHER), (Z1, OTHER)), ((Z2, OWN), (Z0, OTHER)), ((Z2, OTHER), (Z3, OWN)), ((Z3, OWN), (Z2, OTHER)), ((Z3, OTHER), (Z3, OTHER)))

    def chip_of(t):
        (d_end, o_end), (d_mid, o_mid) = order[t]
        other = o_end + q * (o_mid - o_end)
        return mirror(z, d_end + q * (d_mid - d_end)), y + other * (1 - 2 * y)

    def rows_of(chip):
        return pl.ds(pl.multiple_of(chip * 2 * cap, 2 * cap), 2 * cap)

    def h_loads(t):
        d, yy = chip_of(t)
        rows = rows_of(d * 2 + yy)
        return [pltpu.make_async_copy(src.at[:, rows, :], hbuf.at[t % 2, i], h_sem.at[t % 2, i]) for i, src in enumerate((hg_hbm, hu_hbm))]

    w_loads = [pltpu.make_async_copy(src, dst, w_sem.at[i]) for i, (src, dst) in enumerate(((wd_hbm, wd), (wg_hbm, wg), (wu_hbm, wu)))]
    def yr_load(i):
        return pltpu.make_async_copy(yr_hbm.at[pl.ds(pl.multiple_of(i * 256, 256), 256), :], yr.at[i % 2], g_sem.at[i % 2])


    part_rows = gy.shape[0] // 2

    def part(p):
        return pl.ds(p * part_rows, part_rows)

    def put(slot, link, to, p, src=None):
        src = tok.at[slot, part(p)] if src is None else src
        return pltpu.make_async_remote_copy(src_ref=src, dst_ref=tok.at[slot, part(p)], send_sem=send.at[slot, link, p], recv_sem=recv.at[slot, p], device_id={"ep": to})

    def arrive(slot, p):
        put(slot, 0, me, p).wait_recv()

    def meta_copy(k):
        to = (me + k) % GROUP
        return pltpu.make_async_remote_copy(src_ref=meta_out.at[to // 2], dst_ref=meta.at[me], send_sem=m_send.at[k], recv_sem=m_recv.at[me], device_id={"ep": to})

    own = [(put(me, link, to, p, gy.at[part(p)]), cond) for p in HALVES for link, to, cond in ((ONWARD, up, None), (DOWN, down, mid), (CROSS, ynb, None), (CORE, sib, None))]
    inputs[0].wait()
    for cp in h_loads(0) + w_loads:
        cp.start()
    yr_load(0).start()
    pl.semaphore_wait(barrier, GROUP - 1)
    for cp, cond in own:
        cp.start() if cond is None else pl.when(cond)(cp.start)

    for cp in inputs[1:]:
        cp.wait()
    idx, slots, gates = idx_t[...], slot_t[...], gate_t[...]
    for e in range(n_exp):
        hit = idx == e
        slot = jnp.max(jnp.where(hit, slots, -1), axis=0, keepdims=True)
        slot = jnp.where(slot < counts[0, e], slot, -1)
        meta_out[e // 4, e % 4] = slot.astype(F32)
        meta_out[e // 4, 4 + e % 4] = jnp.sum(jnp.where(hit, gates, 0.0), axis=0, keepdims=True)
    for k in PEERS:
        meta_copy(k).start()
    tok[me] = gy[...]
    meta[me] = meta_out[me // 2]
    acc[...] = jnp.zeros_like(acc)

    gg[...] = jnp.zeros_like(gg)

    def gate_block(i, _):
        yr_load(i).wait()

        @pl.when(i < 7)
        def _():
            yr_load(i + 1).start()

        base = pl.multiple_of((i // 4) * 128, 128)
        prod = dot_nt(yr[i % 2], gy[pl.ds(base, 128), :]).reshape(32, 8, 128)
        t = lax.broadcasted_iota(jnp.int32, prod.shape, 0) + (i % 4) * 32
        mine = t == lax.broadcasted_iota(jnp.int32, prod.shape, 2)
        gg[:, pl.ds(base, 128)] += jnp.sum(jnp.where(mine, prod, 0.0), axis=0)
        return 0

    lax.fori_loop(0, 8, gate_block, 0)
    for cp in w_loads:
        cp.wait()

    def home(d, other, h):
        return mirror(z, d) * 4 + (y + other * (1 - 2 * y)) * 2 + h

    def relay(d, other, p, links):
        slot = home(d, other, c)
        arrive(slot, p)
        for link in links:
            put(slot, link, ynb if link == CROSS else sib if link == CORE else up if d == Z0 else down, p).start()

    def y_arrival(d, p, onward=False):
        slot = home(d, 1, c)
        arrive(slot, p)
        if onward:
            put(slot, ONWARD, up, p).start()
        put(slot, CORE, sib, p).start()

    def z_base(d, other, h):
        return mirror(z, d) * 2 + h if other == 0 else 7 + mirror(z, d)

    def z_slot(d, other, h, leftward, to_z):
        return jnp.where(leftward & (mirror(z, d) == to_z), 12 if other else 10 + h, z_base(d, other, h))

    def z_copy(d, other, h, p, step):
        dst = z_slot(d, other, h, step < 0, z + step)
        return pltpu.make_async_remote_copy(src_ref=tot.at[home(d, other, h), part(p)], dst_ref=z_in.at[dst, part(p)], send_sem=zs_sem.at[z_base(d, other, h), p], recv_sem=zr_sem.at[dst, p], device_id={"ep": (me + 4 * step + GROUP) % GROUP})

    def z_add(d, other, h, p, step):
        src, w = z_slot(d, other, h, step < 0, z), home(d, other, h)
        pltpu.make_async_remote_copy(src_ref=tot.at[w, part(p)], dst_ref=z_in.at[src, part(p)], send_sem=zs_sem.at[z_base(d, other, h), p], recv_sem=zr_sem.at[src, p], device_id={"ep": me}).wait_recv()
        tot[w, part(p)] = tot[w, part(p)] + z_in[src, part(p)]

    def y_copy(d, h, p):
        i = mirror(z, d) * 2 + h
        return pltpu.make_async_remote_copy(src_ref=tot.at[home(d, 1, h), part(p)], dst_ref=y_in.at[i, part(p)], send_sem=ys.at[i, p], recv_sem=yrs.at[i, p], device_id={"ep": ynb})

    def y_add(d, h, p):
        y_copy(d, h, p).wait_recv()
        w = home(d, 0, h)
        tot[w, part(p)] = tot[w, part(p)] + y_in[mirror(z, d) * 2 + h, part(p)]

    def y_start(d, h):
        for p in HALVES:
            y_copy(d, h, p).start()

    def start_up(d, other, h):
        for p in HALVES:
            z_copy(d, other, h, p, way).start()

    def pass_up(d, other, h, p):
        z_add(d, other, h, p, way)
        z_copy(d, other, h, p, way).start()

    def y_up(d, h, p):
        y_add(d, h, p)
        z_copy(d, OWN, h, p, way).start()

    def y_chain(d, h, p):
        y_add(d, h, p)
        pass_up(d, OWN, h, p)

    def y_down(d, h, p):
        y_add(d, h, p)
        z_add(d, OWN, h, p, -way)
        z_copy(d, OWN, h, p, -way).start()

    def swap(chip, slot, e):
        return pltpu.make_async_remote_copy(src_ref=r_send.at[slot, e], dst_ref=r_recv.at[chip, e], send_sem=rs.at[chip, e], recv_sem=rr.at[chip, e], device_id={"ep": sib})

    def build_rows(chip, e):
        for h in CORES:
            s = chip * 2 + h
            hot = one_hot(meta[s, c * 2 + e], cap)
            gate = jnp.sum(jnp.where(hot, meta[s, 4 + c * 2 + e], 0.0), axis=1, keepdims=True)
            picked = jnp.dot(jnp.where(hot, 1.0, 0.0).astype(BF16), tok[s], preferred_element_type=F32)
            d_ref[h * cap:(h + 1) * cap, :] = (picked * gate).astype(BF16)

    def make(t):
        slot = t % 2
        d, yy = chip_of(t)
        chip = d * 2 + yy
        for h in CORES:
            src = chip * 2 + h

            def table(src=src):
                pltpu.make_async_remote_copy(src_ref=meta_out.at[0], dst_ref=meta.at[src], send_sem=m_send.at[0], recv_sem=m_recv.at[src], device_id={"ep": src}).wait_recv()

            table() if t else pl.when(src != me)(table)
        for p in HALVES:
            arrive(chip * 2 + 1 - c, p)
        rows = rows_of(chip)
        for cp in h_loads(t):
            cp.wait()
        if t < 7:
            for cp in h_loads(t + 1):
                cp.start()

        def per_expert(e, _):
            build_rows(chip, e)
            g = dot_nt(d_ref[...], wd[e]).astype(BF16).astype(F32)
            h1 = hbuf[t % 2, 0, e].astype(F32)
            h3 = hbuf[t % 2, 1, e].astype(F32)
            sig = jax.nn.sigmoid(h1)
            act = h1 * sig
            dh1[e, rows, :] = (g * h3 * sig * (1.0 + h1 * (1.0 - sig))).astype(BF16)
            dh3[e, rows, :] = (g * act).astype(BF16)

            def ret_rows(side):
                cols = pl.ds(pl.multiple_of(side * half, half), half)
                return (dot_nt(dh1[e, rows, :], wg[e, cols, :]) + dot_nt(dh3[e, rows, :], wu[e, cols, :])).astype(BF16)

            r_send[slot, e] = ret_rows(1 - c)
            swap(chip, slot, e).start()
            r_own[slot, e] = ret_rows(c)
            return 0

        lax.fori_loop(0, n_loc, per_expert, 0)

    def combine(t):
        slot = t % 2
        d, yy = chip_of(t)
        chip = d * 2 + yy
        for e in range(n_loc):
            swap(chip, slot, e).wait_recv()
        for h in CORES:
            s = chip * 2 + h
            lanes = pl.ds(h * cap, cap)
            ids = (c * 2, c * 2 + 1, 2 - c * 2, 3 - c * 2)
            pick = jnp.concatenate([jnp.where(one_hot(meta[s, i], cap), 1.0, 0.0).astype(BF16) for i in ids], axis=0)
            vals = jnp.concatenate([r_own[slot, 0, lanes, :], r_own[slot, 1, lanes, :], r_recv[chip, 0, lanes, :], r_recv[chip, 1, lanes, :]], axis=0)
            tot[s] = dot_tn(pick, vals)
        for e in range(n_loc):
            swap(chip, slot, e).wait_send()

    def at_end(fn):
        pl.when(end)(fn)

    def at_mid(fn):
        pl.when(mid)(fn)

    make(0)
    combine(0)

    @at_end
    def _():
        for p in HALVES:
            y_arrival(Z0, p, True)
            relay(Z1, OWN, p, (CROSS, CORE))

    @at_mid
    def _():
        for p in HALVES:
            relay(Z0, OWN, p, (ONWARD, CORE))
            y_arrival(Z1, p)
            relay(Z2, OWN, p, (ONWARD, CROSS, CORE))

    def second(p):
        @at_end
        def _():
            y_arrival(Z1, p)
            relay(Z2, OWN, p, (CROSS, CORE))

        @at_mid
        def _():
            relay(Z0, OTHER, p, (ONWARD, CORE))
            y_arrival(Z2, p)
            relay(Z3, OWN, p, (ONWARD, CORE))

    def third(p):
        @at_end
        def _():
            y_arrival(Z2, p)
            relay(Z3, OWN, p, (CORE,))

        @at_mid
        def _():
            relay(Z3, OTHER, p, (ONWARD, CORE))

    make(1)
    make(2)
    second(LO)
    combine(1)
    combine(2)
    at_end(lambda: start_up(Z1, OWN, CORE0))
    second(HI)
    make(3)
    make(4)
    third(LO)
    combine(3)
    y_start(Z1, CORE1)
    combine(4)
    at_end(lambda: start_up(Z2, OWN, CORE0))
    at_mid(lambda: y_start(Z0, CORE0))
    third(HI)
    make(5)
    make(6)
    at_end(lambda: relay(Z3, OTHER, LO, (CORE,)))
    combine(5)

    @at_end
    def _():
        start_up(Z2, OTHER, CORE0)
        y_start(Z2, CORE1)

    combine(6)
    at_end(lambda: relay(Z3, OTHER, HI, (CORE,)))
    at_mid(lambda: pass_up(Z2, OWN, CORE0, LO))
    make(7)
    combine(7)
    y_start(Z3, CORE0)
    y_start(Z3, CORE1)
    at_end(lambda: y_start(Z0, CORE0))
    y_start(Z0, CORE1)
    at_mid(lambda: y_start(Z2, CORE1))

    width = xs.shape[2]

    def x_load(i):
        e, t = i // 4, i % 4
        return pltpu.make_async_copy(x_hbm.at[e, :, pl.ds(pl.multiple_of(t * width, width), width)], xs.at[i % 2], x_sem.at[i % 2])

    def w_out(i):
        e, t = i // 4, i % 4
        rows = pl.ds(pl.multiple_of(t * width, width), width)
        return (pltpu.make_async_copy(og.at[i % 2], gwg_hbm.at[e, rows, :], st_sem.at[i % 2, 0]),
                pltpu.make_async_copy(ou.at[i % 2], gwu_hbm.at[e, rows, :], st_sem.at[i % 2, 1]))

    def end_tail():
        y_up(Z3, CORE1, HI)
        start_up(Z1, OTHER, CORE0)
        for p in HALVES:
            y_up(Z1, CORE1, p)

    def end_first():
        for p in HALVES:
            y_up(Z2, CORE1, p)

    end_events = dict(enumerate((end_first, lambda: y_up(Z3, CORE0, LO), lambda: y_up(Z3, CORE0, HI), lambda: y_up(Z3, CORE1, LO), end_tail)))
    mid_events = {0: lambda: pass_up(Z2, OWN, CORE0, HI), 1: lambda: pass_up(Z2, OTHER, CORE0, LO), 2: lambda: pass_up(Z2, OTHER, CORE0, HI), 6: lambda: y_chain(Z3, CORE0, LO), 7: lambda: y_chain(Z3, CORE0, HI)}
    def tail_loads(i):
        rows = rows_of(i)
        return [pltpu.make_async_copy(src.at[:, rows, :], hbuf.at[i % 2, n], h_sem.at[i % 2, n]) for n, src in enumerate((hg_hbm, hu_hbm))]

    x_load(0).start()
    for cp in tail_loads(0):
        cp.start()

    def down_grad(i):
        for cp in tail_loads(i):
            cp.wait()

        @pl.when(i < 7)
        def _():
            for cp in tail_loads(i + 1):
                cp.start()

        def per_expert(e, _):
            build_rows(i, e)
            h1 = hbuf[i % 2, 0, e].astype(F32)
            a_ref[...] = (h1 * jax.nn.sigmoid(h1) * hbuf[i % 2, 1, e].astype(F32)).astype(BF16)
            acc[e] += dot_tn(a_ref[...], d_ref[...])
            return 0

        lax.fori_loop(0, n_loc, per_expert, 0)


    def weights(i, _):
        x_load(i).wait()

        @pl.when(i < 7)
        def _():
            x_load(i + 1).start()

        @pl.when(i >= 2)
        def _():
            for cp in w_out(i - 2):
                cp.wait()

        e = i // 4
        og[i % 2] = dot_tn(xs[i % 2], dh1[e])
        ou[i % 2] = dot_tn(xs[i % 2], dh3[e])
        for cp in w_out(i):
            cp.start()
        down_grad(i)
        for n, event in mid_events.items():
            pl.when(mid & (i == n))(event)
        for n, event in end_events.items():
            pl.when(end & (i == n))(event)
        return 0

    lax.fori_loop(0, 8, weights, 0)
    acc_out = pltpu.make_async_copy(acc, gwd_hbm, acc_sem.at[0])
    acc_out.start()

    def cross(p):
        z_add(Z1, OTHER, CORE0, p, -way)
        z_add(Z1, OTHER, CORE0, p, way)
        y_copy(Z1, CORE0, p).start()

    @at_mid
    def _():
        y_down(Z0, CORE0, LO)
        y_chain(Z3, CORE1, LO)
        y_down(Z0, CORE0, HI)
        y_chain(Z3, CORE1, HI)
        y_down(Z0, CORE1, LO)
        cross(0)
        y_chain(Z2, CORE1, LO)
        y_down(Z0, CORE1, HI)
        cross(1)
        y_chain(Z2, CORE1, HI)

    def last(p):
        return pltpu.make_async_remote_copy(src_ref=f_send.at[part(p)], dst_ref=f_recv.at[part(p)], send_sem=fs.at[p], recv_sem=fr.at[p], device_id={"ep": sib})

    def finish(h, p):
        w = me - c + h
        i = z * 2 + h
        pltpu.make_async_remote_copy(src_ref=tot.at[w, part(p)], dst_ref=y_in.at[i, part(p)], send_sem=ys.at[i, p], recv_sem=yrs.at[i, p], device_id={"ep": ynb}).wait_recv()
        tot[w, part(p)] = tot[w, part(p)] + y_in[i, part(p)]
        at_end(lambda: z_add(Z0, OWN, h, p, -way))

        @at_mid
        def _():
            z_add(Z1, OWN, h, p, -way)
            z_add(Z1, OWN, h, p, way)

        @pl.when(c == h)
        def _():
            gx[part(p), h * half:(h + 1) * half] = tot[w, part(p)].astype(BF16)

        @pl.when(c != h)
        def _():
            f_send[part(p)] = tot[w, part(p)].astype(BF16)
            last(p).start()

    for p in HALVES:
        for h in CORES:
            finish(h, p)
    for p in HALVES:
        last(p).wait()
    for h in CORES:
        @pl.when(c == h)
        def _():
            gx[:, (1 - h) * half:(2 - h) * half] = f_recv[...]

    for cp, cond in own:
        cp.wait_send() if cond is None else pl.when(cond)(cp.wait_send)

    def drain(tokens, y_units, z_units):
        for p in HALVES:
            for d, other, links in tokens:
                for link in links:
                    put(home(d, other, c), link, me, p).wait_send()
            for d, h in y_units:
                y_copy(d, h, p).wait_send()
            for d, other, h in z_units:
                z_copy(d, other, h, p, way).wait_send()

    SENT = (CORE,)
    at_end(lambda: drain(
        ((Z0, OTHER, (ONWARD, CORE)), (Z1, OWN, (CROSS, CORE)), (Z1, OTHER, SENT), (Z2, OWN, (CROSS, CORE)), (Z2, OTHER, SENT), (Z3, OWN, SENT), (Z3, OTHER, SENT)),
        ((Z0, CORE0), (Z0, CORE1), (Z1, CORE1), (Z2, CORE1), (Z3, CORE0), (Z3, CORE1)),
        ((Z1, OWN, CORE0), (Z1, OTHER, CORE0), (Z2, OWN, CORE0), (Z2, OTHER, CORE0), (Z1, OWN, CORE1), (Z2, OWN, CORE1), (Z3, OWN, CORE0), (Z3, OWN, CORE1))))
    at_mid(lambda: drain(
        ((Z1, OTHER, SENT), (Z0, OWN, (ONWARD, CORE)), (Z0, OTHER, (ONWARD, CORE)), (Z2, OWN, (ONWARD, CROSS, CORE)), (Z2, OTHER, SENT), (Z3, OWN, (ONWARD, CORE)), (Z3, OTHER, (ONWARD, CORE))),
        ((Z0, CORE0), (Z0, CORE1), (Z1, CORE0), (Z1, CORE1), (Z2, CORE1), (Z3, CORE0), (Z3, CORE1)),
        ((Z2, OWN, CORE0), (Z2, OTHER, CORE0), (Z3, OWN, CORE0), (Z3, OWN, CORE1), (Z0, OWN, CORE0), (Z0, OWN, CORE1), (Z2, OWN, CORE1))))
    for k in PEERS:
        meta_copy(k).wait_send()
    for i in (6, 7):
        for cp in w_out(i):
            cp.wait()
    acc_out.wait()


def deliver_kernel(*refs):
    n = (len(refs) - 2) // 3
    src, dst, buf, (in_sem, out_sem) = refs[:n], refs[n:2 * n], refs[2 * n:3 * n], refs[3 * n:]
    pieces = []
    for s, d, b in zip(src, dst, buf):
        rows = s.shape[-2]
        parts = 2 if len(s.shape) == 3 else 1
        for lead in ([(e,) for e in range(s.shape[0])] if len(s.shape) == 3 else [()]):
            for k in range(parts):
                at = lead + (pl.ds(k * rows // parts, rows // parts),)
                i = len(pieces)
                pieces.append((pltpu.make_async_copy(s.at[at], b.at[at], in_sem.at[i]), pltpu.make_async_copy(b.at[at], d.at[at], out_sem.at[i])))
    for read, _ in pieces:
        read.start()
    for read, write in pieces:
        read.wait()
        write.start()
    for _, write in pieces:
        write.wait()


def deliver(arrays):
    n = 2 + 4 * (len(arrays) - 2)
    return pl.pallas_call(
        deliver_kernel,
        out_shape=tuple(jax.ShapeDtypeStruct(a.shape, a.dtype) for a in arrays),
        in_specs=[ANY] * len(arrays),
        out_specs=(ANY,) * len(arrays),
        scratch_shapes=[VMEM(a.shape, a.dtype) for a in arrays] + [DMA((n,)), DMA((n,))],
        compiler_params=pltpu.CompilerParams(vmem_limit_bytes=67043328),
        name="deliver",
    )(*arrays)


def solution(mesh):
    rows_spec = P(("dp", "ep"), None)
    cube_spec = P(("dp", "ep"), None, None)
    weight_spec = P("ep", None, None)

    def local_step(grad_y, gate_vals, topk_idx, slot_ids, pair_counts, y_routed, x_disp, h_gate, h_up, w_gate, w_up, w_down):
        n_loc, n_rows, ffn = h_gate.shape
        tok, dim = grad_y.shape
        top_k = topk_idx.shape[1]
        half = dim // 2
        cap = n_rows // 16
        shape = jax.ShapeDtypeStruct
        grad_x, grad_gate, grad_wdown, grad_wgate, grad_wup = pl.pallas_call(
            step_kernel,
            out_shape=(shape((tok, dim), BF16), shape((top_k, tok), F32), shape((n_loc, ffn, dim), F32), shape((n_loc, dim, ffn), F32), shape((n_loc, dim, ffn), F32)),
            in_specs=[ANY] * 12,
            out_specs=(VM, VM, ANY, ANY, ANY),
            scratch_shapes=[
                VMEM((tok, dim), BF16), VMEM((top_k, tok), jnp.int32), VMEM((top_k, tok), jnp.int32), VMEM((top_k, tok), F32), pltpu.SMEM(pair_counts.shape, jnp.int32),
                VMEM((16, tok, dim), BF16), VMEM((16, 8, 1, tok), F32), VMEM((8, 8, 1, tok), F32),
                VMEM((2, 2, n_loc, 2 * cap, ffn), BF16),
                VMEM((n_loc, ffn, dim), BF16), VMEM((n_loc, dim, ffn), BF16), VMEM((n_loc, dim, ffn), BF16),
                VMEM((2, n_rows, 256), BF16), VMEM((2, 256, dim), BF16),
                VMEM((2 * cap, dim), BF16), VMEM((2 * cap, ffn), BF16),
                VMEM((n_loc, n_rows, ffn), BF16), VMEM((n_loc, n_rows, ffn), BF16), VMEM((n_loc, ffn, dim), F32),
                VMEM((2, n_loc, 2 * cap, half), BF16), VMEM((2, n_loc, 2 * cap, half), BF16), VMEM((8, n_loc, 2 * cap, half), BF16),
                VMEM((16, tok, half), F32), VMEM((13, tok, half), F32), VMEM((8, tok, half), F32),
                VMEM((tok, half), BF16), VMEM((tok, half), BF16),
                VMEM((2, 256, ffn), F32), VMEM((2, 256, ffn), F32),
                DMA((5,)), DMA((3,)), DMA((2, 2)), DMA((2,)), DMA((2,)), DMA((2, 2)), DMA((1,)),
                DMA((16, 4, 2)), DMA((16, 2)), DMA((16,)), DMA((16,)), DMA((8, n_loc)), DMA((8, n_loc)), DMA((8, 2)), DMA((8, 2)), DMA((10, 2)), DMA((13, 2)), DMA((2,)), DMA((2,)),
            ],
            compiler_params=pltpu.CompilerParams(collective_id=1, has_side_effects=True, vmem_limit_bytes=67043328),
            name="step",
        )(grad_y, topk_idx.T, slot_ids.T, gate_vals.T, pair_counts, y_routed.reshape(tok * top_k, dim), h_gate, h_up, w_down, w_gate, w_up, x_disp)
        grad_wgate, grad_wup, grad_wdown, grad_x, grad_gate = deliver((grad_wgate, grad_wup, grad_wdown, grad_x, grad_gate))
        return grad_x, grad_gate.T, grad_wgate, grad_wup, grad_wdown

    return jax.shard_map(local_step, mesh=mesh, in_specs=(rows_spec, rows_spec, rows_spec, rows_spec, rows_spec, cube_spec, cube_spec, cube_spec, cube_spec, weight_spec, weight_spec, weight_spec), out_specs=(rows_spec, rows_spec, cube_spec, cube_spec, cube_spec), check_vma=False)
```

```python
import jax
import jax.numpy as jnp
from jax import lax
from jax.experimental import pallas as pl
from jax.experimental.pallas import tpu as pltpu
from jax.sharding import PartitionSpec as P

F32 = jnp.float32
BF16 = jnp.bfloat16
VMEM = pltpu.VMEM
DMA = pltpu.SemaphoreType.DMA
Z0, Z1, Z2, Z3 = range(4)
OWN, OTHER = CORE0, CORE1 = LO, HI = CORES = HALVES = range(2)
ONWARD, DOWN, CROSS, CORE = range(4)
NZ, GROUP = 4, 16
PEERS = range(1, GROUP)
ANY = pl.BlockSpec(memory_space=pl.ANY)
VM = pl.BlockSpec(memory_space=pltpu.VMEM)


def position():
    me = lax.axis_index("ep")
    return me, me // 4, (me // 2) % 2, me % 2


def mirror(z, v):
    return v + (z // 2) * (3 - 2 * v)


def dot_nt(a, b):
    return lax.dot_general(a, b, (((1,), (1,)), ((), ())), preferred_element_type=F32)


def dot_tn(a, b):
    return lax.dot_general(a, b, (((0,), (0,)), ((), ())), preferred_element_type=F32)


def one_hot(slot, cap):
    return slot == lax.broadcasted_iota(jnp.int32, (cap, slot.shape[1]), 0).astype(F32)


def step_kernel(gy_hbm, idx_hbm, slot_hbm, gate_hbm, counts_hbm, yr_hbm, hg_hbm, hu_hbm, wd_hbm, wg_hbm, wu_hbm, x_hbm, gx, gg, gwd_hbm, gwg_hbm, gwu_hbm,
                gy, idx_t, slot_t, gate_t, counts, tok, meta, meta_out, hbuf, wd, wg, wu, xs, yr, d_ref, a_ref, dh1, dh3, acc, r_own, r_send, r_recv, tot, z_in, y_in, f_send, f_recv, f_own, og, ou,
                in_sem, w_sem, h_sem, x_sem, g_sem, st_sem, acc_sem, send, recv, m_send, m_recv, rs, rr, ys, yrs, zs_sem, zr_sem, fs, fr, gx_sem):
    me, z, y, c = position()
    n_loc, n_rows, ffn = dh1.shape
    cap = n_rows // 16
    half = r_own.shape[3]
    n_exp = counts.shape[1]
    sib = me + 1 - 2 * c
    ynb = me + 2 - 4 * y
    m = z // 2
    q = mirror(z, z)
    way = 1 - 2 * m
    end = q == 0
    mid = q == 1
    up = (me + 4 * way + GROUP) % GROUP
    down = (me - 4 * way + GROUP) % GROUP

    barrier = pltpu.get_barrier_semaphore()
    for k in PEERS:
        pl.semaphore_signal(barrier, inc=1, device_id={"ep": (me + k) % GROUP})
    inputs = [pltpu.make_async_copy(src, dst, in_sem.at[i]) for i, (src, dst) in enumerate(((gy_hbm, gy), (idx_hbm, idx_t), (slot_hbm, slot_t), (gate_hbm, gate_t), (counts_hbm, counts)))]
    for cp in inputs:
        cp.start()

    order = (((Z0, OWN), (Z1, OWN)), ((Z0, OTHER), (Z0, OWN)), ((Z1, OWN), (Z2, OWN)), ((Z1, OTHER), (Z1, OTHER)), ((Z2, OWN), (Z0, OTHER)), ((Z2, OTHER), (Z3, OWN)), ((Z3, OWN), (Z2, OTHER)), ((Z3, OTHER), (Z3, OTHER)))

    def chip_of(t):
        (d_end, o_end), (d_mid, o_mid) = order[t]
        other = o_end + q * (o_mid - o_end)
        return mirror(z, d_end + q * (d_mid - d_end)), y + other * (1 - 2 * y)

    def rows_of(chip):
        return pl.ds(pl.multiple_of(chip * 2 * cap, 2 * cap), 2 * cap)

    def h_loads(t):
        d, yy = chip_of(t)
        rows = rows_of(d * 2 + yy)
        return [pltpu.make_async_copy(src.at[:, rows, :], hbuf.at[t % 2, i], h_sem.at[t % 2, i]) for i, src in enumerate((hg_hbm, hu_hbm))]

    w_loads = [pltpu.make_async_copy(src, dst, w_sem.at[i]) for i, (src, dst) in enumerate(((wd_hbm, wd), (wg_hbm, wg), (wu_hbm, wu)))]
    def yr_load(i):
        return pltpu.make_async_copy(yr_hbm.at[pl.ds(pl.multiple_of(i * 256, 256), 256), :], yr.at[i % 2], g_sem.at[i % 2])


    part_rows = gy.shape[0] // 2

    def part(p):
        return pl.ds(p * part_rows, part_rows)

    def put(slot, link, to, p, src=None):
        src = tok.at[slot, part(p)] if src is None else src
        return pltpu.make_async_remote_copy(src_ref=src, dst_ref=tok.at[slot, part(p)], send_sem=send.at[slot, link, p], recv_sem=recv.at[slot, p], device_id={"ep": to})

    def arrive(slot, p):
        put(slot, 0, me, p).wait_recv()

    def meta_copy(k):
        to = (me + k) % GROUP
        return pltpu.make_async_remote_copy(src_ref=meta_out.at[to // 2], dst_ref=meta.at[me], send_sem=m_send.at[k], recv_sem=m_recv.at[me], device_id={"ep": to})

    own = [(put(me, link, to, p, gy.at[part(p)]), cond) for p in HALVES for link, to, cond in ((ONWARD, up, None), (DOWN, down, mid), (CROSS, ynb, None), (CORE, sib, None))]
    inputs[0].wait()
    for cp in h_loads(0) + w_loads:
        cp.start()
    yr_load(0).start()
    pl.semaphore_wait(barrier, GROUP - 1)
    for cp, cond in own:
        cp.start() if cond is None else pl.when(cond)(cp.start)

    for cp in inputs[1:]:
        cp.wait()
    idx, slots, gates = idx_t[...], slot_t[...], gate_t[...]
    for e in range(n_exp):
        hit = idx == e
        slot = jnp.max(jnp.where(hit, slots, -1), axis=0, keepdims=True)
        slot = jnp.where(slot < counts[0, e], slot, -1)
        meta_out[e // 4, e % 4] = slot.astype(F32)
        meta_out[e // 4, 4 + e % 4] = jnp.sum(jnp.where(hit, gates, 0.0), axis=0, keepdims=True)
    for k in PEERS:
        meta_copy(k).start()
    tok[me] = gy[...]
    meta[me] = meta_out[me // 2]
    acc[...] = jnp.zeros_like(acc)

    gg[...] = jnp.zeros_like(gg)

    def gate_block(i, _):
        yr_load(i).wait()

        @pl.when(i < 7)
        def _():
            yr_load(i + 1).start()

        base = pl.multiple_of((i // 4) * 128, 128)
        prod = dot_nt(yr[i % 2], gy[pl.ds(base, 128), :]).reshape(32, 8, 128)
        t = lax.broadcasted_iota(jnp.int32, prod.shape, 0) + (i % 4) * 32
        mine = t == lax.broadcasted_iota(jnp.int32, prod.shape, 2)
        gg[:, pl.ds(base, 128)] += jnp.sum(jnp.where(mine, prod, 0.0), axis=0)
        return 0

    lax.fori_loop(0, 8, gate_block, 0)
    for cp in w_loads:
        cp.wait()

    def home(d, other, h):
        return mirror(z, d) * 4 + (y + other * (1 - 2 * y)) * 2 + h

    def relay(d, other, p, links):
        slot = home(d, other, c)
        arrive(slot, p)
        for link in links:
            put(slot, link, ynb if link == CROSS else sib if link == CORE else up if d == Z0 else down, p).start()

    def y_arrival(d, p, onward=False):
        slot = home(d, 1, c)
        arrive(slot, p)
        if onward:
            put(slot, ONWARD, up, p).start()
        put(slot, CORE, sib, p).start()

    def z_base(d, other, h):
        return mirror(z, d) * 2 + h if other == 0 else 7 + mirror(z, d)

    def z_slot(d, other, h, leftward, to_z):
        return jnp.where(leftward & (mirror(z, d) == to_z), 12 if other else 10 + h, z_base(d, other, h))

    def z_copy(d, other, h, p, step):
        dst = z_slot(d, other, h, step < 0, z + step)
        return pltpu.make_async_remote_copy(src_ref=tot.at[home(d, other, h), part(p)], dst_ref=z_in.at[dst, part(p)], send_sem=zs_sem.at[z_base(d, other, h), p], recv_sem=zr_sem.at[dst, p], device_id={"ep": (me + 4 * step + GROUP) % GROUP})

    def z_add(d, other, h, p, step):
        src, w = z_slot(d, other, h, step < 0, z), home(d, other, h)
        pltpu.make_async_remote_copy(src_ref=tot.at[w, part(p)], dst_ref=z_in.at[src, part(p)], send_sem=zs_sem.at[z_base(d, other, h), p], recv_sem=zr_sem.at[src, p], device_id={"ep": me}).wait_recv()
        tot[w, part(p)] = tot[w, part(p)] + z_in[src, part(p)]

    def y_copy(d, h, p):
        i = mirror(z, d) * 2 + h
        return pltpu.make_async_remote_copy(src_ref=tot.at[home(d, 1, h), part(p)], dst_ref=y_in.at[i, part(p)], send_sem=ys.at[i, p], recv_sem=yrs.at[i, p], device_id={"ep": ynb})

    def y_add(d, h, p):
        y_copy(d, h, p).wait_recv()
        w = home(d, 0, h)
        tot[w, part(p)] = tot[w, part(p)] + y_in[mirror(z, d) * 2 + h, part(p)]

    def y_start(d, h):
        for p in HALVES:
            y_copy(d, h, p).start()

    def start_up(d, other, h):
        for p in HALVES:
            z_copy(d, other, h, p, way).start()

    def pass_up(d, other, h, p):
        z_add(d, other, h, p, way)
        z_copy(d, other, h, p, way).start()

    def y_up(d, h, p):
        y_add(d, h, p)
        z_copy(d, OWN, h, p, way).start()

    def y_chain(d, h, p):
        y_add(d, h, p)
        pass_up(d, OWN, h, p)

    def y_down(d, h, p):
        y_add(d, h, p)
        z_add(d, OWN, h, p, -way)
        z_copy(d, OWN, h, p, -way).start()

    def swap(chip, slot, e):
        return pltpu.make_async_remote_copy(src_ref=r_send.at[slot, e], dst_ref=r_recv.at[chip, e], send_sem=rs.at[chip, e], recv_sem=rr.at[chip, e], device_id={"ep": sib})

    def build_rows(chip, e):
        for h in CORES:
            s = chip * 2 + h
            hot = one_hot(meta[s, c * 2 + e], cap)
            gate = jnp.sum(jnp.where(hot, meta[s, 4 + c * 2 + e], 0.0), axis=1, keepdims=True)
            picked = jnp.dot(jnp.where(hot, 1.0, 0.0).astype(BF16), tok[s], preferred_element_type=F32)
            d_ref[h * cap:(h + 1) * cap, :] = (picked * gate).astype(BF16)

    def make(t):
        slot = t % 2
        d, yy = chip_of(t)
        chip = d * 2 + yy
        for h in CORES:
            src = chip * 2 + h

            def table(src=src):
                pltpu.make_async_remote_copy(src_ref=meta_out.at[0], dst_ref=meta.at[src], send_sem=m_send.at[0], recv_sem=m_recv.at[src], device_id={"ep": src}).wait_recv()

            table() if t else pl.when(src != me)(table)
        for p in HALVES:
            arrive(chip * 2 + 1 - c, p)
        rows = rows_of(chip)
        for cp in h_loads(t):
            cp.wait()
        if t < 7:
            for cp in h_loads(t + 1):
                cp.start()

        def per_expert(e, _):
            build_rows(chip, e)
            g = dot_nt(d_ref[...], wd[e]).astype(BF16).astype(F32)
            h1 = hbuf[t % 2, 0, e].astype(F32)
            h3 = hbuf[t % 2, 1, e].astype(F32)
            sig = jax.nn.sigmoid(h1)
            act = h1 * sig
            dh1[e, rows, :] = (g * h3 * sig * (1.0 + h1 * (1.0 - sig))).astype(BF16)
            dh3[e, rows, :] = (g * act).astype(BF16)

            def ret_rows(side):
                cols = pl.ds(pl.multiple_of(side * half, half), half)
                return (dot_nt(dh1[e, rows, :], wg[e, cols, :]) + dot_nt(dh3[e, rows, :], wu[e, cols, :])).astype(BF16)

            r_send[slot, e] = ret_rows(1 - c)
            swap(chip, slot, e).start()
            r_own[slot, e] = ret_rows(c)
            return 0

        lax.fori_loop(0, n_loc, per_expert, 0)

    def combine(t):
        slot = t % 2
        d, yy = chip_of(t)
        chip = d * 2 + yy
        for e in range(n_loc):
            swap(chip, slot, e).wait_recv()
        for h in CORES:
            s = chip * 2 + h
            lanes = pl.ds(h * cap, cap)
            ids = (c * 2, c * 2 + 1, 2 - c * 2, 3 - c * 2)
            pick = jnp.concatenate([jnp.where(one_hot(meta[s, i], cap), 1.0, 0.0).astype(BF16) for i in ids], axis=0)
            vals = jnp.concatenate([r_own[slot, 0, lanes, :], r_own[slot, 1, lanes, :], r_recv[chip, 0, lanes, :], r_recv[chip, 1, lanes, :]], axis=0)
            tot[s] = dot_tn(pick, vals)
        for e in range(n_loc):
            swap(chip, slot, e).wait_send()

    def at_end(fn):
        pl.when(end)(fn)

    def at_mid(fn):
        pl.when(mid)(fn)

    make(0)
    combine(0)

    @at_end
    def _():
        for p in HALVES:
            y_arrival(Z0, p, True)
            relay(Z1, OWN, p, (CROSS, CORE))

    @at_mid
    def _():
        for p in HALVES:
            relay(Z0, OWN, p, (ONWARD, CORE))
            y_arrival(Z1, p)
            relay(Z2, OWN, p, (ONWARD, CROSS, CORE))

    def second(p):
        @at_end
        def _():
            y_arrival(Z1, p)
            relay(Z2, OWN, p, (CROSS, CORE))

        @at_mid
        def _():
            relay(Z0, OTHER, p, (ONWARD, CORE))
            y_arrival(Z2, p)
            relay(Z3, OWN, p, (ONWARD, CORE))

    def third(p):
        @at_end
        def _():
            y_arrival(Z2, p)
            relay(Z3, OWN, p, (CORE,))

        @at_mid
        def _():
            relay(Z3, OTHER, p, (ONWARD, CORE))

    make(1)
    make(2)
    second(LO)
    combine(1)
    combine(2)
    at_end(lambda: start_up(Z1, OWN, CORE0))
    second(HI)
    make(3)
    make(4)
    third(LO)
    combine(3)
    y_start(Z1, CORE1)
    combine(4)
    at_end(lambda: start_up(Z2, OWN, CORE0))
    at_mid(lambda: y_start(Z0, CORE0))
    third(HI)
    make(5)
    make(6)
    at_end(lambda: relay(Z3, OTHER, LO, (CORE,)))
    combine(5)

    @at_end
    def _():
        start_up(Z2, OTHER, CORE0)
        y_start(Z2, CORE1)

    combine(6)
    at_end(lambda: relay(Z3, OTHER, HI, (CORE,)))
    at_mid(lambda: pass_up(Z2, OWN, CORE0, LO))
    make(7)
    combine(7)
    y_start(Z3, CORE0)
    y_start(Z3, CORE1)
    at_end(lambda: y_start(Z0, CORE0))
    y_start(Z0, CORE1)
    at_mid(lambda: y_start(Z2, CORE1))

    width = xs.shape[2]

    def x_load(i):
        e, t = i // 4, i % 4
        return pltpu.make_async_copy(x_hbm.at[e, :, pl.ds(pl.multiple_of(t * width, width), width)], xs.at[i % 2], x_sem.at[i % 2])

    def w_out(i):
        e, t = i // 4, i % 4
        rows = pl.ds(pl.multiple_of(t * width, width), width)
        return (pltpu.make_async_copy(og.at[i % 2], gwg_hbm.at[e, rows, :], st_sem.at[i % 2, 0]),
                pltpu.make_async_copy(ou.at[i % 2], gwu_hbm.at[e, rows, :], st_sem.at[i % 2, 1]))

    def end_tail():
        y_up(Z3, CORE1, HI)
        start_up(Z1, OTHER, CORE0)
        for p in HALVES:
            y_up(Z1, CORE1, p)

    def end_first():
        for p in HALVES:
            y_up(Z2, CORE1, p)

    end_events = dict(enumerate((end_first, lambda: y_up(Z3, CORE0, LO), lambda: y_up(Z3, CORE0, HI), lambda: y_up(Z3, CORE1, LO), end_tail)))
    mid_events = {0: lambda: pass_up(Z2, OWN, CORE0, HI), 1: lambda: pass_up(Z2, OTHER, CORE0, LO), 2: lambda: pass_up(Z2, OTHER, CORE0, HI), 6: lambda: y_chain(Z3, CORE0, LO), 7: lambda: y_chain(Z3, CORE0, HI)}
    def tail_loads(i):
        rows = rows_of(i)
        return [pltpu.make_async_copy(src.at[:, rows, :], hbuf.at[i % 2, n], h_sem.at[i % 2, n]) for n, src in enumerate((hg_hbm, hu_hbm))]

    x_load(0).start()
    for cp in tail_loads(0):
        cp.start()

    def down_grad(i):
        for cp in tail_loads(i):
            cp.wait()

        @pl.when(i < 7)
        def _():
            for cp in tail_loads(i + 1):
                cp.start()

        def per_expert(e, _):
            build_rows(i, e)
            h1 = hbuf[i % 2, 0, e].astype(F32)
            a_ref[...] = (h1 * jax.nn.sigmoid(h1) * hbuf[i % 2, 1, e].astype(F32)).astype(BF16)
            acc[e] += dot_tn(a_ref[...], d_ref[...])
            return 0

        lax.fori_loop(0, n_loc, per_expert, 0)


    def weights(i, _):
        x_load(i).wait()

        @pl.when(i < 7)
        def _():
            x_load(i + 1).start()

        @pl.when(i >= 2)
        def _():
            for cp in w_out(i - 2):
                cp.wait()

        e = i // 4
        og[i % 2] = dot_tn(xs[i % 2], dh1[e])
        ou[i % 2] = dot_tn(xs[i % 2], dh3[e])
        for cp in w_out(i):
            cp.start()
        down_grad(i)
        for n, event in mid_events.items():
            pl.when(mid & (i == n))(event)
        for n, event in end_events.items():
            pl.when(end & (i == n))(event)
        return 0

    lax.fori_loop(0, 8, weights, 0)
    acc_out = pltpu.make_async_copy(acc, gwd_hbm, acc_sem.at[0])
    acc_out.start()

    def cross(p):
        z_add(Z1, OTHER, CORE0, p, -way)
        z_add(Z1, OTHER, CORE0, p, way)
        y_copy(Z1, CORE0, p).start()

    @at_mid
    def _():
        y_down(Z0, CORE0, LO)
        y_chain(Z3, CORE1, LO)
        y_down(Z0, CORE0, HI)
        y_chain(Z3, CORE1, HI)
        y_down(Z0, CORE1, LO)
        cross(0)
        y_chain(Z2, CORE1, LO)
        y_down(Z0, CORE1, HI)
        cross(1)
        y_chain(Z2, CORE1, HI)

    for cp, cond in own:
        cp.wait_send() if cond is None else pl.when(cond)(cp.wait_send)

    def drain_tokens(*tokens):
        for p in HALVES:
            for d, other, links in tokens:
                for link in links:
                    put(home(d, other, c), link, me, p).wait_send()

    def drain_units(y_units, z_units):
        for p in HALVES:
            for d, h in y_units:
                y_copy(d, h, p).wait_send()
            for d, other, h in z_units:
                z_copy(d, other, h, p, way).wait_send()

    SENT = (CORE,)
    at_end(lambda: drain_tokens((Z0, OTHER, (ONWARD, CORE)), (Z1, OWN, (CROSS, CORE)), (Z1, OTHER, SENT), (Z2, OWN, (CROSS, CORE)), (Z2, OTHER, SENT), (Z3, OWN, SENT), (Z3, OTHER, SENT)))
    at_mid(lambda: drain_tokens((Z1, OTHER, SENT), (Z0, OWN, (ONWARD, CORE)), (Z0, OTHER, (ONWARD, CORE)), (Z2, OWN, (ONWARD, CROSS, CORE)), (Z2, OTHER, SENT), (Z3, OWN, (ONWARD, CORE)), (Z3, OTHER, (ONWARD, CORE))))
    for k in PEERS:
        meta_copy(k).wait_send()
    for i in (6, 7):
        for cp in w_out(i):
            cp.wait()
    acc_out.wait()

    def last(p):
        return pltpu.make_async_remote_copy(src_ref=f_send.at[part(p)], dst_ref=f_recv.at[part(p)], send_sem=fs.at[p], recv_sem=fr.at[p], device_id={"ep": sib})

    def gx_copy(side, p):
        cols = pl.ds(pl.multiple_of((c + side * (1 - 2 * c)) * half, half), half)
        return pltpu.make_async_copy((f_recv if side else f_own).at[part(p)], gx.at[part(p), cols], gx_sem.at[side, p])

    def finish(h, p):
        w = me - c + h
        i = z * 2 + h
        pltpu.make_async_remote_copy(src_ref=tot.at[w, part(p)], dst_ref=y_in.at[i, part(p)], send_sem=ys.at[i, p], recv_sem=yrs.at[i, p], device_id={"ep": ynb}).wait_recv()
        tot[w, part(p)] = tot[w, part(p)] + y_in[i, part(p)]
        at_end(lambda: z_add(Z0, OWN, h, p, -way))

        @at_mid
        def _():
            z_add(Z1, OWN, h, p, -way)
            z_add(Z1, OWN, h, p, way)

        @pl.when(c == h)
        def _():
            f_own[part(p)] = tot[w, part(p)].astype(BF16)
            gx_copy(OWN, p).start()

        @pl.when(c != h)
        def _():
            f_send[part(p)] = tot[w, part(p)].astype(BF16)
            last(p).start()

    for p in HALVES:
        for h in CORES:
            finish(h, p)
    for p in HALVES:
        last(p).wait()
        gx_copy(OTHER, p).start()
    at_end(lambda: drain_units(((Z0, CORE0), (Z0, CORE1), (Z1, CORE1), (Z2, CORE1), (Z3, CORE0), (Z3, CORE1)), ((Z1, OWN, CORE0), (Z1, OTHER, CORE0), (Z2, OWN, CORE0), (Z2, OTHER, CORE0), (Z1, OWN, CORE1), (Z2, OWN, CORE1), (Z3, OWN, CORE0), (Z3, OWN, CORE1))))
    at_mid(lambda: drain_units(((Z0, CORE0), (Z0, CORE1), (Z1, CORE0), (Z1, CORE1), (Z2, CORE1), (Z3, CORE0), (Z3, CORE1)), ((Z2, OWN, CORE0), (Z2, OTHER, CORE0), (Z3, OWN, CORE0), (Z3, OWN, CORE1), (Z0, OWN, CORE0), (Z0, OWN, CORE1), (Z2, OWN, CORE1))))
    for p in HALVES:
        for side in (OWN, OTHER):
            gx_copy(side, p).wait()


def deliver_kernel(*refs):
    n = (len(refs) - 2) // 3
    src, dst, buf, (in_sem, out_sem) = refs[:n], refs[n:2 * n], refs[2 * n:3 * n], refs[3 * n:]
    pieces = []
    for s, d, b in zip(src, dst, buf):
        rows = s.shape[-2]
        parts = 2 if len(s.shape) == 3 else 1
        for lead in ([(e,) for e in range(s.shape[0])] if len(s.shape) == 3 else [()]):
            for k in range(parts):
                at = lead + (pl.ds(k * rows // parts, rows // parts),)
                i = len(pieces)
                pieces.append((pltpu.make_async_copy(s.at[at], b.at[at], in_sem.at[i]), pltpu.make_async_copy(b.at[at], d.at[at], out_sem.at[i])))
    for read, _ in pieces:
        read.start()
    for read, write in pieces:
        read.wait()
        write.start()
    for _, write in pieces:
        write.wait()


def deliver(arrays):
    n = 2 + 4 * (len(arrays) - 2)
    return pl.pallas_call(
        deliver_kernel,
        out_shape=tuple(jax.ShapeDtypeStruct(a.shape, a.dtype) for a in arrays),
        in_specs=[ANY] * len(arrays),
        out_specs=(ANY,) * len(arrays),
        scratch_shapes=[VMEM(a.shape, a.dtype) for a in arrays] + [DMA((n,)), DMA((n,))],
        compiler_params=pltpu.CompilerParams(vmem_limit_bytes=67043328),
        name="deliver",
    )(*arrays)


def solution(mesh):
    rows_spec = P(("dp", "ep"), None)
    cube_spec = P(("dp", "ep"), None, None)
    weight_spec = P("ep", None, None)

    def local_step(grad_y, gate_vals, topk_idx, slot_ids, pair_counts, y_routed, x_disp, h_gate, h_up, w_gate, w_up, w_down):
        n_loc, n_rows, ffn = h_gate.shape
        tok, dim = grad_y.shape
        top_k = topk_idx.shape[1]
        half = dim // 2
        cap = n_rows // 16
        shape = jax.ShapeDtypeStruct
        grad_x, grad_gate, grad_wdown, grad_wgate, grad_wup = pl.pallas_call(
            step_kernel,
            out_shape=(shape((tok, dim), BF16), shape((top_k, tok), F32), shape((n_loc, ffn, dim), F32), shape((n_loc, dim, ffn), F32), shape((n_loc, dim, ffn), F32)),
            in_specs=[ANY] * 12,
            out_specs=(ANY, VM, ANY, ANY, ANY),
            scratch_shapes=[
                VMEM((tok, dim), BF16), VMEM((top_k, tok), jnp.int32), VMEM((top_k, tok), jnp.int32), VMEM((top_k, tok), F32), pltpu.SMEM(pair_counts.shape, jnp.int32),
                VMEM((16, tok, dim), BF16), VMEM((16, 8, 1, tok), F32), VMEM((8, 8, 1, tok), F32),
                VMEM((2, 2, n_loc, 2 * cap, ffn), BF16),
                VMEM((n_loc, ffn, dim), BF16), VMEM((n_loc, dim, ffn), BF16), VMEM((n_loc, dim, ffn), BF16),
                VMEM((2, n_rows, 256), BF16), VMEM((2, 256, dim), BF16),
                VMEM((2 * cap, dim), BF16), VMEM((2 * cap, ffn), BF16),
                VMEM((n_loc, n_rows, ffn), BF16), VMEM((n_loc, n_rows, ffn), BF16), VMEM((n_loc, ffn, dim), F32),
                VMEM((2, n_loc, 2 * cap, half), BF16), VMEM((2, n_loc, 2 * cap, half), BF16), VMEM((8, n_loc, 2 * cap, half), BF16),
                VMEM((16, tok, half), F32), VMEM((13, tok, half), F32), VMEM((8, tok, half), F32),
                VMEM((tok, half), BF16), VMEM((tok, half), BF16), VMEM((tok, half), BF16),
                VMEM((2, 256, ffn), F32), VMEM((2, 256, ffn), F32),
                DMA((5,)), DMA((3,)), DMA((2, 2)), DMA((2,)), DMA((2,)), DMA((2, 2)), DMA((1,)),
                DMA((16, 4, 2)), DMA((16, 2)), DMA((16,)), DMA((16,)), DMA((8, n_loc)), DMA((8, n_loc)), DMA((8, 2)), DMA((8, 2)), DMA((10, 2)), DMA((13, 2)), DMA((2,)), DMA((2,)), DMA((2, 2)),
            ],
            compiler_params=pltpu.CompilerParams(collective_id=1, has_side_effects=True, vmem_limit_bytes=67043328),
            name="step",
        )(grad_y, topk_idx.T, slot_ids.T, gate_vals.T, pair_counts, y_routed.reshape(tok * top_k, dim), h_gate, h_up, w_down, w_gate, w_up, x_disp)
        grad_wgate, grad_wup, grad_wdown, grad_x, grad_gate = deliver((grad_wgate, grad_wup, grad_wdown, grad_x, grad_gate))
        return grad_x, grad_gate.T, grad_wgate, grad_wup, grad_wdown

    return jax.shard_map(local_step, mesh=mesh, in_specs=(rows_spec, rows_spec, rows_spec, rows_spec, rows_spec, cube_spec, cube_spec, cube_spec, cube_spec, weight_spec, weight_spec, weight_spec), out_specs=(rows_spec, rows_spec, cube_spec, cube_spec, cube_spec), check_vma=False)
```
